16 devices in a mesh: fsdp: 4 (over z, y), ep: 4 (over x, core).
Axes of the slice: x: 2, y: 2, z: 2, core: 2. Of those that a mesh axis runs over, the one named last changes fastest.
Arguments:
- x_tok: bfloat16 [16384, 512], P(('fsdp', 'ep'))
- dy_tok: bfloat16 [16384, 512], P(('fsdp', 'ep'))
- expert_ids: int32 [16384, 8], P(('fsdp', 'ep'))
- route_w: float32 [16384, 8], P(('fsdp', 'ep'))
- w_gate: bfloat16 [64, 512, 1280], P('ep', 'fsdp')
- w_up: bfloat16 [64, 512, 1280], P('ep', 'fsdp')
- w_down: bfloat16 [64, 1280, 512], P('ep', None, 'fsdp')
Outputs:
- output 1: bfloat16 [16384, 512], P(('fsdp', 'ep'))
- output 2: float32 [16384, 8], P(('fsdp', 'ep'))
- output 3: float32 [64, 512, 1280], P('ep', 'fsdp')
- output 4: float32 [64, 512, 1280], P('ep', 'fsdp')
- output 5: float32 [64, 1280, 512], P('ep', None, 'fsdp')
All inputs are finite; a program needn't handle non-finite values.
Results may differ from the reference program's by a relative error of at most 0.00989157.
Values are sent between devices in bfloat16 or wider.
A program may use at most 1 GiB of HBM per device.

```python
import jax
import jax.numpy as jnp
from jax import lax

D_MODEL = 512
D_FF = 1280
EXPERTS = 64
TOP_K = 8
TOK_DEV = 1024
DEVICES = 16
CAPACITY = 384

TOKENS = DEVICES * TOK_DEV
SLOTS = EXPERTS * CAPACITY
HOT_COUNT = max(1, TOP_K // 2)


def draw_routing(root_key):
    key_hot, key_score = jax.random.split(root_key)
    hot_rank = jax.random.permutation(key_hot, EXPERTS)
    bias = jnp.where(hot_rank < HOT_COUNT, 768, 0).astype(jnp.int32)
    expert_col = jnp.arange(EXPERTS, dtype=jnp.int32)

    def one_device(dev_key):
        noise = jax.random.randint(dev_key, (TOK_DEV, EXPERTS), 0, 1024, dtype=jnp.int32)
        score = (noise + bias[None, :]) * EXPERTS + expert_col[None, :]
        return lax.top_k(score, TOP_K)[1]

    chosen = lax.map(one_device, jax.random.split(key_score, DEVICES))
    return chosen.reshape(TOKENS, TOP_K).astype(jnp.int32)


def setup_inputs(seed: int = 0) -> dict:
    key_list = jax.random.split(jax.random.key(seed), 7)
    x_tok = jax.random.normal(key_list[0], (TOKENS, D_MODEL), jnp.float32)
    dy_tok = jax.random.normal(key_list[1], (TOKENS, D_MODEL), jnp.float32)
    expert_ids = draw_routing(key_list[2])
    route_w = jax.random.uniform(key_list[3], (TOKENS, TOP_K), jnp.float32, 0.1, 1.0)
    w_gate = jax.random.normal(key_list[4], (EXPERTS, D_MODEL, D_FF), jnp.float32) * D_MODEL ** -0.5
    w_up = jax.random.normal(key_list[5], (EXPERTS, D_MODEL, D_FF), jnp.float32) * D_MODEL ** -0.5
    w_down = jax.random.normal(key_list[6], (EXPERTS, D_FF, D_MODEL), jnp.float32) * D_FF ** -0.5
    return {
        "x_tok": x_tok.astype(jnp.bfloat16),
        "dy_tok": dy_tok.astype(jnp.bfloat16),
        "expert_ids": expert_ids,
        "route_w": route_w,
        "w_gate": w_gate.astype(jnp.bfloat16),
        "w_up": w_up.astype(jnp.bfloat16),
        "w_down": w_down.astype(jnp.bfloat16),
    }


def slot_positions(ids_dev):
    onehot = (ids_dev[:, None] == jnp.arange(EXPERTS, dtype=jnp.int32)[None, :]).astype(jnp.int32)
    before = jnp.cumsum(onehot, axis=0) - onehot
    position = jnp.sum(before * onehot, axis=1)
    return jnp.where(position < CAPACITY, ids_dev * CAPACITY + position, SLOTS)


def swiglu_grads(pre_gate, pre_up, grad_hidden):
    sigma = jax.nn.sigmoid(pre_gate)
    grad_gate = grad_hidden * pre_up * sigma * (1.0 + pre_gate * (1.0 - sigma))
    grad_up = grad_hidden * pre_gate * sigma
    return grad_gate.astype(jnp.bfloat16), grad_up.astype(jnp.bfloat16)


def reference(x_tok, dy_tok, expert_ids, route_w, w_gate, w_up, w_down):
    dest_slot = lax.map(slot_positions, expert_ids.reshape(DEVICES, TOK_DEV * TOP_K))
    pair_ids = jnp.arange(TOKENS * TOP_K, dtype=jnp.int32).reshape(DEVICES, TOK_DEV * TOP_K)
    dev_rows = jnp.broadcast_to(jnp.arange(DEVICES, dtype=jnp.int32)[:, None], dest_slot.shape)
    slot_src = jnp.full((DEVICES, SLOTS + 1), TOKENS * TOP_K, jnp.int32)
    slot_src = slot_src.at[dev_rows, dest_slot].set(pair_ids)[:, :SLOTS]
    per_expert = slot_src.reshape(DEVICES, EXPERTS, CAPACITY).transpose(1, 0, 2).reshape(EXPERTS, DEVICES * CAPACITY)
    route_flat = route_w.reshape(-1)

    def expert_step(carry, step_in):
        dx_acc, dr_acc = carry
        pair_src, w_gate_e, w_up_e, w_down_e = step_in
        tok_rows = pair_src // TOP_K
        x_rows = jnp.take(x_tok, tok_rows, axis=0, mode="fill", fill_value=0)
        dy_rows = jnp.take(dy_tok, tok_rows, axis=0, mode="fill", fill_value=0)
        gate_rows = jnp.take(route_flat, pair_src, axis=0, mode="fill", fill_value=0)
        pre_gate = jnp.dot(x_rows, w_gate_e, preferred_element_type=jnp.float32)
        pre_up = jnp.dot(x_rows, w_up_e, preferred_element_type=jnp.float32)
        hidden = (jax.nn.silu(pre_gate) * pre_up).astype(jnp.bfloat16)
        y_rows = jnp.dot(hidden, w_down_e, preferred_element_type=jnp.float32)
        dy_wide = dy_rows.astype(jnp.float32)
        scaled_dy = (gate_rows[:, None] * dy_wide).astype(jnp.bfloat16)
        dr_rows = jnp.sum(dy_wide * y_rows, axis=1)
        grad_hidden = jnp.dot(scaled_dy, w_down_e.T, preferred_element_type=jnp.float32)
        grad_gate, grad_up = swiglu_grads(pre_gate, pre_up, grad_hidden)
        dx_rows = (jnp.dot(grad_gate, w_gate_e.T, preferred_element_type=jnp.float32)
                   + jnp.dot(grad_up, w_up_e.T, preferred_element_type=jnp.float32)).astype(jnp.bfloat16)
        dw_gate = jnp.dot(x_rows.T, grad_gate, preferred_element_type=jnp.float32)
        dw_up = jnp.dot(x_rows.T, grad_up, preferred_element_type=jnp.float32)
        dw_down = jnp.dot(hidden.T, scaled_dy, preferred_element_type=jnp.float32)
        dx_acc = dx_acc.at[tok_rows].add(dx_rows.astype(jnp.float32), mode="drop")
        dr_acc = dr_acc.at[pair_src].set(dr_rows, mode="drop")
        return (dx_acc, dr_acc), (dw_gate, dw_up, dw_down)

    init = (jnp.zeros((TOKENS, D_MODEL), jnp.float32), jnp.zeros((TOKENS * TOP_K,), jnp.float32))
    (dx_acc, dr_acc), (grad_w_gate, grad_w_up, grad_w_down) = lax.scan(
        expert_step, init, (per_expert, w_gate, w_up, w_down))
    grad_x = dx_acc.astype(jnp.bfloat16)
    route_w_grad = dr_acc.reshape(TOKENS, TOP_K)
    return (grad_x, route_w_grad, grad_w_gate, grad_w_up, grad_w_down)
```

```python
import functools

import jax
import jax.numpy as jnp
from jax import lax
from jax.experimental import pallas as pl
from jax.experimental.pallas import tpu as pltpu
from jax.sharding import PartitionSpec as P


CAP_FACTOR = 3
CHUNK = 128
TILE = 512
MM = 256
COPY = 64
VMEM_LIMIT = 60 * 1024 * 1024
F32 = jnp.float32
BF16 = jnp.bfloat16


def capacity_of(tok_dev, top_k, experts):
    return max(8, ((CAP_FACTOR * tok_dev * top_k // experts + 7) // 8) * 8)


def up(n, m):
    return (n + m - 1) // m * m


def blocks(n, size):
    return lax.div(n + (size - 1), jnp.full_like(n, size))


def dot(a, b):
    return lax.dot_general(a, b, (((1,), (0,)), ((), ())), preferred_element_type=F32)


def dot_nt(a, b):
    return lax.dot_general(a, b, (((1,), (1,)), ((), ())), preferred_element_type=F32)


def dot_tn(a, b):
    return lax.dot_general(a, b, (((0,), (0,)), ((), ())), preferred_element_type=F32)


def route_tables(expert_ids, route_w, experts, capacity):
    tok_dev, _ = expert_ids.shape
    ids_t, w_t = expert_ids.T, route_w.T
    hit = ids_t[:, None, :] == jnp.arange(experts, dtype=jnp.int32)[None, :, None]
    chosen = jnp.any(hit, axis=0)
    weight = jnp.sum(jnp.where(hit, w_t[:, None, :], 0.0), axis=0)
    earlier = jnp.arange(tok_dev)[:, None] < jnp.arange(tok_dev)[None, :]
    before = dot(chosen.astype(BF16), earlier.astype(BF16))
    position = jnp.where(chosen & (before < capacity), before, -1.0)
    return position, weight


def one_hot_block(pos_row, c):
    row = lax.broadcasted_iota(jnp.int32, (CHUNK, pos_row.shape[1]), 0) + c * CHUNK
    return row == pos_row


def aligned(v, m=16):
    return pl.multiple_of(v, m)


def gather_kernel(n_src, n_loc, region, with_r, *refs):
    if with_r:
        (cnt, off, pos_ref, r_ref, src_ref, out, r_out, hot, stage, pool, rstage, rpool, sem) = refs
    else:
        (cnt, off, pos_ref, src_ref, out, hot, stage, pool, sem) = refs
    s = pl.program_id(0)
    base = jnp.int32(0)
    starts = []
    for k in range(n_loc):
        n = cnt[s * n_loc + k]
        starts.append(base)
        pos_row = pos_ref[0, k:k + 1, :]

        def build(c, carry, base=base, pos_row=pos_row, k=k):
            m = one_hot_block(pos_row, c)
            at = pl.ds(aligned(base + c * CHUNK), CHUNK)
            hot[at, :] = jnp.where(m, 1.0, 0.0).astype(BF16)
            if with_r:
                r = jnp.sum(jnp.where(m, r_ref[0, k:k + 1, :], 0.0), axis=1, keepdims=True)
                rstage[at, :] = jnp.broadcast_to(r, (CHUNK, 128))
            return carry

        lax.fori_loop(0, blocks(n, CHUNK), build, 0)
        base = base + blocks(n, 16) * 16

    def mm(c, carry):
        at = pl.ds(aligned(c * MM), MM)
        stage[at, :] = dot(hot[at, :], src_ref[...]).astype(BF16)
        return carry

    lax.fori_loop(0, blocks(base, MM), mm, 0)

    for k in range(n_loc):
        n = cnt[s * n_loc + k]
        to = off[s * n_loc + k] + k * region

        def move(c, carry, start=starts[k], to=to):
            dst = pl.ds(aligned(to + c * COPY), COPY)
            frm = pl.ds(aligned(start + c * COPY), COPY)
            pool[dst, :] = stage[frm, :]
            if with_r:
                rpool[dst, :] = rstage[frm, :]
            return carry

        lax.fori_loop(0, blocks(n, COPY), move, 0)

    @pl.when(s == n_src - 1)
    def _():
        def copies(k, i):
            at = pl.ds(aligned(k * region + i * TILE, TILE), TILE)
            made = [pltpu.make_async_copy(pool.at[at], out.at[at], sem)]
            if with_r:
                made.append(pltpu.make_async_copy(rpool.at[at], r_out.at[at], sem))
            return made

        tiles = []
        for k in range(n_loc):
            end = off[s * n_loc + k] + blocks(cnt[s * n_loc + k], 16) * 16
            at = pl.ds(aligned(k * region + end), TILE)
            pool[at, :] = jnp.zeros((TILE, pool.shape[1]), BF16)
            if with_r:
                rpool[at, :] = jnp.zeros((TILE, 128), F32)
            tiles.append(jnp.maximum(1, blocks(end, TILE)))
        for k in range(n_loc):
            def start(i, carry, k=k):
                for copy in copies(k, i):
                    copy.start()
                return carry

            lax.fori_loop(0, tiles[k], start, 0)
        for k in range(n_loc):
            def wait(i, carry, k=k):
                for copy in copies(k, i):
                    copy.wait()
                return carry

            lax.fori_loop(0, tiles[k], wait, 0)


def gather_rows(src, cnt, off, pos, r, region):
    n_src, n_loc, tok = pos.shape
    d = src.shape[1]
    with_r = r is not None
    rows = n_loc * region
    scr = n_loc * ((region - TILE) // n_src) + CHUNK
    scr = up(scr, MM)
    table = pl.BlockSpec((1, n_loc, tok), lambda s, *_: (s, 0, 0))
    in_specs = [table] + ([table] if with_r else []) + [pl.BlockSpec((tok, d), lambda s, *_: (s, 0))]
    out_shape = [jax.ShapeDtypeStruct((rows, d), BF16)]
    scratch = [pltpu.VMEM((scr, tok), BF16), pltpu.VMEM((scr, d), BF16), pltpu.VMEM((rows, d), BF16)]
    if with_r:
        out_shape.append(jax.ShapeDtypeStruct((rows, 128), F32))
        scratch += [pltpu.VMEM((scr, 128), F32), pltpu.VMEM((rows, 128), F32)]
    out = pl.pallas_call(
        functools.partial(gather_kernel, n_src, n_loc, region, with_r),
        out_shape=out_shape,
        grid_spec=pltpu.PrefetchScalarGridSpec(
            num_scalar_prefetch=2, grid=(n_src,), in_specs=in_specs,
            out_specs=[pl.BlockSpec(memory_space=pl.ANY)] * len(out_shape),
            scratch_shapes=scratch + [pltpu.SemaphoreType.DMA]),
        compiler_params=pltpu.CompilerParams(vmem_limit_bytes=VMEM_LIMIT, dimension_semantics=("arbitrary",)),
        cost_estimate=pl.CostEstimate(flops=2 * 12000 * tok * d, bytes_accessed=n_src * tok * d * 4, transcendentals=0),
        name="gather_r" if with_r else "gather_x",
    )(*([cnt, off, pos] + ([r] if with_r else []) + [src]))
    return out if with_r else out[0]


def expert_kernel(n_fs, info, x_ref, dy_ref, r_ref, w1_ref, w3_ref, w2s_ref, dx_ref, dr_ref, *refs):
    outs, (w2, a_buf, dh1_buf, dh3_buf, dw1, dw3, dw2t) = refs[:n_fs], refs[n_fs:]
    i = pl.program_id(0)
    d, f = w1_ref.shape
    dsl = d // n_fs

    @pl.when(i == 0)
    def _():
        dw1[...] = jnp.zeros_like(dw1)
        dw3[...] = jnp.zeros_like(dw3)
        dw2t[...] = jnp.zeros_like(dw2t)
        for q in range(n_fs):
            w2[:, q * dsl:(q + 1) * dsl] = w2s_ref[q]

    def tile(m):
        x, dy = x_ref[:m, :], dy_ref[:m, :]
        dy_wide = dy.astype(F32)
        g = (r_ref[:m, 0:1] * dy_wide).astype(BF16)
        step = 256
        for c in range(0, f, step):
            cs = slice(c, c + step)
            h1 = dot(x, w1_ref[:, cs])
            h3 = dot(x, w3_ref[:, cs])
            da = dot_nt(g, w2[cs, :])
            s = jax.nn.sigmoid(h1)
            hs = h1 * s
            a_buf[:m, cs] = (hs * h3).astype(BF16)
            dh1_buf[:m, cs] = (da * h3 * s * (1.0 + h1 * (1.0 - s))).astype(BF16)
            dh3_buf[:m, cs] = (da * hs).astype(BF16)
        y = dot(a_buf[:m, :], w2[...])
        dr = jnp.sum(dy_wide * y, axis=1, keepdims=True)
        dr_ref[:m, :] = jnp.broadcast_to(dr, (m, 128))
        dx_ref[:m, :] = (dot_nt(dh1_buf[:m, :], w1_ref[...]) + dot_nt(dh3_buf[:m, :], w3_ref[...])).astype(BF16)
        dw1[...] += dot_tn(x, dh1_buf[:m, :])
        dw3[...] += dot_tn(x, dh3_buf[:m, :])
        dw2t[...] += dot_tn(g, a_buf[:m, :])

    left = info[0] - i * TILE

    @pl.when(left > TILE // 2)
    def _():
        tile(TILE)

    @pl.when((i < info[1]) & (left <= TILE // 2))
    def _():
        tile(TILE // 2)
        dx_ref[TILE // 2:, :] = jnp.zeros((TILE // 2, d), BF16)
        dr_ref[TILE // 2:, :] = jnp.zeros((TILE // 2, 128), F32)

    @pl.when(i == info[1] - 1)
    def _():
        for m in range(n_fs):
            at = pl.ds(aligned((info[2] ^ m) * dsl, dsl), dsl)
            for t, acc in enumerate((dw1, dw3, dw2t)):
                outs[m][t] = acc[at, :]


def expert_call(k, info, x_pool, dy_pool, r_pool, w1, w3, w2s, region):
    n_fs, f, dsl = w2s.shape
    d = w1.shape[0]
    first = k * (region // TILE)
    row_map = lambda i, info: (first + jnp.minimum(i, info[1] - 1), 0)
    out_map = lambda i, info: (jnp.minimum(i, info[1] - 1), 0)
    whole = lambda i, info: (0, 0)
    whole3 = lambda i, info: (0, 0, 0)
    return pl.pallas_call(
        functools.partial(expert_kernel, n_fs),
        out_shape=[jax.ShapeDtypeStruct((region, d), BF16), jax.ShapeDtypeStruct((region, 128), F32)]
        + [jax.ShapeDtypeStruct((3, dsl, f), F32)] * n_fs,
        grid_spec=pltpu.PrefetchScalarGridSpec(
            num_scalar_prefetch=1, grid=(region // TILE - 1,),
            in_specs=[pl.BlockSpec((TILE, d), row_map), pl.BlockSpec((TILE, d), row_map), pl.BlockSpec((TILE, 128), row_map),
                      pl.BlockSpec((d, f), whole), pl.BlockSpec((d, f), whole),
                      pl.BlockSpec((n_fs, f, dsl), whole3)],
            out_specs=[pl.BlockSpec((TILE, d), out_map), pl.BlockSpec((TILE, 128), out_map)]
            + [pl.BlockSpec((3, dsl, f), whole3)] * n_fs,
            scratch_shapes=[pltpu.VMEM((f, d), BF16)] + [pltpu.VMEM((TILE, f), BF16)] * 3 + [pltpu.VMEM((d, f), F32)] * 3),
        compiler_params=pltpu.CompilerParams(vmem_limit_bytes=VMEM_LIMIT, dimension_semantics=("arbitrary",)),
        cost_estimate=pl.CostEstimate(flops=18 * 3000 * d * f, bytes_accessed=24 * d * f, transcendentals=3000 * f),
    )(info, x_pool, dy_pool, r_pool, w1, w3, w2s)


def place_kernel(n_fs, n_loc, k, first, me, *refs):
    pieces = refs[:n_fs]
    n_in = n_fs if first else n_fs + 3
    outs, (turned, sem) = refs[n_in:n_in + 3], refs[n_in + 3:]
    copies = []
    for m in range(n_fs):
        to = (me[0] ^ m) * n_loc + k
        copies.append(pltpu.make_async_copy(pieces[m].at[0], outs[0].at[to], sem))
        copies.append(pltpu.make_async_copy(pieces[m].at[1], outs[1].at[to], sem))
    for copy in copies:
        copy.start()
    for m in range(n_fs):
        turned[m] = pieces[m][2].T
        copies.append(pltpu.make_async_copy(turned.at[m], outs[2].at[(me[0] ^ m) * n_loc + k], sem))
        copies[-1].start()
    for copy in copies:
        copy.wait()


def place(k, n_loc, me, pieces, grads):
    n_fs = len(pieces)
    _, dsl, f = pieces[0].shape
    vmem, hbm = pl.BlockSpec(memory_space=pltpu.VMEM), pl.BlockSpec(memory_space=pl.ANY)
    first = grads is None
    shapes = [(n_fs * n_loc, dsl, f)] * 2 + [(n_fs * n_loc, f, dsl)]
    return pl.pallas_call(
        functools.partial(place_kernel, n_fs, n_loc, k, first),
        out_shape=[jax.ShapeDtypeStruct(v, F32) for v in shapes],
        in_specs=[pl.BlockSpec(memory_space=pltpu.SMEM)] + [vmem] * n_fs + ([] if first else [hbm] * 3),
        out_specs=[hbm] * 3,
        scratch_shapes=[pltpu.VMEM((n_fs, f, dsl), F32), pltpu.SemaphoreType.DMA],
        input_output_aliases={} if first else {n_fs + 1 + t: t for t in range(3)},
        compiler_params=pltpu.CompilerParams(vmem_limit_bytes=VMEM_LIMIT),
        cost_estimate=pl.CostEstimate(flops=0, bytes_accessed=6 * 4 * n_fs * dsl * f, transcendentals=0),
    )(me, *pieces, *([] if first else grads))


def combine_kernel(n_src, n_loc, cnt, off, pos_ref, *refs):
    dx_in, dr_in = refs[:n_loc], refs[n_loc:2 * n_loc]
    out, dr_out, hot, stage, pool, rpool, sem = refs[2 * n_loc:]
    s = pl.program_id(0)
    tok = pos_ref.shape[2]
    d = pool.shape[2]

    @pl.when(s == 0)
    def _():
        def copies(k, i):
            at = pl.ds(aligned(i * TILE, TILE), TILE)
            return [pltpu.make_async_copy(dx_in[k].at[at], pool.at[k, at], sem),
                    pltpu.make_async_copy(dr_in[k].at[at], rpool.at[k, at], sem)]

        tiles = []
        for k in range(n_loc):
            last = (n_src - 1) * n_loc + k
            end = off[last] + blocks(cnt[last], 16) * 16
            tiles.append(jnp.maximum(1, blocks(end, TILE)))
        for k in range(n_loc):
            def start(i, carry, k=k):
                for copy in copies(k, i):
                    copy.start()
                return carry

            lax.fori_loop(0, tiles[k], start, 0)
            at = pl.ds(aligned(tiles[k] * TILE), CHUNK)
            pool[k, at, :] = jnp.zeros((CHUNK, d), BF16)
            rpool[k, at, :] = jnp.zeros((CHUNK, 128), F32)
        for k in range(n_loc):
            def wait(i, carry, k=k):
                for copy in copies(k, i):
                    copy.wait()
                return carry

            lax.fori_loop(0, tiles[k], wait, 0)

    dr_out[...] = jnp.zeros_like(dr_out)
    base = jnp.int32(0)
    for k in range(n_loc):
        n = cnt[s * n_loc + k]
        frm = off[s * n_loc + k]
        pos_row = pos_ref[0, k:k + 1, :]

        def build(c, carry, base=base, frm=frm, pos_row=pos_row, k=k):
            m = one_hot_block(pos_row, c)
            at = pl.ds(aligned(base + c * CHUNK), CHUNK)
            src = pl.ds(aligned(frm + c * CHUNK), CHUNK)
            hot[at, :] = jnp.where(m, 1.0, 0.0).astype(BF16)
            stage[at, :] = pool[k, src, :]
            r = jnp.concatenate([rpool[k, src, :]] * (tok // 128), axis=1)
            dr_out[0, k:k + 1, :] += jnp.sum(jnp.where(m, r, 0.0), axis=0, keepdims=True)
            return carry

        lax.fori_loop(0, blocks(n, CHUNK), build, 0)
        base = base + blocks(n, 16) * 16
    tail = pl.ds(aligned(base), MM)
    hot[tail, :] = jnp.zeros((MM, tok), BF16)
    stage[tail, :] = jnp.zeros((MM, d), BF16)
    out[...] = jnp.zeros_like(out)

    def mm(c, carry):
        at = pl.ds(aligned(c * MM), MM)
        out[...] += dot_tn(hot[at, :], stage[at, :])
        return carry

    lax.fori_loop(0, blocks(base, MM), mm, 0)


def combine_rows(cnt, off, pos, dx_pools, dr_pools, region):
    n_src, n_loc, tok = pos.shape
    d = dx_pools[0].shape[1]
    scr = up(n_loc * ((region - TILE) // n_src) + MM, MM)
    hbm = pl.BlockSpec(memory_space=pl.ANY)
    return pl.pallas_call(
        functools.partial(combine_kernel, n_src, n_loc),
        out_shape=[jax.ShapeDtypeStruct((n_src * tok, d), F32), jax.ShapeDtypeStruct((n_src, n_loc, tok), F32)],
        grid_spec=pltpu.PrefetchScalarGridSpec(
            num_scalar_prefetch=2, grid=(n_src,),
            in_specs=[pl.BlockSpec((1, n_loc, tok), lambda s, *_: (s, 0, 0))] + [hbm] * (2 * n_loc),
            out_specs=[pl.BlockSpec((tok, d), lambda s, *_: (s, 0)),
                       pl.BlockSpec((1, n_loc, tok), lambda s, *_: (s, 0, 0))],
            scratch_shapes=[pltpu.VMEM((scr, tok), BF16), pltpu.VMEM((scr, d), BF16),
                            pltpu.VMEM((n_loc, region, d), BF16), pltpu.VMEM((n_loc, region, 128), F32),
                            pltpu.SemaphoreType.DMA]),
        compiler_params=pltpu.CompilerParams(vmem_limit_bytes=VMEM_LIMIT, dimension_semantics=("arbitrary",)),
        cost_estimate=pl.CostEstimate(flops=2 * 12000 * tok * d, bytes_accessed=n_src * tok * d * 4, transcendentals=0),
        name="combine",
    )(cnt, off, pos, *dx_pools, *dr_pools)


def solution(mesh):
    n_ep, n_fs = mesh.shape["ep"], mesh.shape["fsdp"]
    n_dev = n_ep * n_fs
    both = ("fsdp", "ep")
    tok_spec = P(both, None)
    spec_in = P("ep", "fsdp", None)
    spec_out = P("ep", None, "fsdp")

    def body(x_tok, dy_tok, expert_ids, route_w, w_gate, w_up, w_down):
        tok, top_k = expert_ids.shape
        d = x_tok.shape[1]
        exp_local, _, f = w_gate.shape
        n_loc = exp_local // n_fs
        experts = exp_local * n_ep
        capacity = capacity_of(tok, top_k, experts)
        region = n_dev * up(capacity, 16) + TILE

        position, weight = route_tables(expert_ids, route_w, experts, capacity)
        table = jnp.stack([position, weight], axis=1).reshape(n_ep, n_fs, n_loc, 2, tok)
        table = table.transpose(1, 0, 2, 3, 4).reshape(n_dev, n_loc * 2, tok)
        table = lax.all_to_all(table, both, 0, 0, tiled=True).reshape(n_dev, n_loc, 2, tok)
        x_all = lax.all_gather(x_tok, both, axis=0, tiled=True)
        dy_all = lax.all_gather(dy_tok, both, axis=0, tiled=True)

        def to_owner(w):
            return lax.all_to_all(w.reshape(n_fs, n_loc, *w.shape[1:]), "fsdp", 0, 0, tiled=True)

        wg, wu, wd = to_owner(w_gate), to_owner(w_up), to_owner(w_down)

        pos = table[:, :, 0, :].astype(jnp.int32)
        r = table[:, :, 1, :]
        cnt = jnp.max(pos, axis=2) + 1
        padded = blocks(cnt, 16) * 16
        off = jnp.cumsum(padded, axis=0) - padded
        rows = jnp.sum(padded, axis=0)
        cnt_flat, off_flat = cnt.reshape(-1), off.reshape(-1)
        x_pool = gather_rows(x_all, cnt_flat, off_flat, pos, None, region)
        dy_pool, r_pool = gather_rows(dy_all, cnt_flat, off_flat, pos, r, region)

        me = lax.axis_index("fsdp").astype(jnp.int32)
        dx_pools, dr_pools, pieces = [], [], []
        for k in range(n_loc):
            info = jnp.stack([rows[k], jnp.maximum(1, blocks(rows[k], TILE)), me])
            w1, w3, w2s = wg[:, k].reshape(d, f), wu[:, k].reshape(d, f), wd[:, k]
            dxk, drk, *slices = expert_call(k, info, x_pool, dy_pool, r_pool, w1, w3, w2s, region)
            dx_pools.append(dxk)
            dr_pools.append(drk)
            pieces.append([slices[0]] + [lax.ppermute(slices[m], "fsdp", [(i, i ^ m) for i in range(n_fs)])
                                         for m in range(1, n_fs)])
        dx_part, dr_part = combine_rows(cnt_flat, off_flat, pos, dx_pools, dr_pools, region)
        grad_x = lax.psum_scatter(dx_part, both, scatter_dimension=0, tiled=True).astype(BF16)
        dr_home = lax.all_to_all(dr_part, both, 0, 0, tiled=True)
        dr_home = dr_home.reshape(n_fs, n_ep, n_loc, tok).transpose(1, 0, 2, 3).reshape(experts, tok)
        hit = expert_ids.T[:, None, :] == jnp.arange(experts, dtype=jnp.int32)[None, :, None]
        route_grad = jnp.sum(jnp.where(hit, dr_home[None], 0.0), axis=1).T
        grads = None
        for k in range(n_loc):
            grads = place(k, n_loc, me.reshape(1), pieces[k], grads)
        return grad_x, route_grad, *grads

    return jax.shard_map(
        body, mesh=mesh,
        in_specs=(tok_spec, tok_spec, tok_spec, tok_spec, spec_in, spec_in, spec_out),
        out_specs=(tok_spec, tok_spec, spec_in, spec_in, spec_out),
        check_vma=False)
```

```python
import functools

import jax
import jax.numpy as jnp
from jax import lax
from jax.experimental import pallas as pl
from jax.experimental.pallas import tpu as pltpu
from jax.sharding import PartitionSpec as P


CAP_FACTOR = 3
CHUNK = 128
TILE = 512
MM = 256
COPY = 64
VMEM_LIMIT = 60 * 1024 * 1024
F32 = jnp.float32
BF16 = jnp.bfloat16


def capacity_of(tok_dev, top_k, experts):
    return max(8, ((CAP_FACTOR * tok_dev * top_k // experts + 7) // 8) * 8)


def up(n, m):
    return (n + m - 1) // m * m


def blocks(n, size):
    return lax.div(n + (size - 1), jnp.full_like(n, size))


def dot(a, b):
    return lax.dot_general(a, b, (((1,), (0,)), ((), ())), preferred_element_type=F32)


def dot_nt(a, b):
    return lax.dot_general(a, b, (((1,), (1,)), ((), ())), preferred_element_type=F32)


def dot_tn(a, b):
    return lax.dot_general(a, b, (((0,), (0,)), ((), ())), preferred_element_type=F32)


def route_tables(expert_ids, route_w, experts, capacity):
    tok_dev, _ = expert_ids.shape
    ids_t, w_t = expert_ids.T, route_w.T
    hit = ids_t[:, None, :] == jnp.arange(experts, dtype=jnp.int32)[None, :, None]
    chosen = jnp.any(hit, axis=0)
    weight = jnp.sum(jnp.where(hit, w_t[:, None, :], 0.0), axis=0)
    earlier = jnp.arange(tok_dev)[:, None] < jnp.arange(tok_dev)[None, :]
    before = dot(chosen.astype(BF16), earlier.astype(BF16))
    position = jnp.where(chosen & (before < capacity), before, -1.0)
    return position, weight


def one_hot_block(pos_row, c):
    row = lax.broadcasted_iota(jnp.int32, (CHUNK, pos_row.shape[1]), 0) + c * CHUNK
    return row == pos_row


def aligned(v, m=16):
    return pl.multiple_of(v, m)


def gather_kernel(n_src, n_loc, region, with_r, *refs):
    if with_r:
        (cnt, off, pos_ref, r_ref, src_ref, out, r_out, hot, stage, pool, rstage, rpool, sem) = refs
    else:
        (cnt, off, pos_ref, src_ref, out, hot, stage, pool, sem) = refs
    s = pl.program_id(0)
    base = jnp.int32(0)
    starts = []
    for k in range(n_loc):
        n = cnt[s * n_loc + k]
        starts.append(base)
        pos_row = pos_ref[0, k:k + 1, :]

        def build(c, carry, base=base, pos_row=pos_row, k=k):
            m = one_hot_block(pos_row, c)
            at = pl.ds(aligned(base + c * CHUNK), CHUNK)
            hot[at, :] = jnp.where(m, 1.0, 0.0).astype(BF16)
            if with_r:
                r = jnp.sum(jnp.where(m, r_ref[0, k:k + 1, :], 0.0), axis=1, keepdims=True)
                rstage[at, :] = jnp.broadcast_to(r, (CHUNK, 128))
            return carry

        lax.fori_loop(0, blocks(n, CHUNK), build, 0)
        base = base + blocks(n, 16) * 16

    def mm(c, carry):
        at = pl.ds(aligned(c * MM), MM)
        stage[at, :] = dot(hot[at, :], src_ref[...]).astype(BF16)
        return carry

    lax.fori_loop(0, blocks(base, MM), mm, 0)

    for k in range(n_loc):
        n = cnt[s * n_loc + k]
        to = off[s * n_loc + k] + k * region

        def move(c, carry, start=starts[k], to=to):
            dst = pl.ds(aligned(to + c * COPY), COPY)
            frm = pl.ds(aligned(start + c * COPY), COPY)
            pool[dst, :] = stage[frm, :]
            if with_r:
                rpool[dst, :] = rstage[frm, :]
            return carry

        lax.fori_loop(0, blocks(n, COPY), move, 0)

    @pl.when(s == n_src - 1)
    def _():
        def copies(k, i):
            at = pl.ds(aligned(k * region + i * TILE, TILE), TILE)
            made = [pltpu.make_async_copy(pool.at[at], out.at[at], sem)]
            if with_r:
                made.append(pltpu.make_async_copy(rpool.at[at], r_out.at[at], sem))
            return made

        tiles = []
        for k in range(n_loc):
            end = off[s * n_loc + k] + blocks(cnt[s * n_loc + k], 16) * 16
            at = pl.ds(aligned(k * region + end), TILE)
            pool[at, :] = jnp.zeros((TILE, pool.shape[1]), BF16)
            if with_r:
                rpool[at, :] = jnp.zeros((TILE, 128), F32)
            tiles.append(jnp.maximum(1, blocks(end, TILE)))
        for k in range(n_loc):
            def start(i, carry, k=k):
                for copy in copies(k, i):
                    copy.start()
                return carry

            lax.fori_loop(0, tiles[k], start, 0)
        for k in range(n_loc):
            def wait(i, carry, k=k):
                for copy in copies(k, i):
                    copy.wait()
                return carry

            lax.fori_loop(0, tiles[k], wait, 0)


def gather_rows(src, cnt, off, pos, r, region):
    n_src, n_loc, tok = pos.shape
    d = src.shape[1]
    with_r = r is not None
    rows = n_loc * region
    scr = n_loc * ((region - TILE) // n_src) + CHUNK
    scr = up(scr, MM)
    table = pl.BlockSpec((1, n_loc, tok), lambda s, *_: (s, 0, 0))
    in_specs = [table] + ([table] if with_r else []) + [pl.BlockSpec((tok, d), lambda s, *_: (s, 0))]
    out_shape = [jax.ShapeDtypeStruct((rows, d), BF16)]
    scratch = [pltpu.VMEM((scr, tok), BF16), pltpu.VMEM((scr, d), BF16), pltpu.VMEM((rows, d), BF16)]
    if with_r:
        out_shape.append(jax.ShapeDtypeStruct((rows, 128), F32))
        scratch += [pltpu.VMEM((scr, 128), F32), pltpu.VMEM((rows, 128), F32)]
    out = pl.pallas_call(
        functools.partial(gather_kernel, n_src, n_loc, region, with_r),
        out_shape=out_shape,
        grid_spec=pltpu.PrefetchScalarGridSpec(
            num_scalar_prefetch=2, grid=(n_src,), in_specs=in_specs,
            out_specs=[pl.BlockSpec(memory_space=pl.ANY)] * len(out_shape),
            scratch_shapes=scratch + [pltpu.SemaphoreType.DMA]),
        compiler_params=pltpu.CompilerParams(vmem_limit_bytes=VMEM_LIMIT, dimension_semantics=("arbitrary",)),
        cost_estimate=pl.CostEstimate(flops=2 * 12000 * tok * d, bytes_accessed=n_src * tok * d * 4, transcendentals=0),
        name="gather_r" if with_r else "gather_x",
    )(*([cnt, off, pos] + ([r] if with_r else []) + [src]))
    return out if with_r else out[0]


def expert_kernel(n_fs, info, x_ref, dy_ref, r_ref, *refs):
    gu_refs, down_refs, (dx_ref, dr_ref) = refs[:n_fs], refs[n_fs:2 * n_fs], refs[2 * n_fs:2 * n_fs + 2]
    outs, (w1_ref, w3_ref, w2, a_buf, dh1_buf, dh3_buf, dw1, dw3, dw2t) = refs[2 * n_fs + 2:3 * n_fs + 2], refs[3 * n_fs + 2:]
    i = pl.program_id(0)
    d, f = w1_ref.shape
    dsl = d // n_fs

    @pl.when(i == 0)
    def _():
        dw1[...] = jnp.zeros_like(dw1)
        dw3[...] = jnp.zeros_like(dw3)
        dw2t[...] = jnp.zeros_like(dw2t)
        for m in range(n_fs):
            at = pl.ds(aligned((info[2] ^ m) * dsl, dsl), dsl)
            w1_ref[at, :] = gu_refs[m][0]
            w3_ref[at, :] = gu_refs[m][1]
            w2[:, at] = down_refs[m][...]

    def tile(m):
        x, dy = x_ref[:m, :], dy_ref[:m, :]
        dy_wide = dy.astype(F32)
        g = (r_ref[:m, 0:1] * dy_wide).astype(BF16)
        step = 256
        for c in range(0, f, step):
            cs = slice(c, c + step)
            h1 = dot(x, w1_ref[:, cs])
            h3 = dot(x, w3_ref[:, cs])
            da = dot_nt(g, w2[cs, :])
            s = jax.nn.sigmoid(h1)
            hs = h1 * s
            a_buf[:m, cs] = (hs * h3).astype(BF16)
            dh1_buf[:m, cs] = (da * h3 * s * (1.0 + h1 * (1.0 - s))).astype(BF16)
            dh3_buf[:m, cs] = (da * hs).astype(BF16)
        y = dot(a_buf[:m, :], w2[...])
        dr = jnp.sum(dy_wide * y, axis=1, keepdims=True)
        dr_ref[:m, :] = jnp.broadcast_to(dr, (m, 128))
        dx_ref[:m, :] = (dot_nt(dh1_buf[:m, :], w1_ref[...]) + dot_nt(dh3_buf[:m, :], w3_ref[...])).astype(BF16)
        dw1[...] += dot_tn(x, dh1_buf[:m, :])
        dw3[...] += dot_tn(x, dh3_buf[:m, :])
        dw2t[...] += dot_tn(g, a_buf[:m, :])

    left = info[0] - i * TILE

    @pl.when(left > TILE // 2)
    def _():
        tile(TILE)

    @pl.when((i < info[1]) & (left <= TILE // 2))
    def _():
        tile(TILE // 2)
        dx_ref[TILE // 2:, :] = jnp.zeros((TILE // 2, d), BF16)
        dr_ref[TILE // 2:, :] = jnp.zeros((TILE // 2, 128), F32)

    @pl.when(i == info[1] - 1)
    def _():
        for m in range(n_fs):
            at = pl.ds(aligned((info[2] ^ m) * dsl, dsl), dsl)
            for t, acc in enumerate((dw1, dw3, dw2t)):
                outs[m][t] = acc[at, :]


def expert_call(k, info, x_pool, dy_pool, r_pool, gate_up, down, region):
    n_fs, (f, dsl) = len(down), down[0].shape
    d = n_fs * dsl
    first = k * (region // TILE)
    row_map = lambda i, info: (first + jnp.minimum(i, info[1] - 1), 0)
    out_map = lambda i, info: (jnp.minimum(i, info[1] - 1), 0)
    whole = lambda i, info: (0, 0)
    whole3 = lambda i, info: (0, 0, 0)
    return pl.pallas_call(
        functools.partial(expert_kernel, n_fs),
        out_shape=[jax.ShapeDtypeStruct((region, d), BF16), jax.ShapeDtypeStruct((region, 128), F32)]
        + [jax.ShapeDtypeStruct((3, dsl, f), F32)] * n_fs,
        grid_spec=pltpu.PrefetchScalarGridSpec(
            num_scalar_prefetch=1, grid=(region // TILE - 1,),
            in_specs=[pl.BlockSpec((TILE, d), row_map), pl.BlockSpec((TILE, d), row_map), pl.BlockSpec((TILE, 128), row_map),
                      *[pl.BlockSpec((2, dsl, f), whole3)] * n_fs, *[pl.BlockSpec((f, dsl), whole)] * n_fs],
            out_specs=[pl.BlockSpec((TILE, d), out_map), pl.BlockSpec((TILE, 128), out_map)]
            + [pl.BlockSpec((3, dsl, f), whole3)] * n_fs,
            scratch_shapes=[pltpu.VMEM((d, f), BF16)] * 2 + [pltpu.VMEM((f, d), BF16)] + [pltpu.VMEM((TILE, f), BF16)] * 3 + [pltpu.VMEM((d, f), F32)] * 3),
        compiler_params=pltpu.CompilerParams(vmem_limit_bytes=VMEM_LIMIT, dimension_semantics=("arbitrary",)),
        cost_estimate=pl.CostEstimate(flops=18 * 3000 * d * f, bytes_accessed=24 * d * f, transcendentals=3000 * f),
    )(info, x_pool, dy_pool, r_pool, *gate_up, *down)


def place_kernel(n_fs, n_loc, k, first, me, *refs):
    pieces = refs[:n_fs]
    n_in = n_fs if first else n_fs + 3
    outs, (turned, sem) = refs[n_in:n_in + 3], refs[n_in + 3:]
    copies = []
    for m in range(n_fs):
        to = (me[0] ^ m) * n_loc + k
        copies.append(pltpu.make_async_copy(pieces[m].at[0], outs[0].at[to], sem))
        copies.append(pltpu.make_async_copy(pieces[m].at[1], outs[1].at[to], sem))
    for copy in copies:
        copy.start()
    for m in range(n_fs):
        turned[m] = pieces[m][2].T
        copies.append(pltpu.make_async_copy(turned.at[m], outs[2].at[(me[0] ^ m) * n_loc + k], sem))
        copies[-1].start()
    for copy in copies:
        copy.wait()


def place(k, n_loc, me, pieces, grads):
    n_fs = len(pieces)
    _, dsl, f = pieces[0].shape
    vmem, hbm = pl.BlockSpec(memory_space=pltpu.VMEM), pl.BlockSpec(memory_space=pl.ANY)
    first = grads is None
    shapes = [(n_fs * n_loc, dsl, f)] * 2 + [(n_fs * n_loc, f, dsl)]
    return pl.pallas_call(
        functools.partial(place_kernel, n_fs, n_loc, k, first),
        out_shape=[jax.ShapeDtypeStruct(v, F32) for v in shapes],
        in_specs=[pl.BlockSpec(memory_space=pltpu.SMEM)] + [vmem] * n_fs + ([] if first else [hbm] * 3),
        out_specs=[hbm] * 3,
        scratch_shapes=[pltpu.VMEM((n_fs, f, dsl), F32), pltpu.SemaphoreType.DMA],
        input_output_aliases={} if first else {n_fs + 1 + t: t for t in range(3)},
        compiler_params=pltpu.CompilerParams(vmem_limit_bytes=VMEM_LIMIT),
        cost_estimate=pl.CostEstimate(flops=0, bytes_accessed=6 * 4 * n_fs * dsl * f, transcendentals=0),
    )(me, *pieces, *([] if first else grads))


def combine_kernel(n_src, n_loc, cnt, off, pos_ref, *refs):
    dx_in, dr_in = refs[:n_loc], refs[n_loc:2 * n_loc]
    out, dr_out, hot, stage, pool, rpool, sem = refs[2 * n_loc:]
    s = pl.program_id(0)
    tok = pos_ref.shape[2]
    d = pool.shape[2]

    @pl.when(s == 0)
    def _():
        def copies(k, i):
            at = pl.ds(aligned(i * TILE, TILE), TILE)
            return [pltpu.make_async_copy(dx_in[k].at[at], pool.at[k, at], sem),
                    pltpu.make_async_copy(dr_in[k].at[at], rpool.at[k, at], sem)]

        tiles = []
        for k in range(n_loc):
            last = (n_src - 1) * n_loc + k
            end = off[last] + blocks(cnt[last], 16) * 16
            tiles.append(jnp.maximum(1, blocks(end, TILE)))
        for k in range(n_loc):
            def start(i, carry, k=k):
                for copy in copies(k, i):
                    copy.start()
                return carry

            lax.fori_loop(0, tiles[k], start, 0)
            at = pl.ds(aligned(tiles[k] * TILE), CHUNK)
            pool[k, at, :] = jnp.zeros((CHUNK, d), BF16)
            rpool[k, at, :] = jnp.zeros((CHUNK, 128), F32)
        for k in range(n_loc):
            def wait(i, carry, k=k):
                for copy in copies(k, i):
                    copy.wait()
                return carry

            lax.fori_loop(0, tiles[k], wait, 0)

    dr_out[...] = jnp.zeros_like(dr_out)
    base = jnp.int32(0)
    for k in range(n_loc):
        n = cnt[s * n_loc + k]
        frm = off[s * n_loc + k]
        pos_row = pos_ref[0, k:k + 1, :]

        def build(c, carry, base=base, frm=frm, pos_row=pos_row, k=k):
            m = one_hot_block(pos_row, c)
            at = pl.ds(aligned(base + c * CHUNK), CHUNK)
            src = pl.ds(aligned(frm + c * CHUNK), CHUNK)
            hot[at, :] = jnp.where(m, 1.0, 0.0).astype(BF16)
            stage[at, :] = pool[k, src, :]
            r = jnp.concatenate([rpool[k, src, :]] * (tok // 128), axis=1)
            dr_out[0, k:k + 1, :] += jnp.sum(jnp.where(m, r, 0.0), axis=0, keepdims=True)
            return carry

        lax.fori_loop(0, blocks(n, CHUNK), build, 0)
        base = base + blocks(n, 16) * 16
    tail = pl.ds(aligned(base), MM)
    hot[tail, :] = jnp.zeros((MM, tok), BF16)
    stage[tail, :] = jnp.zeros((MM, d), BF16)
    out[...] = jnp.zeros_like(out)

    def mm(c, carry):
        at = pl.ds(aligned(c * MM), MM)
        out[...] += dot_tn(hot[at, :], stage[at, :])
        return carry

    lax.fori_loop(0, blocks(base, MM), mm, 0)


def combine_rows(cnt, off, pos, dx_pools, dr_pools, region):
    n_src, n_loc, tok = pos.shape
    d = dx_pools[0].shape[1]
    scr = up(n_loc * ((region - TILE) // n_src) + MM, MM)
    hbm = pl.BlockSpec(memory_space=pl.ANY)
    return pl.pallas_call(
        functools.partial(combine_kernel, n_src, n_loc),
        out_shape=[jax.ShapeDtypeStruct((n_src * tok, d), F32), jax.ShapeDtypeStruct((n_src, n_loc, tok), F32)],
        grid_spec=pltpu.PrefetchScalarGridSpec(
            num_scalar_prefetch=2, grid=(n_src,),
            in_specs=[pl.BlockSpec((1, n_loc, tok), lambda s, *_: (s, 0, 0))] + [hbm] * (2 * n_loc),
            out_specs=[pl.BlockSpec((tok, d), lambda s, *_: (s, 0)),
                       pl.BlockSpec((1, n_loc, tok), lambda s, *_: (s, 0, 0))],
            scratch_shapes=[pltpu.VMEM((scr, tok), BF16), pltpu.VMEM((scr, d), BF16),
                            pltpu.VMEM((n_loc, region, d), BF16), pltpu.VMEM((n_loc, region, 128), F32),
                            pltpu.SemaphoreType.DMA]),
        compiler_params=pltpu.CompilerParams(vmem_limit_bytes=VMEM_LIMIT, dimension_semantics=("arbitrary",)),
        cost_estimate=pl.CostEstimate(flops=2 * 12000 * tok * d, bytes_accessed=n_src * tok * d * 4, transcendentals=0),
        name="combine",
    )(cnt, off, pos, *dx_pools, *dr_pools)


MESH = pl.DeviceIdType.MESH
HOPS = ((0, 2), (1, 0), (2, 0))
SIBLING = (0, 1)
ORDERS = ((0, 1, 2), (1, 2, 0), (2, 0, 1))


def here():
    return lax.axis_index("fsdp"), lax.axis_index("ep")


def peer_of(hop):
    f, p = here()
    return {"fsdp": f ^ hop[0], "ep": p ^ hop[1]}


def block_of(bits, core=0):
    f, p = here()
    for axis in range(3):
        if bits >> axis & 1:
            f, p = f ^ HOPS[axis][0], p ^ HOPS[axis][1]
    return f * 4 + (p ^ core)


def enter(n_fs, n_ep):
    barrier = pltpu.get_barrier_semaphore()
    for df in range(n_fs):
        for dp in range(n_ep):
            if df or dp:
                pl.semaphore_signal(barrier, inc=1, device_id=peer_of((df, dp)), device_id_type=MESH)
    pl.semaphore_wait(barrier, n_fs * n_ep - 1)


def exchange(n_fs, n_ep, src, dst, send, recv):
    f, p = here()
    copies = []
    for df in range(n_fs):
        for dp in range(n_ep):
            if df or dp:
                n = df * n_ep + dp
                copies.append(pltpu.make_async_remote_copy(
                    src_ref=src.at[(f ^ df) * n_ep + (p ^ dp)], dst_ref=dst.at[f * n_ep + p],
                    send_sem=send.at[n], recv_sem=recv.at[n], device_id=peer_of((df, dp)), device_id_type=MESH))
                copies[-1].start()
    return copies


def spread_kernel(n_fs, n_ep, parts, x_ref, dy_ref, table_ref, x_all, dy_all, table_all,
                  send, recv, c_send, c_recv, t_send, t_recv, own_sem):
    tok = x_ref.shape[0]
    mine = block_of(0)
    enter(n_fs, n_ep)
    pending = []
    local = []
    for n, (src, dst) in enumerate(((x_ref, x_all), (dy_ref, dy_all))):
        local.append(pltpu.make_async_copy(src, dst.at[pl.ds(aligned(mine * tok, tok), tok)], own_sem.at[n]))
    local.append(pltpu.make_async_copy(table_ref.at[mine], table_all.at[mine], own_sem.at[2]))
    for copy in local:
        copy.start()
    pending += exchange(n_fs, n_ep, table_ref, table_all, t_send, t_recv)
    arrays = ((x_ref, x_all), (dy_ref, dy_all))
    starts = [sum(parts[:q]) for q in range(3)]
    sem_at = {}
    inbound = {}

    def send_on(a, q, phase, bits):
        own, full = arrays[a]
        to = pl.ds(aligned(block_of(bits) * tok + starts[q], 16), parts[q])
        src = own.at[pl.ds(starts[q], parts[q])] if bits == 0 else full.at[to]
        n = sem_at.setdefault((a, q, phase, bits), len(sem_at))
        copy = pltpu.make_async_remote_copy(
            src_ref=src, dst_ref=full.at[to], send_sem=send.at[n], recv_sem=recv.at[n],
            device_id=peer_of(HOPS[ORDERS[q][phase]]), device_id_type=MESH)
        copy.start()
        inbound[(a, q, phase, bits)] = copy

    shared = []

    def share(a, q, bits):
        own, full = arrays[a]
        to = pl.ds(aligned(block_of(bits) * tok + starts[q], 16), parts[q])
        src = own.at[pl.ds(starts[q], parts[q])] if bits == 0 else full.at[to]
        n = len(shared)
        copy = pltpu.make_async_remote_copy(
            src_ref=src, dst_ref=full.at[to], send_sem=c_send.at[n], recv_sem=c_recv.at[n],
            device_id=peer_of(SIBLING), device_id_type=MESH)
        copy.start()
        shared.append(copy)

    for phase in range(3):
        for a in range(2):
            for q in range(3):
                send_on(a, q, phase, 0)
    for a in range(2):
        for q in range(3):
            share(a, q, 0)
    for phase in range(3):
        for a in range(2):
            for q in range(3):
                held = [0]
                for axis in ORDERS[q][:phase]:
                    held += [b | 1 << axis for b in held]
                for b in held:
                    inbound[(a, q, phase, b)].wait_recv()
                    got = b | 1 << ORDERS[q][phase]
                    for later in range(phase + 1, 3):
                        send_on(a, q, later, got)
                    share(a, q, got)
    for copy in inbound.values():
        copy.wait_send()
    for copy in shared:
        copy.wait()
    for copy in pending:
        copy.wait()
    for copy in local:
        copy.wait()


def spread(x_tok, dy_tok, table, n_fs, n_ep):
    n_dev = n_fs * n_ep
    tok, d = x_tok.shape
    third = tok // 3 // 16 * 16
    parts = (tok - 2 * third, third, third)
    vmem, hbm = pl.BlockSpec(memory_space=pltpu.VMEM), pl.BlockSpec(memory_space=pl.ANY)
    full = jax.ShapeDtypeStruct((n_dev * tok, d), x_tok.dtype)
    dma = pltpu.SemaphoreType.DMA
    return pl.pallas_call(
        functools.partial(spread_kernel, n_fs, n_ep, parts),
        out_shape=[full, full, jax.ShapeDtypeStruct(table.shape, table.dtype)],
        in_specs=[vmem] * 3, out_specs=[hbm] * 3,
        scratch_shapes=[dma((42,)), dma((42,)), dma((48,)), dma((48,)), dma((n_dev,)), dma((n_dev,)), dma((3,))],
        compiler_params=pltpu.CompilerParams(collective_id=0, has_side_effects=True, vmem_limit_bytes=VMEM_LIMIT),
        cost_estimate=pl.CostEstimate(flops=0, bytes_accessed=8 * n_dev * tok * d, transcendentals=0),
        name="spread",
    )(x_tok, dy_tok, table)


def collect_kernel(n_fs, n_ep, parts, part_ref, dr_ref, gx_ref, dr_home, acc, sib, got,
                   c_send, c_recv, send, recv, t_send, t_recv, own_sem):
    tok = gx_ref.shape[0]
    mine = block_of(0)
    enter(n_fs, n_ep)
    drs = exchange(n_fs, n_ep, dr_ref, dr_home, t_send, t_recv)
    local_dr = pltpu.make_async_copy(dr_ref.at[mine], dr_home.at[mine], own_sem.at[8])
    local_dr.start()
    order = (7, 3, 5, 6, 1, 2, 4, 0)
    loads, shares = {}, {}
    for bits in order:
        theirs = pl.ds(aligned(block_of(bits, 1) * tok, tok), tok)
        shares[bits] = pltpu.make_async_remote_copy(
            src_ref=part_ref.at[theirs], dst_ref=sib.at[bits], send_sem=c_send.at[bits], recv_sem=c_recv.at[bits],
            device_id=peer_of(SIBLING), device_id_type=MESH)
        shares[bits].start()
        ours = pl.ds(aligned(block_of(bits) * tok, tok), tok)
        loads[bits] = pltpu.make_async_copy(part_ref.at[ours], acc.at[bits], own_sem.at[bits])
        loads[bits].start()
    starts = [sum(parts[:q]) for q in range(3)]
    slots = [(q, bits) for q in range(3) for bits in range(1, 8)]
    hops = {}

    def phase_of(q, bits):
        return next(n for n in range(3) if bits >> ORDERS[q][n] & 1)

    def send_off(q, bits):
        n = slots.index((q, bits))
        rows = pl.ds(starts[q], parts[q])
        hops[(q, bits)] = pltpu.make_async_remote_copy(
            src_ref=acc.at[bits, rows], dst_ref=got.at[bits - 1, rows], send_sem=send.at[n], recv_sem=recv.at[n],
            device_id=peer_of(HOPS[ORDERS[q][phase_of(q, bits)]]), device_id_type=MESH)
        hops[(q, bits)].start()

    def add_arrival(q, bits, phase):
        frm = bits | 1 << ORDERS[q][phase]
        hops[(q, frm)].wait_recv()
        rows = slice(starts[q], starts[q] + parts[q])
        acc[bits, rows, :] = acc[bits, rows, :] + got[frm - 1, rows, :]

    for bits in order:
        loads[bits].wait()
        shares[bits].wait_recv()
        acc[bits] = acc[bits] + sib[bits]
        for q in range(3):
            if bits and phase_of(q, bits) == 0:
                send_off(q, bits)
    for phase in (1, 2):
        for q in range(3):
            for bits in range(1, 8):
                if phase_of(q, bits) == phase:
                    for earlier in range(phase):
                        add_arrival(q, bits, earlier)
                    send_off(q, bits)
    for q in range(3):
        for phase in range(3):
            add_arrival(q, 0, phase)
        rows = slice(starts[q], starts[q] + parts[q])
        gx_ref[rows, :] = acc[0, rows, :].astype(gx_ref.dtype)
    for bits in order:
        shares[bits].wait_send()
    for copy in hops.values():
        copy.wait_send()
    for copy in drs:
        copy.wait()
    local_dr.wait()


def collect(dx_part, dr_part, n_fs, n_ep):
    n_dev = n_fs * n_ep
    tok, d = dx_part.shape[0] // n_dev, dx_part.shape[1]
    quarter = tok // 4 // 8 * 8
    parts = (tok - 2 * quarter, quarter, quarter)
    vmem, hbm = pl.BlockSpec(memory_space=pltpu.VMEM), pl.BlockSpec(memory_space=pl.ANY)
    dma = pltpu.SemaphoreType.DMA
    return pl.pallas_call(
        functools.partial(collect_kernel, n_fs, n_ep, parts),
        out_shape=[jax.ShapeDtypeStruct((tok, d), BF16), jax.ShapeDtypeStruct(dr_part.shape, F32)],
        in_specs=[hbm, vmem], out_specs=[vmem, vmem],
        scratch_shapes=[pltpu.VMEM((8, tok, d), F32), pltpu.VMEM((8, tok, d), F32), pltpu.VMEM((7, tok, d), F32),
                        dma((8,)), dma((8,)), dma((21,)), dma((21,)), dma((n_dev,)), dma((n_dev,)), dma((9,))],
        compiler_params=pltpu.CompilerParams(collective_id=1, has_side_effects=True, vmem_limit_bytes=VMEM_LIMIT),
        cost_estimate=pl.CostEstimate(flops=0, bytes_accessed=8 * n_dev * tok * d, transcendentals=0),
        name="collect",
    )(dx_part, dr_part)


def solution(mesh):
    n_ep, n_fs = mesh.shape["ep"], mesh.shape["fsdp"]
    n_dev = n_ep * n_fs
    both = ("fsdp", "ep")
    tok_spec = P(both, None)
    spec_in = P("ep", "fsdp", None)
    spec_out = P("ep", None, "fsdp")

    def body(x_tok, dy_tok, expert_ids, route_w, w_gate, w_up, w_down):
        tok, top_k = expert_ids.shape
        exp_local, _, _ = w_gate.shape
        n_loc = exp_local // n_fs
        experts = exp_local * n_ep
        capacity = capacity_of(tok, top_k, experts)
        region = n_dev * up(capacity, 16) + TILE

        position, weight = route_tables(expert_ids, route_w, experts, capacity)
        table = jnp.stack([position, weight], axis=1).reshape(n_ep, n_fs, n_loc, 2, tok)
        table = table.transpose(1, 0, 2, 3, 4).reshape(n_dev, n_loc * 2, tok)
        x_all, dy_all, table = spread(x_tok, dy_tok, table, n_fs, n_ep)
        table = table.reshape(n_dev, n_loc, 2, tok)
        me = lax.axis_index("fsdp").astype(jnp.int32)

        def to_owners(k):
            gate_up, down = [], []
            for m in range(n_fs):
                at = (me ^ m) * n_loc + k
                gu = jnp.stack([lax.dynamic_index_in_dim(w, at, 0, keepdims=False) for w in (w_gate, w_up)])
                dn = lax.dynamic_index_in_dim(w_down, at, 0, keepdims=False)
                if m:
                    gu, dn = [lax.ppermute(v, "fsdp", [(i, i ^ m) for i in range(n_fs)]) for v in (gu, dn)]
                gate_up.append(gu)
                down.append(dn)
            return gate_up, down

        weights = [to_owners(k) for k in range(n_loc)]

        pos = table[:, :, 0, :].astype(jnp.int32)
        r = table[:, :, 1, :]
        cnt = jnp.max(pos, axis=2) + 1
        padded = blocks(cnt, 16) * 16
        off = jnp.cumsum(padded, axis=0) - padded
        rows = jnp.sum(padded, axis=0)
        cnt_flat, off_flat = cnt.reshape(-1), off.reshape(-1)
        x_pool = gather_rows(x_all, cnt_flat, off_flat, pos, None, region)
        dy_pool, r_pool = gather_rows(dy_all, cnt_flat, off_flat, pos, r, region)

        dx_pools, dr_pools, pieces = [], [], []
        for k in range(n_loc):
            info = jnp.stack([rows[k], jnp.maximum(1, blocks(rows[k], TILE)), me])
            dxk, drk, *slices = expert_call(k, info, x_pool, dy_pool, r_pool, *weights[k], region)
            dx_pools.append(dxk)
            dr_pools.append(drk)
            pieces.append([slices[0]] + [lax.ppermute(slices[m], "fsdp", [(i, i ^ m) for i in range(n_fs)])
                                         for m in range(1, n_fs)])
        dx_part, dr_part = combine_rows(cnt_flat, off_flat, pos, dx_pools, dr_pools, region)
        grad_x, dr_home = collect(dx_part, dr_part, n_fs, n_ep)
        dr_home = dr_home.reshape(n_fs, n_ep, n_loc, tok).transpose(1, 0, 2, 3).reshape(experts, tok)
        hit = expert_ids.T[:, None, :] == jnp.arange(experts, dtype=jnp.int32)[None, :, None]
        route_grad = jnp.sum(jnp.where(hit, dr_home[None], 0.0), axis=1).T
        grads = None
        for k in range(n_loc):
            grads = place(k, n_loc, me.reshape(1), pieces[k], grads)
        return grad_x, route_grad, *grads

    return jax.shard_map(
        body, mesh=mesh,
        in_specs=(tok_spec, tok_spec, tok_spec, tok_spec, spec_in, spec_in, spec_out),
        out_specs=(tok_spec, tok_spec, spec_in, spec_in, spec_out),
        check_vma=False)
```

```python
import functools

import jax
import jax.numpy as jnp
from jax import lax
from jax.experimental import pallas as pl
from jax.experimental.pallas import tpu as pltpu
from jax.sharding import PartitionSpec as P


CAP_FACTOR = 3
CHUNK = 128
TILE = 512
MM = 256
HEAD = 384
VMEM_LIMIT = 60 * 1024 * 1024
F32 = jnp.float32
BF16 = jnp.bfloat16


def capacity_of(tok_dev, top_k, experts):
    return max(8, ((CAP_FACTOR * tok_dev * top_k // experts + 7) // 8) * 8)


def up(n, m):
    return (n + m - 1) // m * m


def blocks(n, size):
    return lax.div(n + (size - 1), jnp.full_like(n, size))


def dot(a, b):
    return lax.dot_general(a, b, (((1,), (0,)), ((), ())), preferred_element_type=F32)


def dot_nt(a, b):
    return lax.dot_general(a, b, (((1,), (1,)), ((), ())), preferred_element_type=F32)


def dot_tn(a, b):
    return lax.dot_general(a, b, (((0,), (0,)), ((), ())), preferred_element_type=F32)


def route_tables(expert_ids, route_w, experts, capacity):
    tok_dev, _ = expert_ids.shape
    ids_t, w_t = expert_ids.T, route_w.T
    hit = ids_t[:, None, :] == jnp.arange(experts, dtype=jnp.int32)[None, :, None]
    chosen = jnp.any(hit, axis=0)
    weight = jnp.sum(jnp.where(hit, w_t[:, None, :], 0.0), axis=0)
    earlier = jnp.arange(tok_dev)[:, None] < jnp.arange(tok_dev)[None, :]
    before = dot(chosen.astype(BF16), earlier.astype(BF16))
    position = jnp.where(chosen & (before < capacity), before, -1.0)
    return position, weight


def one_hot_block(pos_row, c):
    row = lax.broadcasted_iota(jnp.int32, (CHUNK, pos_row.shape[1]), 0) + c * CHUNK
    return row == pos_row


def aligned(v, m=16):
    return pl.multiple_of(v, m)


def gather_kernel(n_src, n_loc, region, with_r, *refs):
    if with_r:
        (cnt, off, pos_ref, r_ref, src_ref, out, r_out, hot, stage, pool, rstage, rpool, sem) = refs
    else:
        (cnt, off, pos_ref, src_ref, out, hot, stage, pool, sem) = refs
    s = pl.program_id(0)
    base = jnp.int32(0)
    starts = []
    for k in range(n_loc):
        n = cnt[s * n_loc + k]
        starts.append(base)
        pos_row = pos_ref[0, k:k + 1, :]

        def build(c, carry=0, base=base, pos_row=pos_row, k=k):
            m = one_hot_block(pos_row, c)
            at = pl.ds(aligned(base + c * CHUNK), CHUNK)
            hot[at, :] = jnp.where(m, 1.0, 0.0).astype(BF16)
            if with_r:
                r = jnp.sum(jnp.where(m, r_ref[0, k:k + 1, :], 0.0), axis=1, keepdims=True)
                rstage[at, :] = jnp.broadcast_to(r, (CHUNK, 128))
            return carry

        build(0)
        lax.fori_loop(1, blocks(n, CHUNK), build, 0)
        base = base + blocks(n, 16) * 16

    head = pl.ds(0, HEAD)
    stage[head, :] = dot(hot[head, :], src_ref[...]).astype(BF16)

    def mm(c, carry):
        at = pl.ds(aligned(HEAD + c * MM), MM)
        stage[at, :] = dot(hot[at, :], src_ref[...]).astype(BF16)
        return carry

    lax.fori_loop(0, blocks(jnp.maximum(base - HEAD, 0), MM), mm, 0)

    for k in range(n_loc):
        n = cnt[s * n_loc + k]
        to = off[s * n_loc + k] + k * region

        def move(c, carry=0, start=starts[k], to=to):
            dst = pl.ds(aligned(to + c * CHUNK), CHUNK)
            frm = pl.ds(aligned(start + c * CHUNK), CHUNK)
            pool[dst, :] = stage[frm, :]
            if with_r:
                rpool[dst, :] = rstage[frm, :]
            return carry

        move(0)
        lax.fori_loop(1, blocks(n, CHUNK), move, 0)

    @pl.when(s == n_src - 1)
    def _():
        def copies(k, i):
            at = pl.ds(aligned(k * region + i * TILE, TILE), TILE)
            made = [pltpu.make_async_copy(pool.at[at], out.at[at], sem)]
            if with_r:
                made.append(pltpu.make_async_copy(rpool.at[at], r_out.at[at], sem))
            return made

        tiles = []
        for k in range(n_loc):
            end = off[s * n_loc + k] + blocks(cnt[s * n_loc + k], 16) * 16
            at = pl.ds(aligned(k * region + end), TILE)
            pool[at, :] = jnp.zeros((TILE, pool.shape[1]), BF16)
            if with_r:
                rpool[at, :] = jnp.zeros((TILE, 128), F32)
            tiles.append(jnp.maximum(1, blocks(end, TILE)))
        for k in range(n_loc):
            def start(i, carry, k=k):
                for copy in copies(k, i):
                    copy.start()
                return carry

            lax.fori_loop(0, tiles[k], start, 0)
        for k in range(n_loc):
            def wait(i, carry, k=k):
                for copy in copies(k, i):
                    copy.wait()
                return carry

            lax.fori_loop(0, tiles[k], wait, 0)


def gather_rows(src, cnt, off, pos, r, region):
    n_src, n_loc, tok = pos.shape
    d = src.shape[1]
    with_r = r is not None
    rows = n_loc * region
    scr = HEAD + up(n_loc * ((region - TILE) // n_src) + CHUNK - HEAD, MM)
    table = pl.BlockSpec((1, n_loc, tok), lambda s, *_: (s, 0, 0))
    in_specs = [table] + ([table] if with_r else []) + [pl.BlockSpec((tok, d), lambda s, *_: (s, 0))]
    out_shape = [jax.ShapeDtypeStruct((rows, d), BF16)]
    scratch = [pltpu.VMEM((scr, tok), BF16), pltpu.VMEM((scr, d), BF16), pltpu.VMEM((rows, d), BF16)]
    if with_r:
        out_shape.append(jax.ShapeDtypeStruct((rows, 128), F32))
        scratch += [pltpu.VMEM((scr, 128), F32), pltpu.VMEM((rows, 128), F32)]
    out = pl.pallas_call(
        functools.partial(gather_kernel, n_src, n_loc, region, with_r),
        out_shape=out_shape,
        grid_spec=pltpu.PrefetchScalarGridSpec(
            num_scalar_prefetch=2, grid=(n_src,), in_specs=in_specs,
            out_specs=[pl.BlockSpec(memory_space=pl.ANY)] * len(out_shape),
            scratch_shapes=scratch + [pltpu.SemaphoreType.DMA]),
        compiler_params=pltpu.CompilerParams(vmem_limit_bytes=VMEM_LIMIT, dimension_semantics=("arbitrary",)),
        cost_estimate=pl.CostEstimate(flops=2 * 12000 * tok * d, bytes_accessed=n_src * tok * d * 4, transcendentals=0),
        name="gather_r" if with_r else "gather_x",
    )(*([cnt, off, pos] + ([r] if with_r else []) + [src]))
    return out if with_r else out[0]


def expert_kernel(n_fs, info, x_ref, dy_ref, r_ref, *refs):
    own, gu_refs, down_refs, refs = refs[:3], refs[3:n_fs + 2], refs[n_fs + 2:2 * n_fs + 1], refs[2 * n_fs + 1:]
    (dx_ref, dr_ref), outs, refs = refs[:2], refs[2:n_fs + 2], refs[n_fs + 2:]
    w1_ref, w3_ref, w2, a_buf, dh1_buf, dh3_buf, dw1, dw3, dw2t = refs
    i = pl.program_id(0)
    d, f = w1_ref.shape
    dsl = d // n_fs

    @pl.when(i == 0)
    def _():
        dw1[...] = jnp.zeros_like(dw1)
        dw3[...] = jnp.zeros_like(dw3)
        dw2t[...] = jnp.zeros_like(dw2t)
        for m in range(n_fs):
            at = pl.ds(aligned((info[2] ^ m) * dsl, dsl), dsl)
            w1_ref[at, :] = gu_refs[m - 1][0] if m else own[0][0]
            w3_ref[at, :] = gu_refs[m - 1][1] if m else own[1][0]
            w2[:, at] = down_refs[m - 1][...] if m else own[2][0]

    def tile(m):
        x, dy = x_ref[:m, :], dy_ref[:m, :]
        dy_wide = dy.astype(F32)
        g = (r_ref[:m, 0:1] * dy_wide).astype(BF16)
        step = 256
        for c in range(0, f, step):
            cs = slice(c, c + step)
            h1 = dot(x, w1_ref[:, cs])
            h3 = dot(x, w3_ref[:, cs])
            da = dot_nt(g, w2[cs, :])
            s = jax.nn.sigmoid(h1)
            hs = h1 * s
            a_buf[:m, cs] = (hs * h3).astype(BF16)
            dh1_buf[:m, cs] = (da * h3 * s * (1.0 + h1 * (1.0 - s))).astype(BF16)
            dh3_buf[:m, cs] = (da * hs).astype(BF16)
        y = dot(a_buf[:m, :], w2[...])
        dr = jnp.sum(dy_wide * y, axis=1, keepdims=True)
        dr_ref[:m, :] = jnp.broadcast_to(dr, (m, 128))
        dx_ref[:m, :] = (dot_nt(dh1_buf[:m, :], w1_ref[...]) + dot_nt(dh3_buf[:m, :], w3_ref[...])).astype(BF16)
        dw1[...] += dot_tn(x, dh1_buf[:m, :])
        dw3[...] += dot_tn(x, dh3_buf[:m, :])
        dw2t[...] += dot_tn(g, a_buf[:m, :])

    left = info[0] - i * TILE

    @pl.when(left > TILE // 2)
    def _():
        tile(TILE)

    @pl.when((i < info[1]) & (left <= TILE // 2))
    def _():
        tile(TILE // 2)
        dx_ref[TILE // 2:, :] = jnp.zeros((TILE // 2, d), BF16)
        dr_ref[TILE // 2:, :] = jnp.zeros((TILE // 2, 128), F32)

    @pl.when(i == info[1] - 1)
    def _():
        for m in range(n_fs):
            at = pl.ds(aligned((info[2] ^ m) * dsl, dsl), dsl)
            for t, acc in enumerate((dw1, dw3, dw2t)):
                outs[m][t] = acc[at, :]


def expert_call(k, n_loc, info, x_pool, dy_pool, r_pool, own, gate_up, down, region):
    n_fs, (f, dsl) = len(down) + 1, down[0].shape
    d = n_fs * dsl
    first = k * (region // TILE)
    row_map = lambda i, info: (first + jnp.minimum(i, info[1] - 1), 0)
    out_map = lambda i, info: (jnp.minimum(i, info[1] - 1), 0)
    whole = lambda i, info: (0, 0)
    whole3 = lambda i, info: (0, 0, 0)
    mine = lambda i, info: (info[2] * n_loc + k, 0, 0)
    return pl.pallas_call(
        functools.partial(expert_kernel, n_fs),
        out_shape=[jax.ShapeDtypeStruct((region, d), BF16), jax.ShapeDtypeStruct((region, 128), F32)]
        + [jax.ShapeDtypeStruct((3, dsl, f), F32)] * n_fs,
        grid_spec=pltpu.PrefetchScalarGridSpec(
            num_scalar_prefetch=1, grid=(region // TILE - 1,),
            in_specs=[pl.BlockSpec((TILE, d), row_map), pl.BlockSpec((TILE, d), row_map), pl.BlockSpec((TILE, 128), row_map),
                      *[pl.BlockSpec((1, dsl, f), mine)] * 2, pl.BlockSpec((1, f, dsl), mine),
                      *[pl.BlockSpec((2, dsl, f), whole3)] * (n_fs - 1), *[pl.BlockSpec((f, dsl), whole)] * (n_fs - 1)],
            out_specs=[pl.BlockSpec((TILE, d), out_map), pl.BlockSpec((TILE, 128), out_map)]
            + [pl.BlockSpec((3, dsl, f), whole3)] * n_fs,
            scratch_shapes=[pltpu.VMEM((d, f), BF16)] * 2 + [pltpu.VMEM((f, d), BF16)] + [pltpu.VMEM((TILE, f), BF16)] * 3 + [pltpu.VMEM((d, f), F32)] * 3),
        compiler_params=pltpu.CompilerParams(vmem_limit_bytes=VMEM_LIMIT, dimension_semantics=("arbitrary",)),
        cost_estimate=pl.CostEstimate(flops=18 * 3000 * d * f, bytes_accessed=24 * d * f, transcendentals=3000 * f),
    )(info, x_pool, dy_pool, r_pool, *own, *gate_up, *down)


def place_kernel(n_fs, n_loc, k, first, me, *refs):
    pieces = refs[:n_fs]
    n_in = n_fs if first else n_fs + 3
    outs, (turned, sem) = refs[n_in:n_in + 3], refs[n_in + 3:]
    copies = []
    for m in range(n_fs):
        to = (me[0] ^ m) * n_loc + k
        copies.append(pltpu.make_async_copy(pieces[m].at[0], outs[0].at[to], sem))
        copies.append(pltpu.make_async_copy(pieces[m].at[1], outs[1].at[to], sem))
    for copy in copies:
        copy.start()
    for m in range(n_fs):
        turned[m] = pieces[m][2].T
        copies.append(pltpu.make_async_copy(turned.at[m], outs[2].at[(me[0] ^ m) * n_loc + k], sem))
        copies[-1].start()
    for copy in copies:
        copy.wait()


def place(k, n_loc, me, pieces, grads):
    n_fs = len(pieces)
    _, dsl, f = pieces[0].shape
    vmem, hbm = pl.BlockSpec(memory_space=pltpu.VMEM), pl.BlockSpec(memory_space=pl.ANY)
    first = grads is None
    shapes = [(n_fs * n_loc, dsl, f)] * 2 + [(n_fs * n_loc, f, dsl)]
    return pl.pallas_call(
        functools.partial(place_kernel, n_fs, n_loc, k, first),
        out_shape=[jax.ShapeDtypeStruct(v, F32) for v in shapes],
        in_specs=[pl.BlockSpec(memory_space=pltpu.SMEM)] + [vmem] * n_fs + ([] if first else [hbm] * 3),
        out_specs=[hbm] * 3,
        scratch_shapes=[pltpu.VMEM((n_fs, f, dsl), F32), pltpu.SemaphoreType.DMA],
        input_output_aliases={} if first else {n_fs + 1 + t: t for t in range(3)},
        compiler_params=pltpu.CompilerParams(vmem_limit_bytes=VMEM_LIMIT),
        cost_estimate=pl.CostEstimate(flops=0, bytes_accessed=6 * 4 * n_fs * dsl * f, transcendentals=0),
    )(me, *pieces, *([] if first else grads))


def combine_kernel(n_src, n_loc, cnt, off, pos_ref, *refs):
    dx_in, dr_in = refs[:n_loc], refs[n_loc:2 * n_loc]
    out, dr_out, hot, stage, pool, rpool, sem = refs[2 * n_loc:]
    s = pl.program_id(0)
    tok = pos_ref.shape[2]
    d = pool.shape[2]

    @pl.when(s == 0)
    def _():
        def copies(k, i):
            at = pl.ds(aligned(i * TILE, TILE), TILE)
            return [pltpu.make_async_copy(dx_in[k].at[at], pool.at[k, at], sem),
                    pltpu.make_async_copy(dr_in[k].at[at], rpool.at[k, at], sem)]

        tiles = []
        for k in range(n_loc):
            last = (n_src - 1) * n_loc + k
            end = off[last] + blocks(cnt[last], 16) * 16
            tiles.append(jnp.maximum(1, blocks(end, TILE)))
        for k in range(n_loc):
            def start(i, carry, k=k):
                for copy in copies(k, i):
                    copy.start()
                return carry

            lax.fori_loop(0, tiles[k], start, 0)
            at = pl.ds(aligned(tiles[k] * TILE), CHUNK)
            pool[k, at, :] = jnp.zeros((CHUNK, d), BF16)
            rpool[k, at, :] = jnp.zeros((CHUNK, 128), F32)
        for k in range(n_loc):
            def wait(i, carry, k=k):
                for copy in copies(k, i):
                    copy.wait()
                return carry

            lax.fori_loop(0, tiles[k], wait, 0)

    dr_out[...] = jnp.zeros_like(dr_out)
    base = jnp.int32(0)
    for k in range(n_loc):
        n = cnt[s * n_loc + k]
        frm = off[s * n_loc + k]
        pos_row = pos_ref[0, k:k + 1, :]

        def build(c, carry=0, base=base, frm=frm, pos_row=pos_row, k=k):
            m = one_hot_block(pos_row, c)
            at = pl.ds(aligned(base + c * CHUNK), CHUNK)
            src = pl.ds(aligned(frm + c * CHUNK), CHUNK)
            hot[at, :] = jnp.where(m, 1.0, 0.0).astype(BF16)
            stage[at, :] = pool[k, src, :]
            r = jnp.concatenate([rpool[k, src, :]] * (tok // 128), axis=1)
            dr_out[0, k:k + 1, :] += jnp.sum(jnp.where(m, r, 0.0), axis=0, keepdims=True)
            return carry

        build(0)
        lax.fori_loop(1, blocks(n, CHUNK), build, 0)
        base = base + blocks(n, 16) * 16
    tail = pl.ds(aligned(base), HEAD)
    hot[tail, :] = jnp.zeros((HEAD, tok), BF16)
    stage[tail, :] = jnp.zeros((HEAD, d), BF16)
    head = pl.ds(0, HEAD)
    out[...] = dot_tn(hot[head, :], stage[head, :])

    def mm(c, carry):
        at = pl.ds(aligned(HEAD + c * MM), MM)
        out[...] += dot_tn(hot[at, :], stage[at, :])
        return carry

    lax.fori_loop(0, blocks(jnp.maximum(base - HEAD, 0), MM), mm, 0)


def combine_rows(cnt, off, pos, dx_pools, dr_pools, region):
    n_src, n_loc, tok = pos.shape
    d = dx_pools[0].shape[1]
    scr = n_loc * ((region - TILE) // n_src) + HEAD
    hbm = pl.BlockSpec(memory_space=pl.ANY)
    return pl.pallas_call(
        functools.partial(combine_kernel, n_src, n_loc),
        out_shape=[jax.ShapeDtypeStruct((n_src * tok, d), F32), jax.ShapeDtypeStruct((n_src, n_loc, tok), F32)],
        grid_spec=pltpu.PrefetchScalarGridSpec(
            num_scalar_prefetch=2, grid=(n_src,),
            in_specs=[pl.BlockSpec((1, n_loc, tok), lambda s, *_: (s, 0, 0))] + [hbm] * (2 * n_loc),
            out_specs=[pl.BlockSpec((tok, d), lambda s, *_: (s, 0)),
                       pl.BlockSpec((1, n_loc, tok), lambda s, *_: (s, 0, 0))],
            scratch_shapes=[pltpu.VMEM((scr, tok), BF16), pltpu.VMEM((scr, d), BF16),
                            pltpu.VMEM((n_loc, region, d), BF16), pltpu.VMEM((n_loc, region, 128), F32),
                            pltpu.SemaphoreType.DMA]),
        compiler_params=pltpu.CompilerParams(vmem_limit_bytes=VMEM_LIMIT, dimension_semantics=("arbitrary",)),
        cost_estimate=pl.CostEstimate(flops=2 * 12000 * tok * d, bytes_accessed=n_src * tok * d * 4, transcendentals=0),
        name="combine",
    )(cnt, off, pos, *dx_pools, *dr_pools)


MESH = pl.DeviceIdType.MESH
HOPS = ((0, 2), (1, 0), (2, 0))
SIBLING = (0, 1)
ORDERS = ((0, 1, 2), (1, 2, 0), (2, 0, 1))


def here():
    return lax.axis_index("fsdp"), lax.axis_index("ep")


def peer_of(hop):
    f, p = here()
    return {"fsdp": f ^ hop[0], "ep": p ^ hop[1]}


def block_of(bits, core=0):
    f, p = here()
    for axis in range(3):
        if bits >> axis & 1:
            f, p = f ^ HOPS[axis][0], p ^ HOPS[axis][1]
    return f * 4 + (p ^ core)


def enter(n_fs, n_ep):
    barrier = pltpu.get_barrier_semaphore()
    for df in range(n_fs):
        for dp in range(n_ep):
            if df or dp:
                pl.semaphore_signal(barrier, inc=1, device_id=peer_of((df, dp)), device_id_type=MESH)
    pl.semaphore_wait(barrier, n_fs * n_ep - 1)


def exchange(n_fs, n_ep, src, dst, send, recv):
    f, p = here()
    copies = []
    for df in range(n_fs):
        for dp in range(n_ep):
            if df or dp:
                n = df * n_ep + dp
                copies.append(pltpu.make_async_remote_copy(
                    src_ref=src.at[(f ^ df) * n_ep + (p ^ dp)], dst_ref=dst.at[f * n_ep + p],
                    send_sem=send.at[n], recv_sem=recv.at[n], device_id=peer_of((df, dp)), device_id_type=MESH))
                copies[-1].start()
    return copies


def spread_kernel(n_fs, n_ep, n_loc, parts, x_ref, dy_ref, table_ref, wg_ref, wu_ref, wd_ref, x_all, dy_all, table_all, *refs):
    n_out = n_loc * (n_fs - 1)
    gu_out, down_out, refs = refs[:n_out], refs[n_out:2 * n_out], refs[2 * n_out:]
    send, recv, c_send, c_recv, t_send, t_recv, own_sem, gu_buf, down_buf, in_sem, out_sem = refs
    tok = x_ref.shape[0]
    mine = block_of(0)
    enter(n_fs, n_ep)
    pending = []
    local = []
    for n, (src, dst) in enumerate(((x_ref, x_all), (dy_ref, dy_all))):
        local.append(pltpu.make_async_copy(src, dst.at[pl.ds(aligned(mine * tok, tok), tok)], own_sem.at[n]))
    local.append(pltpu.make_async_copy(table_ref.at[mine], table_all.at[mine], own_sem.at[2]))
    for copy in local:
        copy.start()
    pending += exchange(n_fs, n_ep, table_ref, table_all, t_send, t_recv)
    arrays = ((x_ref, x_all), (dy_ref, dy_all))
    starts = [sum(parts[:q]) for q in range(3)]
    sem_at = {}
    inbound = {}

    def send_on(a, q, phase, bits):
        own, full = arrays[a]
        to = pl.ds(aligned(block_of(bits) * tok + starts[q], 16), parts[q])
        src = own.at[pl.ds(starts[q], parts[q])] if bits == 0 else full.at[to]
        n = sem_at.setdefault((a, q, phase, bits), len(sem_at))
        copy = pltpu.make_async_remote_copy(
            src_ref=src, dst_ref=full.at[to], send_sem=send.at[n], recv_sem=recv.at[n],
            device_id=peer_of(HOPS[ORDERS[q][phase]]), device_id_type=MESH)
        copy.start()
        inbound[(a, q, phase, bits)] = copy

    shared = []

    def share(a, q, bits):
        own, full = arrays[a]
        to = pl.ds(aligned(block_of(bits) * tok + starts[q], 16), parts[q])
        src = own.at[pl.ds(starts[q], parts[q])] if bits == 0 else full.at[to]
        n = len(shared)
        copy = pltpu.make_async_remote_copy(
            src_ref=src, dst_ref=full.at[to], send_sem=c_send.at[n], recv_sem=c_recv.at[n],
            device_id=peer_of(SIBLING), device_id_type=MESH)
        copy.start()
        shared.append(copy)

    for phase in range(3):
        for a in range(2):
            for q in range(3):
                send_on(a, q, phase, 0)
    for a in range(2):
        for q in range(3):
            share(a, q, 0)
    f, _ = here()
    packs = []
    for k in range(n_loc):
        for m in range(1, n_fs):
            n = k * (n_fs - 1) + m - 1
            at = (f ^ m) * n_loc + k
            packs.append([pltpu.make_async_copy(wg_ref.at[at], gu_buf.at[n, 0], in_sem.at[3 * n]),
                          pltpu.make_async_copy(wu_ref.at[at], gu_buf.at[n, 1], in_sem.at[3 * n + 1]),
                          pltpu.make_async_copy(wd_ref.at[at], down_buf.at[n], in_sem.at[3 * n + 2])])
            for copy in packs[-1]:
                copy.start()
    for n in range(n_out):
        for copy in packs[n]:
            copy.wait()
        for copy in (pltpu.make_async_copy(gu_buf.at[n], gu_out[n], out_sem.at[2 * n]),
                     pltpu.make_async_copy(down_buf.at[n], down_out[n], out_sem.at[2 * n + 1])):
            copy.start()
            local.append(copy)
    for phase in range(3):
        for a in range(2):
            for q in range(3):
                held = [0]
                for axis in ORDERS[q][:phase]:
                    held += [b | 1 << axis for b in held]
                for b in held:
                    inbound[(a, q, phase, b)].wait_recv()
                    got = b | 1 << ORDERS[q][phase]
                    for later in range(phase + 1, 3):
                        send_on(a, q, later, got)
                    share(a, q, got)
    for copy in inbound.values():
        copy.wait_send()
    for copy in shared:
        copy.wait()
    for copy in pending:
        copy.wait()
    for copy in local:
        copy.wait()


def spread(x_tok, dy_tok, table, w_gate, w_up, w_down, n_fs, n_ep):
    n_dev = n_fs * n_ep
    tok, d = x_tok.shape
    exp_local, dsl, f = w_gate.shape
    n_loc = exp_local // n_fs
    n_out = n_loc * (n_fs - 1)
    third = tok // 3 // 16 * 16
    parts = (tok - 2 * third, third, third)
    vmem, hbm = pl.BlockSpec(memory_space=pltpu.VMEM), pl.BlockSpec(memory_space=pl.ANY)
    full = jax.ShapeDtypeStruct((n_dev * tok, d), x_tok.dtype)
    dma = pltpu.SemaphoreType.DMA
    return pl.pallas_call(
        functools.partial(spread_kernel, n_fs, n_ep, n_loc, parts),
        out_shape=[full, full, jax.ShapeDtypeStruct(table.shape, table.dtype)]
        + [jax.ShapeDtypeStruct((2, dsl, f), BF16)] * n_out + [jax.ShapeDtypeStruct((f, dsl), BF16)] * n_out,
        in_specs=[vmem] * 3 + [hbm] * 3, out_specs=[hbm] * (3 + 2 * n_out),
        scratch_shapes=[dma((42,)), dma((42,)), dma((48,)), dma((48,)), dma((n_dev,)), dma((n_dev,)), dma((3,)),
                        pltpu.VMEM((n_out, 2, dsl, f), BF16), pltpu.VMEM((n_out, f, dsl), BF16), dma((3 * n_out,)), dma((2 * n_out,))],
        compiler_params=pltpu.CompilerParams(collective_id=0, has_side_effects=True, vmem_limit_bytes=VMEM_LIMIT),
        cost_estimate=pl.CostEstimate(flops=0, bytes_accessed=8 * n_dev * tok * d, transcendentals=0),
        name="spread",
    )(x_tok, dy_tok, table, w_gate, w_up, w_down)


def collect_kernel(n_fs, n_ep, parts, part_ref, dr_ref, gx_ref, dr_home, acc, sib, got,
                   c_send, c_recv, send, recv, t_send, t_recv, own_sem):
    tok = gx_ref.shape[0]
    mine = block_of(0)
    enter(n_fs, n_ep)
    drs = exchange(n_fs, n_ep, dr_ref, dr_home, t_send, t_recv)
    local_dr = pltpu.make_async_copy(dr_ref.at[mine], dr_home.at[mine], own_sem.at[8])
    local_dr.start()
    order = (7, 3, 5, 6, 1, 2, 4, 0)
    loads, shares = {}, {}
    for bits in order:
        theirs = pl.ds(aligned(block_of(bits, 1) * tok, tok), tok)
        shares[bits] = pltpu.make_async_remote_copy(
            src_ref=part_ref.at[theirs], dst_ref=sib.at[bits], send_sem=c_send.at[bits], recv_sem=c_recv.at[bits],
            device_id=peer_of(SIBLING), device_id_type=MESH)
        shares[bits].start()
        ours = pl.ds(aligned(block_of(bits) * tok, tok), tok)
        loads[bits] = pltpu.make_async_copy(part_ref.at[ours], acc.at[bits], own_sem.at[bits])
        loads[bits].start()
    starts = [sum(parts[:q]) for q in range(3)]
    slots = [(q, bits) for q in range(3) for bits in range(1, 8)]
    hops = {}

    def phase_of(q, bits):
        return next(n for n in range(3) if bits >> ORDERS[q][n] & 1)

    def send_off(q, bits):
        n = slots.index((q, bits))
        rows = pl.ds(starts[q], parts[q])
        hops[(q, bits)] = pltpu.make_async_remote_copy(
            src_ref=acc.at[bits, rows], dst_ref=got.at[bits - 1, rows], send_sem=send.at[n], recv_sem=recv.at[n],
            device_id=peer_of(HOPS[ORDERS[q][phase_of(q, bits)]]), device_id_type=MESH)
        hops[(q, bits)].start()

    def add_arrival(q, bits, phase):
        frm = bits | 1 << ORDERS[q][phase]
        hops[(q, frm)].wait_recv()
        rows = slice(starts[q], starts[q] + parts[q])
        acc[bits, rows, :] = acc[bits, rows, :] + got[frm - 1, rows, :]

    for bits in order:
        loads[bits].wait()
        shares[bits].wait_recv()
        acc[bits] = acc[bits] + sib[bits]
        for q in range(3):
            if bits and phase_of(q, bits) == 0:
                send_off(q, bits)
    for phase in (1, 2):
        for q in range(3):
            for bits in range(1, 8):
                if phase_of(q, bits) == phase:
                    for earlier in range(phase):
                        add_arrival(q, bits, earlier)
                    send_off(q, bits)
    for q in range(3):
        for phase in range(3):
            add_arrival(q, 0, phase)
        rows = slice(starts[q], starts[q] + parts[q])
        gx_ref[rows, :] = acc[0, rows, :].astype(gx_ref.dtype)
    for bits in order:
        shares[bits].wait_send()
    for copy in hops.values():
        copy.wait_send()
    for copy in drs:
        copy.wait()
    local_dr.wait()


def collect(dx_part, dr_part, n_fs, n_ep):
    n_dev = n_fs * n_ep
    tok, d = dx_part.shape[0] // n_dev, dx_part.shape[1]
    quarter = tok // 4 // 8 * 8
    parts = (tok - 2 * quarter, quarter, quarter)
    vmem, hbm = pl.BlockSpec(memory_space=pltpu.VMEM), pl.BlockSpec(memory_space=pl.ANY)
    dma = pltpu.SemaphoreType.DMA
    return pl.pallas_call(
        functools.partial(collect_kernel, n_fs, n_ep, parts),
        out_shape=[jax.ShapeDtypeStruct((tok, d), BF16), jax.ShapeDtypeStruct(dr_part.shape, F32)],
        in_specs=[hbm, vmem], out_specs=[vmem, vmem],
        scratch_shapes=[pltpu.VMEM((8, tok, d), F32), pltpu.VMEM((8, tok, d), F32), pltpu.VMEM((7, tok, d), F32),
                        dma((8,)), dma((8,)), dma((21,)), dma((21,)), dma((n_dev,)), dma((n_dev,)), dma((9,))],
        compiler_params=pltpu.CompilerParams(collective_id=1, has_side_effects=True, vmem_limit_bytes=VMEM_LIMIT),
        cost_estimate=pl.CostEstimate(flops=0, bytes_accessed=8 * n_dev * tok * d, transcendentals=0),
        name="collect",
    )(dx_part, dr_part)


def solution(mesh):
    n_ep, n_fs = mesh.shape["ep"], mesh.shape["fsdp"]
    n_dev = n_ep * n_fs
    both = ("fsdp", "ep")
    tok_spec = P(both, None)
    spec_in = P("ep", "fsdp", None)
    spec_out = P("ep", None, "fsdp")

    def body(x_tok, dy_tok, expert_ids, route_w, w_gate, w_up, w_down):
        tok, top_k = expert_ids.shape
        exp_local, _, _ = w_gate.shape
        n_loc = exp_local // n_fs
        experts = exp_local * n_ep
        capacity = capacity_of(tok, top_k, experts)
        region = n_dev * up(capacity, 16) + TILE

        position, weight = route_tables(expert_ids, route_w, experts, capacity)
        table = jnp.stack([position, weight], axis=1).reshape(n_ep, n_fs, n_loc, 2, tok)
        table = table.transpose(1, 0, 2, 3, 4).reshape(n_dev, n_loc * 2, tok)
        x_all, dy_all, table, *packed = spread(x_tok, dy_tok, table, w_gate, w_up, w_down, n_fs, n_ep)
        table = table.reshape(n_dev, n_loc, 2, tok)
        me = lax.axis_index("fsdp").astype(jnp.int32)
        weights = []
        for k in range(n_loc):
            slices = []
            for kind in range(2):
                at = (kind * n_loc + k) * (n_fs - 1)
                slices.append([lax.ppermute(packed[at + m - 1], "fsdp", [(i, i ^ m) for i in range(n_fs)])
                               for m in range(1, n_fs)])
            weights.append(slices)

        pos = table[:, :, 0, :].astype(jnp.int32)
        r = table[:, :, 1, :]
        cnt = jnp.max(pos, axis=2) + 1
        padded = blocks(cnt, 16) * 16
        off = jnp.cumsum(padded, axis=0) - padded
        rows = jnp.sum(padded, axis=0)
        cnt_flat, off_flat = cnt.reshape(-1), off.reshape(-1)
        x_pool = gather_rows(x_all, cnt_flat, off_flat, pos, None, region)
        dy_pool, r_pool = gather_rows(dy_all, cnt_flat, off_flat, pos, r, region)

        dx_pools, dr_pools, pieces = [], [], []
        for k in range(n_loc):
            info = jnp.stack([rows[k], jnp.maximum(1, blocks(rows[k], TILE)), me])
            dxk, drk, *slices = expert_call(
                k, n_loc, info, x_pool, dy_pool, r_pool, (w_gate, w_up, w_down), *weights[k], region)
            dx_pools.append(dxk)
            dr_pools.append(drk)
            pieces.append([slices[0]] + [lax.ppermute(slices[m], "fsdp", [(i, i ^ m) for i in range(n_fs)])
                                         for m in range(1, n_fs)])
        dx_part, dr_part = combine_rows(cnt_flat, off_flat, pos, dx_pools, dr_pools, region)
        grad_x, dr_home = collect(dx_part, dr_part, n_fs, n_ep)
        dr_home = dr_home.reshape(n_fs, n_ep, n_loc, tok).transpose(1, 0, 2, 3).reshape(experts, tok)
        hit = expert_ids.T[:, None, :] == jnp.arange(experts, dtype=jnp.int32)[None, :, None]
        route_grad = jnp.sum(jnp.where(hit, dr_home[None], 0.0), axis=1).T
        grads = None
        for k in range(n_loc):
            grads = place(k, n_loc, me.reshape(1), pieces[k], grads)
        return grad_x, route_grad, *grads

    return jax.shard_map(
        body, mesh=mesh,
        in_specs=(tok_spec, tok_spec, tok_spec, tok_spec, spec_in, spec_in, spec_out),
        out_specs=(tok_spec, tok_spec, spec_in, spec_in, spec_out),
        check_vma=False)
```

```python
import functools

import jax
import jax.numpy as jnp
from jax import lax
from jax.experimental import pallas as pl
from jax.experimental.pallas import tpu as pltpu
from jax.sharding import PartitionSpec as P


CAP_FACTOR = 3
CHUNK = 128
TILE = 512
MM = 256
HEAD = 384
VMEM_LIMIT = 60 * 1024 * 1024
F32 = jnp.float32
BF16 = jnp.bfloat16


def capacity_of(tok_dev, top_k, experts):
    return max(8, ((CAP_FACTOR * tok_dev * top_k // experts + 7) // 8) * 8)


def up(n, m):
    return (n + m - 1) // m * m


def blocks(n, size):
    return lax.div(n + (size - 1), jnp.full_like(n, size))


def dot(a, b):
    return lax.dot_general(a, b, (((1,), (0,)), ((), ())), preferred_element_type=F32)


def dot_nt(a, b):
    return lax.dot_general(a, b, (((1,), (1,)), ((), ())), preferred_element_type=F32)


def dot_tn(a, b):
    return lax.dot_general(a, b, (((0,), (0,)), ((), ())), preferred_element_type=F32)


def route_tables(expert_ids, route_w, experts, capacity):
    tok_dev, _ = expert_ids.shape
    ids_t, w_t = expert_ids.T, route_w.T
    hit = ids_t[:, None, :] == jnp.arange(experts, dtype=jnp.int32)[None, :, None]
    chosen = jnp.any(hit, axis=0)
    weight = jnp.sum(jnp.where(hit, w_t[:, None, :], 0.0), axis=0)
    earlier = jnp.arange(tok_dev)[:, None] < jnp.arange(tok_dev)[None, :]
    before = dot(chosen.astype(BF16), earlier.astype(BF16))
    position = jnp.where(chosen & (before < capacity), before, -1.0)
    return position, weight


def one_hot_block(pos_row, c):
    row = lax.broadcasted_iota(jnp.int32, (CHUNK, pos_row.shape[1]), 0) + c * CHUNK
    return row == pos_row


def aligned(v, m=16):
    return pl.multiple_of(v, m)


def gather_kernel(n_src, n_loc, region, with_r, *refs):
    if with_r:
        (cnt, off, pos_ref, r_ref, src_ref, out, r_out, hot, stage, pool, rstage, rpool, sem) = refs
    else:
        (cnt, off, pos_ref, src_ref, out, hot, stage, pool, sem) = refs
    s = pl.program_id(0)
    base = jnp.int32(0)
    starts = []
    for k in range(n_loc):
        n = cnt[s * n_loc + k]
        starts.append(base)
        pos_row = pos_ref[0, k:k + 1, :]

        def build(c, carry=0, base=base, pos_row=pos_row, k=k):
            m = one_hot_block(pos_row, c)
            at = pl.ds(aligned(base + c * CHUNK), CHUNK)
            hot[at, :] = jnp.where(m, 1.0, 0.0).astype(BF16)
            if with_r:
                r = jnp.sum(jnp.where(m, r_ref[0, k:k + 1, :], 0.0), axis=1, keepdims=True)
                rstage[at, :] = jnp.broadcast_to(r, (CHUNK, 128))
            return carry

        build(0)
        lax.fori_loop(1, blocks(n, CHUNK), build, 0)
        base = base + blocks(n, 16) * 16

    head = pl.ds(0, HEAD)
    stage[head, :] = dot(hot[head, :], src_ref[...]).astype(BF16)

    def mm(c, carry):
        at = pl.ds(aligned(HEAD + c * MM), MM)
        stage[at, :] = dot(hot[at, :], src_ref[...]).astype(BF16)
        return carry

    lax.fori_loop(0, blocks(jnp.maximum(base - HEAD, 0), MM), mm, 0)

    for k in range(n_loc):
        n = cnt[s * n_loc + k]
        to = off[s * n_loc + k] + k * region

        def move(c, carry=0, start=starts[k], to=to):
            dst = pl.ds(aligned(to + c * CHUNK), CHUNK)
            frm = pl.ds(aligned(start + c * CHUNK), CHUNK)
            pool[dst, :] = stage[frm, :]
            if with_r:
                rpool[dst, :] = rstage[frm, :]
            return carry

        move(0)
        lax.fori_loop(1, blocks(n, CHUNK), move, 0)

    @pl.when(s == n_src - 1)
    def _():
        def copies(k, i):
            at = pl.ds(aligned(k * region + i * TILE, TILE), TILE)
            made = [pltpu.make_async_copy(pool.at[at], out.at[at], sem)]
            if with_r:
                made.append(pltpu.make_async_copy(rpool.at[at], r_out.at[at], sem))
            return made

        tiles = []
        for k in range(n_loc):
            end = off[s * n_loc + k] + blocks(cnt[s * n_loc + k], 16) * 16
            at = pl.ds(aligned(k * region + end), TILE)
            pool[at, :] = jnp.zeros((TILE, pool.shape[1]), BF16)
            if with_r:
                rpool[at, :] = jnp.zeros((TILE, 128), F32)
            tiles.append(jnp.maximum(1, blocks(end, TILE)))
        for k in range(n_loc):
            def start(i, carry, k=k):
                for copy in copies(k, i):
                    copy.start()
                return carry

            lax.fori_loop(0, tiles[k], start, 0)
        for k in range(n_loc):
            def wait(i, carry, k=k):
                for copy in copies(k, i):
                    copy.wait()
                return carry

            lax.fori_loop(0, tiles[k], wait, 0)


def gather_rows(src, cnt, off, pos, r, region):
    n_src, n_loc, tok = pos.shape
    d = src.shape[1] // 2
    with_r = r is not None
    rows = n_loc * region
    scr = HEAD + up(n_loc * ((region - TILE) // n_src) + CHUNK - HEAD, MM)
    table = pl.BlockSpec((1, n_loc, tok), lambda s, *_: (s, 0, 0))
    in_specs = [table] + ([table] if with_r else []) + [pl.BlockSpec((tok, d), lambda s, *_: (s, 1 if with_r else 0))]
    out_shape = [jax.ShapeDtypeStruct((rows, d), BF16)]
    scratch = [pltpu.VMEM((scr, tok), BF16), pltpu.VMEM((scr, d), BF16), pltpu.VMEM((rows, d), BF16)]
    if with_r:
        out_shape.append(jax.ShapeDtypeStruct((rows, 128), F32))
        scratch += [pltpu.VMEM((scr, 128), F32), pltpu.VMEM((rows, 128), F32)]
    out = pl.pallas_call(
        functools.partial(gather_kernel, n_src, n_loc, region, with_r),
        out_shape=out_shape,
        grid_spec=pltpu.PrefetchScalarGridSpec(
            num_scalar_prefetch=2, grid=(n_src,), in_specs=in_specs,
            out_specs=[pl.BlockSpec(memory_space=pl.ANY)] * len(out_shape),
            scratch_shapes=scratch + [pltpu.SemaphoreType.DMA]),
        compiler_params=pltpu.CompilerParams(vmem_limit_bytes=VMEM_LIMIT, dimension_semantics=("arbitrary",)),
        cost_estimate=pl.CostEstimate(flops=2 * 12000 * tok * d, bytes_accessed=n_src * tok * d * 4, transcendentals=0),
        name="gather_r" if with_r else "gather_x",
    )(*([cnt, off, pos] + ([r] if with_r else []) + [src]))
    return out if with_r else out[0]


def expert_kernel(n_fs, info, x_ref, dy_ref, r_ref, *refs):
    own, gu_refs, down_refs, refs = refs[:3], refs[3:n_fs + 2], refs[n_fs + 2:2 * n_fs + 1], refs[2 * n_fs + 1:]
    (dx_ref, dr_ref), outs, refs = refs[:2], refs[2:n_fs + 2], refs[n_fs + 2:]
    w1_ref, w3_ref, w2, a_buf, dh1_buf, dh3_buf, dw1, dw3, dw2t = refs
    i = pl.program_id(0)
    d, f = w1_ref.shape
    dsl = d // n_fs

    @pl.when(i == 0)
    def _():
        dw1[...] = jnp.zeros_like(dw1)
        dw3[...] = jnp.zeros_like(dw3)
        dw2t[...] = jnp.zeros_like(dw2t)
        for m in range(n_fs):
            at = pl.ds(aligned((info[2] ^ m) * dsl, dsl), dsl)
            w1_ref[at, :] = gu_refs[m - 1][0, 0] if m else own[0][0]
            w3_ref[at, :] = gu_refs[m - 1][0, 1] if m else own[1][0]
            w2[:, at] = down_refs[m - 1][0] if m else own[2][0]

    def tile(m):
        x, dy = x_ref[:m, :], dy_ref[:m, :]
        dy_wide = dy.astype(F32)
        g = (r_ref[:m, 0:1] * dy_wide).astype(BF16)
        step = 256
        for c in range(0, f, step):
            cs = slice(c, c + step)
            h1 = dot(x, w1_ref[:, cs])
            h3 = dot(x, w3_ref[:, cs])
            da = dot_nt(g, w2[cs, :])
            s = jax.nn.sigmoid(h1)
            hs = h1 * s
            a_buf[:m, cs] = (hs * h3).astype(BF16)
            dh1_buf[:m, cs] = (da * h3 * s * (1.0 + h1 * (1.0 - s))).astype(BF16)
            dh3_buf[:m, cs] = (da * hs).astype(BF16)
        y = dot(a_buf[:m, :], w2[...])
        dr = jnp.sum(dy_wide * y, axis=1, keepdims=True)
        dr_ref[:m, :] = jnp.broadcast_to(dr, (m, 128))
        dx_ref[:m, :] = (dot_nt(dh1_buf[:m, :], w1_ref[...]) + dot_nt(dh3_buf[:m, :], w3_ref[...])).astype(BF16)
        dw1[...] += dot_tn(x, dh1_buf[:m, :])
        dw3[...] += dot_tn(x, dh3_buf[:m, :])
        dw2t[...] += dot_tn(g, a_buf[:m, :])

    left = info[0] - i * TILE

    @pl.when(left > TILE // 2)
    def _():
        tile(TILE)

    @pl.when((i < info[1]) & (left <= TILE // 2))
    def _():
        tile(TILE // 2)
        dx_ref[TILE // 2:, :] = jnp.zeros((TILE // 2, d), BF16)
        dr_ref[TILE // 2:, :] = jnp.zeros((TILE // 2, 128), F32)

    @pl.when(i == info[1] - 1)
    def _():
        for m in range(n_fs):
            at = pl.ds(aligned((info[2] ^ m) * dsl, dsl), dsl)
            for t, acc in enumerate((dw1, dw3, dw2t)):
                outs[m][t] = acc[at, :]


def expert_call(k, group_at, n_loc, info, x_pool, dy_pool, r_pool, own, gate_up, down, region):
    n_fs, (_, f, dsl) = len(down) + 1, down[0].shape
    d = n_fs * dsl
    first = k * (region // TILE)
    row_map = lambda i, info: (first + jnp.minimum(i, info[1] - 1), 0)
    out_map = lambda i, info: (jnp.minimum(i, info[1] - 1), 0)
    whole3 = lambda i, info: (0, 0, 0)
    mine = lambda i, info: (info[2] * n_loc + k, 0, 0)
    return pl.pallas_call(
        functools.partial(expert_kernel, n_fs),
        out_shape=[jax.ShapeDtypeStruct((region, d), BF16), jax.ShapeDtypeStruct((region, 128), F32)]
        + [jax.ShapeDtypeStruct((3, dsl, f), F32)] * n_fs,
        grid_spec=pltpu.PrefetchScalarGridSpec(
            num_scalar_prefetch=1, grid=(region // TILE - 1,),
            in_specs=[pl.BlockSpec((TILE, d), row_map), pl.BlockSpec((TILE, d), row_map), pl.BlockSpec((TILE, 128), row_map),
                      *[pl.BlockSpec((1, dsl, f), mine)] * 2, pl.BlockSpec((1, f, dsl), mine),
                      *[pl.BlockSpec((1, 2, dsl, f), lambda i, info: (group_at, 0, 0, 0))] * (n_fs - 1),
                      *[pl.BlockSpec((1, f, dsl), lambda i, info: (group_at, 0, 0))] * (n_fs - 1)],
            out_specs=[pl.BlockSpec((TILE, d), out_map), pl.BlockSpec((TILE, 128), out_map)]
            + [pl.BlockSpec((3, dsl, f), whole3)] * n_fs,
            scratch_shapes=[pltpu.VMEM((d, f), BF16)] * 2 + [pltpu.VMEM((f, d), BF16)] + [pltpu.VMEM((TILE, f), BF16)] * 3 + [pltpu.VMEM((d, f), F32)] * 3),
        compiler_params=pltpu.CompilerParams(vmem_limit_bytes=VMEM_LIMIT, dimension_semantics=("arbitrary",)),
        cost_estimate=pl.CostEstimate(flops=18 * 3000 * d * f, bytes_accessed=24 * d * f, transcendentals=3000 * f),
    )(info, x_pool, dy_pool, r_pool, *own, *gate_up, *down)


def place_kernel(n_fs, n_loc, k, first, me, *refs):
    pieces = refs[:n_fs]
    n_in = n_fs if first else n_fs + 3
    outs, (turned, sem) = refs[n_in:n_in + 3], refs[n_in + 3:]
    copies = []
    for m in range(n_fs):
        to = (me[0] ^ m) * n_loc + k
        copies.append(pltpu.make_async_copy(pieces[m].at[0], outs[0].at[to], sem))
        copies.append(pltpu.make_async_copy(pieces[m].at[1], outs[1].at[to], sem))
    for copy in copies:
        copy.start()
    for m in range(n_fs):
        turned[m] = pieces[m][2].T
        copies.append(pltpu.make_async_copy(turned.at[m], outs[2].at[(me[0] ^ m) * n_loc + k], sem))
        copies[-1].start()
    for copy in copies:
        copy.wait()


def place(k, n_loc, me, pieces, grads):
    n_fs = len(pieces)
    _, dsl, f = pieces[0].shape
    vmem, hbm = pl.BlockSpec(memory_space=pltpu.VMEM), pl.BlockSpec(memory_space=pl.ANY)
    first = grads is None
    shapes = [(n_fs * n_loc, dsl, f)] * 2 + [(n_fs * n_loc, f, dsl)]
    return pl.pallas_call(
        functools.partial(place_kernel, n_fs, n_loc, k, first),
        out_shape=[jax.ShapeDtypeStruct(v, F32) for v in shapes],
        in_specs=[pl.BlockSpec(memory_space=pltpu.SMEM)] + [vmem] * n_fs + ([] if first else [hbm] * 3),
        out_specs=[hbm] * 3,
        scratch_shapes=[pltpu.VMEM((n_fs, f, dsl), F32), pltpu.SemaphoreType.DMA],
        input_output_aliases={} if first else {n_fs + 1 + t: t for t in range(3)},
        compiler_params=pltpu.CompilerParams(vmem_limit_bytes=VMEM_LIMIT),
        cost_estimate=pl.CostEstimate(flops=0, bytes_accessed=6 * 4 * n_fs * dsl * f, transcendentals=0),
    )(me, *pieces, *([] if first else grads))


def combine_kernel(n_src, n_loc, cnt, off, pos_ref, *refs):
    dx_in, dr_in = refs[:n_loc], refs[n_loc:2 * n_loc]
    out, dr_out, hot, stage, pool, rpool, sem = refs[2 * n_loc:]
    s = pl.program_id(0)
    tok = pos_ref.shape[2]
    d = pool.shape[2]

    @pl.when(s == 0)
    def _():
        def copies(k, i):
            at = pl.ds(aligned(i * TILE, TILE), TILE)
            return [pltpu.make_async_copy(dx_in[k].at[at], pool.at[k, at], sem),
                    pltpu.make_async_copy(dr_in[k].at[at], rpool.at[k, at], sem)]

        tiles = []
        for k in range(n_loc):
            last = (n_src - 1) * n_loc + k
            end = off[last] + blocks(cnt[last], 16) * 16
            tiles.append(jnp.maximum(1, blocks(end, TILE)))
        for k in range(n_loc):
            def start(i, carry, k=k):
                for copy in copies(k, i):
                    copy.start()
                return carry

            lax.fori_loop(0, tiles[k], start, 0)
            at = pl.ds(aligned(tiles[k] * TILE), CHUNK)
            pool[k, at, :] = jnp.zeros((CHUNK, d), BF16)
            rpool[k, at, :] = jnp.zeros((CHUNK, 128), F32)
        for k in range(n_loc):
            def wait(i, carry, k=k):
                for copy in copies(k, i):
                    copy.wait()
                return carry

            lax.fori_loop(0, tiles[k], wait, 0)

    dr_out[...] = jnp.zeros_like(dr_out)
    base = jnp.int32(0)
    for k in range(n_loc):
        n = cnt[s * n_loc + k]
        frm = off[s * n_loc + k]
        pos_row = pos_ref[0, k:k + 1, :]

        def build(c, carry=0, base=base, frm=frm, pos_row=pos_row, k=k):
            m = one_hot_block(pos_row, c)
            at = pl.ds(aligned(base + c * CHUNK), CHUNK)
            src = pl.ds(aligned(frm + c * CHUNK), CHUNK)
            hot[at, :] = jnp.where(m, 1.0, 0.0).astype(BF16)
            stage[at, :] = pool[k, src, :]
            r = jnp.concatenate([rpool[k, src, :]] * (tok // 128), axis=1)
            dr_out[0, k:k + 1, :] += jnp.sum(jnp.where(m, r, 0.0), axis=0, keepdims=True)
            return carry

        build(0)
        lax.fori_loop(1, blocks(n, CHUNK), build, 0)
        base = base + blocks(n, 16) * 16
    tail = pl.ds(aligned(base), HEAD)
    hot[tail, :] = jnp.zeros((HEAD, tok), BF16)
    stage[tail, :] = jnp.zeros((HEAD, d), BF16)
    head = pl.ds(0, HEAD)
    out[...] = dot_tn(hot[head, :], stage[head, :])

    def mm(c, carry):
        at = pl.ds(aligned(HEAD + c * MM), MM)
        out[...] += dot_tn(hot[at, :], stage[at, :])
        return carry

    lax.fori_loop(0, blocks(jnp.maximum(base - HEAD, 0), MM), mm, 0)


def combine_rows(cnt, off, pos, dx_pools, dr_pools, region):
    n_src, n_loc, tok = pos.shape
    d = dx_pools[0].shape[1]
    scr = n_loc * ((region - TILE) // n_src) + HEAD
    hbm = pl.BlockSpec(memory_space=pl.ANY)
    return pl.pallas_call(
        functools.partial(combine_kernel, n_src, n_loc),
        out_shape=[jax.ShapeDtypeStruct((n_src * tok, d), F32), jax.ShapeDtypeStruct((n_src, n_loc, tok), F32)],
        grid_spec=pltpu.PrefetchScalarGridSpec(
            num_scalar_prefetch=2, grid=(n_src,),
            in_specs=[pl.BlockSpec((1, n_loc, tok), lambda s, *_: (s, 0, 0))] + [hbm] * (2 * n_loc),
            out_specs=[pl.BlockSpec((tok, d), lambda s, *_: (s, 0)),
                       pl.BlockSpec((1, n_loc, tok), lambda s, *_: (s, 0, 0))],
            scratch_shapes=[pltpu.VMEM((scr, tok), BF16), pltpu.VMEM((scr, d), BF16),
                            pltpu.VMEM((n_loc, region, d), BF16), pltpu.VMEM((n_loc, region, 128), F32),
                            pltpu.SemaphoreType.DMA]),
        compiler_params=pltpu.CompilerParams(vmem_limit_bytes=VMEM_LIMIT, dimension_semantics=("arbitrary",)),
        cost_estimate=pl.CostEstimate(flops=2 * 12000 * tok * d, bytes_accessed=n_src * tok * d * 4, transcendentals=0),
        name="combine",
    )(cnt, off, pos, *dx_pools, *dr_pools)


MESH = pl.DeviceIdType.MESH
HOPS = ((0, 2), (1, 0), (2, 0))
SIBLING = (0, 1)
ORDERS = ((0, 1, 2), (1, 2, 0), (2, 0, 1))
COLLECT_ORDERS = ((0, 1, 2), (0, 2, 1))


def here():
    return lax.axis_index("fsdp"), lax.axis_index("ep")


def peer_of(hop):
    f, p = here()
    return {"fsdp": f ^ hop[0], "ep": p ^ hop[1]}


def block_of(bits, core=0):
    f, p = here()
    for axis in range(3):
        if bits >> axis & 1:
            f, p = f ^ HOPS[axis][0], p ^ HOPS[axis][1]
    return f * 4 + (p ^ core)


def enter(n_fs, n_ep):
    barrier = pltpu.get_barrier_semaphore()
    for df in range(n_fs):
        for dp in range(n_ep):
            if df or dp:
                pl.semaphore_signal(barrier, inc=1, device_id=peer_of((df, dp)), device_id_type=MESH)
    pl.semaphore_wait(barrier, n_fs * n_ep - 1)


def exchange(n_fs, n_ep, src, dst, send, recv):
    f, p = here()
    copies = []
    for df in range(n_fs):
        for dp in range(n_ep):
            if df or dp:
                n = df * n_ep + dp
                copies.append(pltpu.make_async_remote_copy(
                    src_ref=src.at[(f ^ df) * n_ep + (p ^ dp)], dst_ref=dst.at[f * n_ep + p],
                    send_sem=send.at[n], recv_sem=recv.at[n], device_id=peer_of((df, dp)), device_id_type=MESH))
                copies[-1].start()
    return copies


def spread_kernel(n_fs, n_ep, n_loc, parts, x_ref, dy_ref, table_ref, wg_ref, wu_ref, wd_ref, full, table_all, *refs):
    n_slices, n_out = n_loc * (n_fs - 1), 2 * (n_fs - 1)
    gu_out, down_out, refs = refs[:n_out], refs[n_out:2 * n_out], refs[2 * n_out:]
    own, send, recv, c_send, c_recv, t_send, t_recv, own_sem, gu_buf, down_buf, in_sem, out_sem = refs
    tok, d = x_ref.shape
    mine = block_of(0)
    local = []
    for n, src in enumerate((x_ref, dy_ref)):
        local.append(pltpu.make_async_copy(src, own.at[:, pl.ds(n * d, d)], own_sem.at[n]))
        local[-1].start()
    enter(n_fs, n_ep)
    for copy in local:
        copy.wait()
    local = [pltpu.make_async_copy(own, full.at[pl.ds(aligned(mine * tok, tok), tok)], own_sem.at[0]),
             pltpu.make_async_copy(table_ref.at[mine], table_all.at[mine], own_sem.at[2])]
    starts = [sum(parts[:q]) for q in range(3)]
    sem_at = {}
    inbound = {}

    def send_on(q, phase, bits):
        to = pl.ds(aligned(block_of(bits) * tok + starts[q], 16), parts[q])
        src = own.at[pl.ds(starts[q], parts[q])] if bits == 0 else full.at[to]
        n = sem_at.setdefault((q, phase, bits), len(sem_at))
        copy = pltpu.make_async_remote_copy(
            src_ref=src, dst_ref=full.at[to], send_sem=send.at[n], recv_sem=recv.at[n],
            device_id=peer_of(HOPS[ORDERS[q][phase]]), device_id_type=MESH)
        copy.start()
        inbound[(q, phase, bits)] = copy

    shared = []

    def share(q, bits):
        to = pl.ds(aligned(block_of(bits) * tok + starts[q], 16), parts[q])
        src = own.at[pl.ds(starts[q], parts[q])] if bits == 0 else full.at[to]
        n = len(shared)
        copy = pltpu.make_async_remote_copy(
            src_ref=src, dst_ref=full.at[to], send_sem=c_send.at[n], recv_sem=c_recv.at[n],
            device_id=peer_of(SIBLING), device_id_type=MESH)
        copy.start()
        shared.append(copy)

    for phase in range(3):
        for q in range(3):
            send_on(q, phase, 0)
    for q in range(3):
        share(q, 0)
    for copy in local:
        copy.start()
    pending = exchange(n_fs, n_ep, table_ref, table_all, t_send, t_recv)
    f, _ = here()
    packs = []
    for k in range(n_loc):
        for m in range(1, n_fs):
            n = k * (n_fs - 1) + m - 1
            at = (f ^ m) * n_loc + k
            packs.append([pltpu.make_async_copy(wg_ref.at[at], gu_buf.at[n, 0], in_sem.at[3 * n]),
                          pltpu.make_async_copy(wu_ref.at[at], gu_buf.at[n, 1], in_sem.at[3 * n + 1]),
                          pltpu.make_async_copy(wd_ref.at[at], down_buf.at[n], in_sem.at[3 * n + 2])])
            for copy in packs[-1]:
                copy.start()
    for n in range(n_slices):
        for copy in packs[n]:
            copy.wait()
        k, m = n // (n_fs - 1), n % (n_fs - 1)
        to, at = (m, 0) if k == 0 else (n_fs - 1 + m, k - 1)
        for copy in (pltpu.make_async_copy(gu_buf.at[n], gu_out[to].at[at], out_sem.at[2 * n]),
                     pltpu.make_async_copy(down_buf.at[n], down_out[to].at[at], out_sem.at[2 * n + 1])):
            copy.start()
            local.append(copy)
    for phase in range(3):
        for q in range(3):
            held = [0]
            for axis in ORDERS[q][:phase]:
                held += [b | 1 << axis for b in held]
            for b in held:
                inbound[(q, phase, b)].wait_recv()
                got = b | 1 << ORDERS[q][phase]
                for later in range(phase + 1, 3):
                    send_on(q, later, got)
                share(q, got)
    for copy in inbound.values():
        copy.wait_send()
    for copy in shared:
        copy.wait()
    for copy in pending:
        copy.wait()
    for copy in local:
        copy.wait()


def spread(x_tok, dy_tok, table, w_gate, w_up, w_down, n_fs, n_ep):
    n_dev = n_fs * n_ep
    tok, d = x_tok.shape
    exp_local, dsl, f = w_gate.shape
    n_loc = exp_local // n_fs
    n_slices, groups = n_loc * (n_fs - 1), [1] * (n_fs - 1) + [n_loc - 1] * (n_fs - 1)
    third = tok // 3 // 16 * 16
    parts = (tok - 2 * third, third, third)
    vmem, hbm = pl.BlockSpec(memory_space=pltpu.VMEM), pl.BlockSpec(memory_space=pl.ANY)
    dma = pltpu.SemaphoreType.DMA
    return pl.pallas_call(
        functools.partial(spread_kernel, n_fs, n_ep, n_loc, parts),
        out_shape=[jax.ShapeDtypeStruct((n_dev * tok, 2 * d), x_tok.dtype), jax.ShapeDtypeStruct(table.shape, table.dtype)]
        + [jax.ShapeDtypeStruct((g, 2, dsl, f), BF16) for g in groups] + [jax.ShapeDtypeStruct((g, f, dsl), BF16) for g in groups],
        in_specs=[hbm] * 2 + [vmem] + [hbm] * 3, out_specs=[hbm] * (2 + 2 * len(groups)),
        scratch_shapes=[pltpu.VMEM((tok, 2 * d), BF16), dma((21,)), dma((21,)), dma((24,)), dma((24,)), dma((n_dev,)), dma((n_dev,)),
                        dma((3,)), pltpu.VMEM((n_slices, 2, dsl, f), BF16), pltpu.VMEM((n_slices, f, dsl), BF16),
                        dma((3 * n_slices,)), dma((2 * n_slices,))],
        compiler_params=pltpu.CompilerParams(collective_id=0, has_side_effects=True, vmem_limit_bytes=VMEM_LIMIT),
        cost_estimate=pl.CostEstimate(flops=0, bytes_accessed=8 * n_dev * tok * d, transcendentals=0),
        name="spread",
    )(x_tok, dy_tok, table, w_gate, w_up, w_down)


def collect_kernel(n_fs, n_ep, parts, part_ref, dr_ref, gx_ref, dr_home, acc, sib, got,
                   c_send, c_recv, send, recv, t_send, t_recv, own_sem):
    tok = gx_ref.shape[0]
    mine = block_of(0)
    enter(n_fs, n_ep)
    drs = exchange(n_fs, n_ep, dr_ref, dr_home, t_send, t_recv)
    local_dr = pltpu.make_async_copy(dr_ref.at[mine], dr_home.at[mine], own_sem.at[8])
    local_dr.start()
    order = (7, 3, 5, 1, 6, 2, 4, 0)
    loads, shares = {}, {}
    for bits in order:
        theirs = pl.ds(aligned(block_of(bits, 1) * tok, tok), tok)
        shares[bits] = pltpu.make_async_remote_copy(
            src_ref=part_ref.at[theirs], dst_ref=sib.at[bits], send_sem=c_send.at[bits], recv_sem=c_recv.at[bits],
            device_id=peer_of(SIBLING), device_id_type=MESH)
        shares[bits].start()
        ours = pl.ds(aligned(block_of(bits) * tok, tok), tok)
        loads[bits] = pltpu.make_async_copy(part_ref.at[ours], acc.at[bits], own_sem.at[bits])
        loads[bits].start()
    starts = [sum(parts[:q]) for q in range(len(parts))]
    slots = [(q, bits) for q in range(len(parts)) for bits in range(1, 8)]
    hops = {}

    def phase_of(q, bits):
        return next(n for n in range(3) if bits >> COLLECT_ORDERS[q][n] & 1)

    def send_off(q, bits):
        n = slots.index((q, bits))
        rows = pl.ds(starts[q], parts[q])
        hops[(q, bits)] = pltpu.make_async_remote_copy(
            src_ref=acc.at[bits, rows], dst_ref=got.at[bits - 1, rows], send_sem=send.at[n], recv_sem=recv.at[n],
            device_id=peer_of(HOPS[COLLECT_ORDERS[q][phase_of(q, bits)]]), device_id_type=MESH)
        hops[(q, bits)].start()

    def add_arrival(q, bits, phase):
        frm = bits | 1 << COLLECT_ORDERS[q][phase]
        hops[(q, frm)].wait_recv()
        rows = slice(starts[q], starts[q] + parts[q])
        acc[bits, rows, :] = acc[bits, rows, :] + got[frm - 1, rows, :]

    for bits in order:
        loads[bits].wait()
        shares[bits].wait_recv()
        acc[bits] = acc[bits] + sib[bits]
        for q in range(len(parts)):
            if bits and phase_of(q, bits) == 0:
                send_off(q, bits)
    for phase in (1, 2):
        for q in range(len(parts)):
            for bits in range(1, 8):
                if phase_of(q, bits) == phase:
                    for earlier in range(phase):
                        add_arrival(q, bits, earlier)
                    send_off(q, bits)
    for q in range(len(parts)):
        for phase in range(3):
            add_arrival(q, 0, phase)
        rows = slice(starts[q], starts[q] + parts[q])
        gx_ref[rows, :] = acc[0, rows, :].astype(gx_ref.dtype)
    for bits in order:
        shares[bits].wait_send()
    for copy in hops.values():
        copy.wait_send()
    for copy in drs:
        copy.wait()
    local_dr.wait()


def collect(dx_part, dr_part, n_fs, n_ep):
    n_dev = n_fs * n_ep
    tok, d = dx_part.shape[0] // n_dev, dx_part.shape[1]
    half = tok // 2 // 8 * 8
    parts = (tok - half, half)
    vmem, hbm = pl.BlockSpec(memory_space=pltpu.VMEM), pl.BlockSpec(memory_space=pl.ANY)
    dma = pltpu.SemaphoreType.DMA
    return pl.pallas_call(
        functools.partial(collect_kernel, n_fs, n_ep, parts),
        out_shape=[jax.ShapeDtypeStruct((tok, d), BF16), jax.ShapeDtypeStruct(dr_part.shape, F32)],
        in_specs=[hbm, vmem], out_specs=[vmem, vmem],
        scratch_shapes=[pltpu.VMEM((8, tok, d), F32), pltpu.VMEM((8, tok, d), F32), pltpu.VMEM((7, tok, d), F32),
                        dma((8,)), dma((8,)), dma((14,)), dma((14,)), dma((n_dev,)), dma((n_dev,)), dma((9,))],
        compiler_params=pltpu.CompilerParams(collective_id=1, has_side_effects=True, vmem_limit_bytes=VMEM_LIMIT),
        cost_estimate=pl.CostEstimate(flops=0, bytes_accessed=8 * n_dev * tok * d, transcendentals=0),
        name="collect",
    )(dx_part, dr_part)


def solution(mesh):
    n_ep, n_fs = mesh.shape["ep"], mesh.shape["fsdp"]
    n_dev = n_ep * n_fs
    both = ("fsdp", "ep")
    tok_spec = P(both, None)
    spec_in = P("ep", "fsdp", None)
    spec_out = P("ep", None, "fsdp")

    def body(x_tok, dy_tok, expert_ids, route_w, w_gate, w_up, w_down):
        tok, top_k = expert_ids.shape
        exp_local, _, _ = w_gate.shape
        n_loc = exp_local // n_fs
        experts = exp_local * n_ep
        capacity = capacity_of(tok, top_k, experts)
        region = n_dev * up(capacity, 16) + TILE

        position, weight = route_tables(expert_ids, route_w, experts, capacity)
        table = jnp.stack([position, weight], axis=1).reshape(n_ep, n_fs, n_loc, 2, tok)
        table = table.transpose(1, 0, 2, 3, 4).reshape(n_dev, n_loc * 2, tok)
        xdy_all, table, *packed = spread(x_tok, dy_tok, table, w_gate, w_up, w_down, n_fs, n_ep)
        table = table.reshape(n_dev, n_loc, 2, tok)
        me = lax.axis_index("fsdp").astype(jnp.int32)
        weights = []
        for group in range(2):
            weights.append([[lax.ppermute(packed[(2 * kind + group) * (n_fs - 1) + m - 1], "fsdp",
                                          [(i, i ^ m) for i in range(n_fs)]) for m in range(1, n_fs)]
                            for kind in range(2)])

        pos = table[:, :, 0, :].astype(jnp.int32)
        r = table[:, :, 1, :]
        cnt = jnp.max(pos, axis=2) + 1
        padded = blocks(cnt, 16) * 16
        off = jnp.cumsum(padded, axis=0) - padded
        rows = jnp.sum(padded, axis=0)
        cnt_flat, off_flat = cnt.reshape(-1), off.reshape(-1)
        x_pool = gather_rows(xdy_all, cnt_flat, off_flat, pos, None, region)
        dy_pool, r_pool = gather_rows(xdy_all, cnt_flat, off_flat, pos, r, region)

        dx_pools, dr_pools, pieces = [], [], []
        for k in range(n_loc):
            info = jnp.stack([rows[k], jnp.maximum(1, blocks(rows[k], TILE)), me])
            dxk, drk, *slices = expert_call(
                k, max(k - 1, 0), n_loc, info, x_pool, dy_pool, r_pool, (w_gate, w_up, w_down),
                *weights[min(k, 1)], region)
            dx_pools.append(dxk)
            dr_pools.append(drk)
            pieces.append([slices[0]] + [lax.ppermute(slices[m], "fsdp", [(i, i ^ m) for i in range(n_fs)])
                                         for m in range(1, n_fs)])
        dx_part, dr_part = combine_rows(cnt_flat, off_flat, pos, dx_pools, dr_pools, region)
        grad_x, dr_home = collect(dx_part, dr_part, n_fs, n_ep)
        dr_home = dr_home.reshape(n_fs, n_ep, n_loc, tok).transpose(1, 0, 2, 3).reshape(experts, tok)
        hit = expert_ids.T[:, None, :] == jnp.arange(experts, dtype=jnp.int32)[None, :, None]
        route_grad = jnp.sum(jnp.where(hit, dr_home[None], 0.0), axis=1).T
        grads = None
        for k in range(n_loc):
            grads = place(k, n_loc, me.reshape(1), pieces[k], grads)
        return grad_x, route_grad, *grads

    return jax.shard_map(
        body, mesh=mesh,
        in_specs=(tok_spec, tok_spec, tok_spec, tok_spec, spec_in, spec_in, spec_out),
        out_specs=(tok_spec, tok_spec, spec_in, spec_in, spec_out),
        check_vma=False)
```

```python
import functools

import jax
import jax.numpy as jnp
from jax import lax
from jax.experimental import pallas as pl
from jax.experimental.pallas import tpu as pltpu
from jax.sharding import PartitionSpec as P


CAP_FACTOR = 3
CHUNK = 128
TILE = 512
TIERS = (384, 640, 1024)
VMEM_LIMIT = 60 * 1024 * 1024
F32 = jnp.float32
BF16 = jnp.bfloat16


def capacity_of(tok_dev, top_k, experts):
    return max(8, ((CAP_FACTOR * tok_dev * top_k // experts + 7) // 8) * 8)


def up(n, m):
    return (n + m - 1) // m * m


def blocks(n, size):
    return lax.div(n + (size - 1), jnp.full_like(n, size))


def dot(a, b):
    return lax.dot_general(a, b, (((1,), (0,)), ((), ())), preferred_element_type=F32)


def dot_nt(a, b):
    return lax.dot_general(a, b, (((1,), (1,)), ((), ())), preferred_element_type=F32)


def dot_tn(a, b):
    return lax.dot_general(a, b, (((0,), (0,)), ((), ())), preferred_element_type=F32)


def route_tables(expert_ids, route_w, experts, capacity):
    tok_dev, _ = expert_ids.shape
    ids_t, w_t = expert_ids.T, route_w.T
    hit = ids_t[:, None, :] == jnp.arange(experts, dtype=jnp.int32)[None, :, None]
    chosen = jnp.any(hit, axis=0)
    weight = jnp.sum(jnp.where(hit, w_t[:, None, :], 0.0), axis=0)
    earlier = jnp.arange(tok_dev)[:, None] < jnp.arange(tok_dev)[None, :]
    before = dot(chosen.astype(BF16), earlier.astype(BF16))
    position = jnp.where(chosen & (before < capacity), before, -1.0)
    return position, weight


def one_hot_block(pos_row, first, size):
    return lax.broadcasted_iota(jnp.int32, (size, pos_row.shape[1]), 0) + first == pos_row


def tiers(rows, limit, work):
    work(0, TIERS[0])
    for first, last in zip(TIERS, (*TIERS[1:], limit)):
        pl.when(rows > first)(functools.partial(work, first, last - first))


def aligned(v, m=16):
    return pl.multiple_of(v, m)


def gather_kernel(n_src, n_loc, region, slots, with_r, *refs):
    if with_r:
        (cnt, off, pos_ref, r_ref, src_ref, out, r_out, hot, stage, pool, rstage, rpool, sem) = refs
    else:
        (cnt, off, pos_ref, src_ref, out, hot, stage, pool, sem) = refs
    s = pl.program_id(0)
    base = jnp.int32(0)
    starts = []
    for k in range(n_loc):
        n = cnt[s * n_loc + k]
        starts.append(base)
        pos_row = pos_ref[0, k:k + 1, :]

        def build(first, size, base=base, pos_row=pos_row, k=k):
            m = one_hot_block(pos_row, first, size)
            at = pl.ds(aligned(base + first), size)
            hot[at, :] = jnp.where(m, 1.0, 0.0).astype(BF16)
            if with_r:
                r = jnp.sum(jnp.where(m, r_ref[0, k:k + 1, :], 0.0), axis=1, keepdims=True)
                rstage[at, :] = jnp.broadcast_to(r, (size, 128))

        build(0, CHUNK)
        pl.when(n > CHUNK)(functools.partial(build, CHUNK, slots - CHUNK))
        base = base + blocks(n, 16) * 16

    def mm(first, size):
        at = pl.ds(first, size)
        stage[at, :] = dot(hot[at, :], src_ref[...]).astype(BF16)

    tiers(base, hot.shape[0], mm)

    for k in range(n_loc):
        n = cnt[s * n_loc + k]
        to = off[s * n_loc + k] + k * region

        def move(first, size, start=starts[k], to=to):
            dst = pl.ds(aligned(to + first), size)
            frm = pl.ds(aligned(start + first), size)
            pool[dst, :] = stage[frm, :]
            if with_r:
                rpool[dst, :] = rstage[frm, :]

        move(0, CHUNK)
        pl.when(n > CHUNK)(functools.partial(move, CHUNK, slots - CHUNK))

    @pl.when(s == n_src - 1)
    def _():
        def copies(k, i):
            at = pl.ds(aligned(k * region + i * TILE, TILE), TILE)
            made = [pltpu.make_async_copy(pool.at[at], out.at[at], sem)]
            if with_r:
                made.append(pltpu.make_async_copy(rpool.at[at], r_out.at[at], sem))
            return made

        tiles = []
        for k in range(n_loc):
            end = off[s * n_loc + k] + blocks(cnt[s * n_loc + k], 16) * 16
            at = pl.ds(aligned(k * region + end), TILE)
            pool[at, :] = jnp.zeros((TILE, pool.shape[1]), BF16)
            if with_r:
                rpool[at, :] = jnp.zeros((TILE, 128), F32)
            tiles.append(jnp.maximum(1, blocks(end, TILE)))
        for k in range(n_loc):
            def start(i, carry, k=k):
                for copy in copies(k, i):
                    copy.start()
                return carry

            lax.fori_loop(0, tiles[k], start, 0)
        for k in range(n_loc):
            def wait(i, carry, k=k):
                for copy in copies(k, i):
                    copy.wait()
                return carry

            lax.fori_loop(0, tiles[k], wait, 0)


def gather_rows(src, cnt, off, pos, r, region):
    n_src, n_loc, tok = pos.shape
    d = src.shape[1] // 2
    with_r = r is not None
    rows = n_loc * region
    scr = up(n_loc * ((region - TILE) // n_src) + CHUNK, CHUNK)
    table = pl.BlockSpec((1, n_loc, tok), lambda s, *_: (s, 0, 0))
    in_specs = [table] + ([table] if with_r else []) + [pl.BlockSpec((tok, d), lambda s, *_: (s, 1 if with_r else 0))]
    out_shape = [jax.ShapeDtypeStruct((rows, d), BF16)]
    scratch = [pltpu.VMEM((scr, tok), BF16), pltpu.VMEM((scr, d), BF16), pltpu.VMEM((rows, d), BF16)]
    if with_r:
        out_shape.append(jax.ShapeDtypeStruct((rows, 128), F32))
        scratch += [pltpu.VMEM((scr, 128), F32), pltpu.VMEM((rows, 128), F32)]
    out = pl.pallas_call(
        functools.partial(gather_kernel, n_src, n_loc, region, up((region - TILE) // n_src, CHUNK), with_r),
        out_shape=out_shape,
        grid_spec=pltpu.PrefetchScalarGridSpec(
            num_scalar_prefetch=2, grid=(n_src,), in_specs=in_specs,
            out_specs=[pl.BlockSpec(memory_space=pl.ANY)] * len(out_shape),
            scratch_shapes=scratch + [pltpu.SemaphoreType.DMA]),
        compiler_params=pltpu.CompilerParams(vmem_limit_bytes=VMEM_LIMIT, dimension_semantics=("arbitrary",)),
        cost_estimate=pl.CostEstimate(flops=2 * 12000 * tok * d, bytes_accessed=n_src * tok * d * 4, transcendentals=0),
        name="gather_r" if with_r else "gather_x",
    )(*([cnt, off, pos] + ([r] if with_r else []) + [src]))
    return out if with_r else out[0]


def expert_kernel(n_fs, info, x_ref, dy_ref, r_ref, *refs):
    own, peers, refs = refs[:3], refs[3:n_fs + 2], refs[n_fs + 2:]
    (dx_ref, dr_ref), outs, refs = refs[:2], refs[2:n_fs + 2], refs[n_fs + 2:]
    w1_ref, w3_ref, w2t, a_buf, dh1_buf, dh3_buf, dw1, dw3, dw2t = refs
    i = pl.program_id(0)
    d, f = w1_ref.shape
    dsl = d // n_fs

    @pl.when(i == 0)
    def _():
        dw1[...] = jnp.zeros_like(dw1)
        dw3[...] = jnp.zeros_like(dw3)
        dw2t[...] = jnp.zeros_like(dw2t)
        for m in range(n_fs):
            at = pl.ds(aligned((info[2] ^ m) * dsl, dsl), dsl)
            for t, whole in enumerate((w1_ref, w3_ref, w2t)):
                whole[at, :] = peers[m - 1][0, t] if m else own[t][0]

    def tile(m):
        x, dy = x_ref[:m, :], dy_ref[:m, :]
        dy_wide = dy.astype(F32)
        g = (r_ref[:m, 0:1] * dy_wide).astype(BF16)
        step = 256
        for c in range(0, f, step):
            cs = slice(c, c + step)
            h1 = dot(x, w1_ref[:, cs])
            h3 = dot(x, w3_ref[:, cs])
            da = dot(g, w2t[:, cs])
            s = jax.nn.sigmoid(h1)
            hs = h1 * s
            a_buf[:m, cs] = (hs * h3).astype(BF16)
            dh1_buf[:m, cs] = (da * h3 * s * (1.0 + h1 * (1.0 - s))).astype(BF16)
            dh3_buf[:m, cs] = (da * hs).astype(BF16)
        y = dot_nt(a_buf[:m, :], w2t[...])
        dr = jnp.sum(dy_wide * y, axis=1, keepdims=True)
        dr_ref[:m, :] = jnp.broadcast_to(dr, (m, 128))
        dx_ref[:m, :] = (dot_nt(dh1_buf[:m, :], w1_ref[...]) + dot_nt(dh3_buf[:m, :], w3_ref[...])).astype(BF16)
        dw1[...] += dot_tn(x, dh1_buf[:m, :])
        dw3[...] += dot_tn(x, dh3_buf[:m, :])
        dw2t[...] += dot_tn(g, a_buf[:m, :])

    left = info[0] - i * TILE

    @pl.when(left > TILE // 2)
    def _():
        tile(TILE)

    @pl.when((i < info[1]) & (left <= TILE // 2))
    def _():
        tile(TILE // 2)
        dx_ref[TILE // 2:, :] = jnp.zeros((TILE // 2, d), BF16)
        dr_ref[TILE // 2:, :] = jnp.zeros((TILE // 2, 128), F32)

    @pl.when(i == info[1] - 1)
    def _():
        for m in range(n_fs):
            at = pl.ds(aligned((info[2] ^ m) * dsl, dsl), dsl)
            for t, acc in enumerate((dw1, dw3, dw2t)):
                outs[m][t] = acc[at, :]


def expert_call(k, group_at, n_loc, info, x_pool, dy_pool, r_pool, own, peers, region):
    n_fs, (_, _, dsl, f) = len(peers) + 1, peers[0].shape
    d = n_fs * dsl
    first = k * (region // TILE)
    row_map = lambda i, info: (first + jnp.minimum(i, info[1] - 1), 0)
    out_map = lambda i, info: (jnp.minimum(i, info[1] - 1), 0)
    whole3 = lambda i, info: (0, 0, 0)
    mine = lambda i, info: (info[2] * n_loc + k, 0, 0)
    return pl.pallas_call(
        functools.partial(expert_kernel, n_fs),
        out_shape=[jax.ShapeDtypeStruct((region, d), BF16), jax.ShapeDtypeStruct((region, 128), F32)]
        + [jax.ShapeDtypeStruct((3, dsl, f), F32)] * n_fs,
        grid_spec=pltpu.PrefetchScalarGridSpec(
            num_scalar_prefetch=1, grid=(region // TILE - 1,),
            in_specs=[pl.BlockSpec((TILE, d), row_map), pl.BlockSpec((TILE, d), row_map), pl.BlockSpec((TILE, 128), row_map),
                      *[pl.BlockSpec((1, dsl, f), mine)] * 2, pl.BlockSpec((1, dsl, f), lambda i, info: (k, 0, 0)),
                      *[pl.BlockSpec((1, 3, dsl, f), lambda i, info: (group_at, 0, 0, 0))] * (n_fs - 1)],
            out_specs=[pl.BlockSpec((TILE, d), out_map), pl.BlockSpec((TILE, 128), out_map)]
            + [pl.BlockSpec((3, dsl, f), whole3)] * n_fs,
            scratch_shapes=[pltpu.VMEM((d, f), BF16)] * 3 + [pltpu.VMEM((TILE, f), BF16)] * 3 + [pltpu.VMEM((d, f), F32)] * 3),
        compiler_params=pltpu.CompilerParams(vmem_limit_bytes=VMEM_LIMIT, dimension_semantics=("arbitrary",)),
        cost_estimate=pl.CostEstimate(flops=18 * 3000 * d * f, bytes_accessed=24 * d * f, transcendentals=3000 * f),
    )(info, x_pool, dy_pool, r_pool, *own, *peers)


def place_kernel(n_fs, n_loc, k, first, me, *refs):
    pieces = refs[:n_fs]
    n_in = n_fs if first else n_fs + 3
    outs, (turned, sem) = refs[n_in:n_in + 3], refs[n_in + 3:]
    copies = []
    for m in range(n_fs):
        to = (me[0] ^ m) * n_loc + k
        copies.append(pltpu.make_async_copy(pieces[m].at[0], outs[0].at[to], sem))
        copies.append(pltpu.make_async_copy(pieces[m].at[1], outs[1].at[to], sem))
    for copy in copies:
        copy.start()
    for m in range(n_fs):
        turned[m] = pieces[m][2].T
        copies.append(pltpu.make_async_copy(turned.at[m], outs[2].at[(me[0] ^ m) * n_loc + k], sem))
        copies[-1].start()
    for copy in copies:
        copy.wait()


def place(k, n_loc, me, pieces, grads):
    n_fs = len(pieces)
    _, dsl, f = pieces[0].shape
    vmem, hbm = pl.BlockSpec(memory_space=pltpu.VMEM), pl.BlockSpec(memory_space=pl.ANY)
    first = grads is None
    shapes = [(n_fs * n_loc, dsl, f)] * 2 + [(n_fs * n_loc, f, dsl)]
    return pl.pallas_call(
        functools.partial(place_kernel, n_fs, n_loc, k, first),
        out_shape=[jax.ShapeDtypeStruct(v, F32) for v in shapes],
        in_specs=[pl.BlockSpec(memory_space=pltpu.SMEM)] + [vmem] * n_fs + ([] if first else [hbm] * 3),
        out_specs=[hbm] * 3,
        scratch_shapes=[pltpu.VMEM((n_fs, f, dsl), F32), pltpu.SemaphoreType.DMA],
        input_output_aliases={} if first else {n_fs + 1 + t: t for t in range(3)},
        compiler_params=pltpu.CompilerParams(vmem_limit_bytes=VMEM_LIMIT),
        cost_estimate=pl.CostEstimate(flops=0, bytes_accessed=6 * 4 * n_fs * dsl * f, transcendentals=0),
    )(me, *pieces, *([] if first else grads))


def combine_kernel(n_src, n_loc, slots, cnt, off, pos_ref, *refs):
    dx_in, dr_in = refs[:n_loc], refs[n_loc:2 * n_loc]
    out, dr_out, hot, stage, pool, rpool, sem = refs[2 * n_loc:]
    s = pl.program_id(0)
    tok = pos_ref.shape[2]
    d = pool.shape[2]

    @pl.when(s == 0)
    def _():
        def copies(k, i):
            at = pl.ds(aligned(i * TILE, TILE), TILE)
            return [pltpu.make_async_copy(dx_in[k].at[at], pool.at[k, at], sem),
                    pltpu.make_async_copy(dr_in[k].at[at], rpool.at[k, at], sem)]

        tiles = []
        for k in range(n_loc):
            last = (n_src - 1) * n_loc + k
            end = off[last] + blocks(cnt[last], 16) * 16
            tiles.append(jnp.maximum(1, blocks(end, TILE)))
        for k in range(n_loc):
            def start(i, carry, k=k):
                for copy in copies(k, i):
                    copy.start()
                return carry

            lax.fori_loop(0, tiles[k], start, 0)
            at = pl.ds(aligned(tiles[k] * TILE), TILE)
            pool[k, at, :] = jnp.zeros((TILE, d), BF16)
            rpool[k, at, :] = jnp.zeros((TILE, 128), F32)
        for k in range(n_loc):
            def wait(i, carry, k=k):
                for copy in copies(k, i):
                    copy.wait()
                return carry

            lax.fori_loop(0, tiles[k], wait, 0)

    dr_out[...] = jnp.zeros_like(dr_out)
    base = jnp.int32(0)
    for k in range(n_loc):
        n = cnt[s * n_loc + k]
        frm = off[s * n_loc + k]
        pos_row = pos_ref[0, k:k + 1, :]

        def build(first, size, base=base, frm=frm, pos_row=pos_row, k=k):
            m = one_hot_block(pos_row, first, size)
            at = pl.ds(aligned(base + first), size)
            src = pl.ds(aligned(frm + first), size)
            hot[at, :] = jnp.where(m, 1.0, 0.0).astype(BF16)
            stage[at, :] = pool[k, src, :]
            r = jnp.concatenate([rpool[k, src, :]] * (tok // 128), axis=1)
            dr_out[0, k:k + 1, :] += jnp.sum(jnp.where(m, r, 0.0), axis=0, keepdims=True)

        build(0, CHUNK)
        pl.when(n > CHUNK)(functools.partial(build, CHUNK, slots - CHUNK))
        base = base + blocks(n, 16) * 16

    def clear(size):
        tail = pl.ds(aligned(base), size)
        hot[tail, :] = jnp.zeros((size, tok), BF16)
        stage[tail, :] = jnp.zeros((size, d), BF16)

    clear(TIERS[0])
    pl.when(base > TIERS[1])(functools.partial(clear, hot.shape[0] - n_loc * slots))

    def mm(first, size):
        at = pl.ds(first, size)
        part = dot_tn(hot[at, :], stage[at, :])
        out[...] = part if first == 0 else out[...] + part

    tiers(base, n_loc * slots, mm)


def combine_rows(cnt, off, pos, dx_pools, dr_pools, region):
    n_src, n_loc, tok = pos.shape
    d = dx_pools[0].shape[1]
    slots = up((region - TILE) // n_src, CHUNK)
    scr = n_loc * slots + TILE
    hbm = pl.BlockSpec(memory_space=pl.ANY)
    return pl.pallas_call(
        functools.partial(combine_kernel, n_src, n_loc, slots),
        out_shape=[jax.ShapeDtypeStruct((n_src * tok, d), F32), jax.ShapeDtypeStruct((n_src, n_loc, tok), F32)],
        grid_spec=pltpu.PrefetchScalarGridSpec(
            num_scalar_prefetch=2, grid=(n_src,),
            in_specs=[pl.BlockSpec((1, n_loc, tok), lambda s, *_: (s, 0, 0))] + [hbm] * (2 * n_loc),
            out_specs=[pl.BlockSpec((tok, d), lambda s, *_: (s, 0)),
                       pl.BlockSpec((1, n_loc, tok), lambda s, *_: (s, 0, 0))],
            scratch_shapes=[pltpu.VMEM((scr, tok), BF16), pltpu.VMEM((scr, d), BF16),
                            pltpu.VMEM((n_loc, region, d), BF16), pltpu.VMEM((n_loc, region, 128), F32),
                            pltpu.SemaphoreType.DMA]),
        compiler_params=pltpu.CompilerParams(vmem_limit_bytes=VMEM_LIMIT, dimension_semantics=("arbitrary",)),
        cost_estimate=pl.CostEstimate(flops=2 * 12000 * tok * d, bytes_accessed=n_src * tok * d * 4, transcendentals=0),
        name="combine",
    )(cnt, off, pos, *dx_pools, *dr_pools)


MESH = pl.DeviceIdType.MESH
HOPS = ((0, 2), (1, 0), (2, 0))
SIBLING = (0, 1)
ORDERS = ((0, 1, 2), (1, 2, 0), (2, 0, 1))


def here():
    return lax.axis_index("fsdp"), lax.axis_index("ep")


def peer_of(hop):
    f, p = here()
    return {"fsdp": f ^ hop[0], "ep": p ^ hop[1]}


def block_of(bits, core=0):
    f, p = here()
    for axis in range(3):
        if bits >> axis & 1:
            f, p = f ^ HOPS[axis][0], p ^ HOPS[axis][1]
    return f * 4 + (p ^ core)


def enter(n_fs, n_ep):
    barrier = pltpu.get_barrier_semaphore()
    for df in range(n_fs):
        for dp in range(n_ep):
            if df or dp:
                pl.semaphore_signal(barrier, inc=1, device_id=peer_of((df, dp)), device_id_type=MESH)
    pl.semaphore_wait(barrier, n_fs * n_ep - 1)


def exchange(n_fs, n_ep, src, dst, send, recv):
    f, p = here()
    copies = []
    for df in range(n_fs):
        for dp in range(n_ep):
            if df or dp:
                n = df * n_ep + dp
                copies.append(pltpu.make_async_remote_copy(
                    src_ref=src.at[(f ^ df) * n_ep + (p ^ dp)], dst_ref=dst.at[f * n_ep + p],
                    send_sem=send.at[n], recv_sem=recv.at[n], device_id=peer_of((df, dp)), device_id_type=MESH))
                copies[-1].start()
    return copies


def spread_kernel(n_fs, n_ep, n_loc, parts, x_ref, dy_ref, table_ref, wg_ref, wu_ref, wd_ref, full, table_all, *refs):
    n_out = 2 * (n_fs - 1)
    own_down, w_out, refs = refs[0], refs[1:n_out + 1], refs[n_out + 1:]
    own, send, recv, c_send, c_recv, t_send, t_recv, own_sem, w_buf, down_buf, in_sem, out_sem = refs
    tok, d = x_ref.shape
    mine = block_of(0)
    local = []
    for n, src in enumerate((x_ref, dy_ref)):
        local.append(pltpu.make_async_copy(src, own.at[:, pl.ds(n * d, d)], own_sem.at[n]))
        local[-1].start()
    enter(n_fs, n_ep)
    for copy in local:
        copy.wait()
    local = [pltpu.make_async_copy(own, full.at[pl.ds(aligned(mine * tok, tok), tok)], own_sem.at[0]),
             pltpu.make_async_copy(table_ref.at[mine], table_all.at[mine], own_sem.at[2])]
    starts = [sum(parts[:q]) for q in range(3)]
    sem_at = {}
    inbound = {}

    def send_on(q, phase, bits):
        to = pl.ds(aligned(block_of(bits) * tok + starts[q], 16), parts[q])
        src = own.at[pl.ds(starts[q], parts[q])] if bits == 0 else full.at[to]
        n = sem_at.setdefault((q, phase, bits), len(sem_at))
        copy = pltpu.make_async_remote_copy(
            src_ref=src, dst_ref=full.at[to], send_sem=send.at[n], recv_sem=recv.at[n],
            device_id=peer_of(HOPS[ORDERS[q][phase]]), device_id_type=MESH)
        copy.start()
        inbound[(q, phase, bits)] = copy

    shared = []

    def share(q, bits):
        to = pl.ds(aligned(block_of(bits) * tok + starts[q], 16), parts[q])
        src = own.at[pl.ds(starts[q], parts[q])] if bits == 0 else full.at[to]
        n = len(shared)
        copy = pltpu.make_async_remote_copy(
            src_ref=src, dst_ref=full.at[to], send_sem=c_send.at[n], recv_sem=c_recv.at[n],
            device_id=peer_of(SIBLING), device_id_type=MESH)
        copy.start()
        shared.append(copy)

    for phase in range(3):
        for q in range(3):
            send_on(q, phase, 0)
    for q in range(3):
        share(q, 0)
    for copy in local:
        copy.start()
    pending = exchange(n_fs, n_ep, table_ref, table_all, t_send, t_recv)
    f, _ = here()
    packs = []
    for k in range(n_loc):
        for m in range(n_fs):
            n = k * n_fs + m
            at = (f ^ m) * n_loc + k
            packs.append([pltpu.make_async_copy(wd_ref.at[at], down_buf.at[n], in_sem.at[3 * n])])
            if m:
                packs[-1] += [pltpu.make_async_copy(w.at[at], w_buf.at[n, t], in_sem.at[3 * n + 1 + t])
                              for t, w in enumerate((wg_ref, wu_ref))]
            for copy in packs[-1]:
                copy.start()
    for n in range(n_loc * n_fs):
        for copy in packs[n]:
            copy.wait()
        w_buf[n, 2] = down_buf[n].T
        k, m = n // n_fs, n % n_fs
        if m == 0:
            copy = pltpu.make_async_copy(w_buf.at[n, 2], own_down.at[k], out_sem.at[n])
        else:
            to, at = (m - 1, 0) if k == 0 else (n_fs + m - 2, k - 1)
            copy = pltpu.make_async_copy(w_buf.at[n], w_out[to].at[at], out_sem.at[n])
        copy.start()
        local.append(copy)
    for phase in range(3):
        for q in range(3):
            held = [0]
            for axis in ORDERS[q][:phase]:
                held += [b | 1 << axis for b in held]
            for b in held:
                inbound[(q, phase, b)].wait_recv()
                got = b | 1 << ORDERS[q][phase]
                for later in range(phase + 1, 3):
                    send_on(q, later, got)
                share(q, got)
    for copy in inbound.values():
        copy.wait_send()
    for copy in shared:
        copy.wait()
    for copy in pending:
        copy.wait()
    for copy in local:
        copy.wait()


def spread(x_tok, dy_tok, table, w_gate, w_up, w_down, n_fs, n_ep):
    n_dev = n_fs * n_ep
    tok, d = x_tok.shape
    exp_local, dsl, f = w_gate.shape
    n_loc = exp_local // n_fs
    n_slices, groups = n_loc * n_fs, [1] * (n_fs - 1) + [n_loc - 1] * (n_fs - 1)
    third = tok // 3 // 16 * 16
    parts = (tok - 2 * third, third, third)
    vmem, hbm = pl.BlockSpec(memory_space=pltpu.VMEM), pl.BlockSpec(memory_space=pl.ANY)
    dma = pltpu.SemaphoreType.DMA
    return pl.pallas_call(
        functools.partial(spread_kernel, n_fs, n_ep, n_loc, parts),
        out_shape=[jax.ShapeDtypeStruct((n_dev * tok, 2 * d), x_tok.dtype), jax.ShapeDtypeStruct(table.shape, table.dtype)]
        + [jax.ShapeDtypeStruct((n_loc, dsl, f), BF16)] + [jax.ShapeDtypeStruct((g, 3, dsl, f), BF16) for g in groups],
        in_specs=[hbm] * 2 + [vmem] + [hbm] * 3, out_specs=[hbm] * (3 + len(groups)),
        scratch_shapes=[pltpu.VMEM((tok, 2 * d), BF16), dma((21,)), dma((21,)), dma((24,)), dma((24,)), dma((n_dev,)), dma((n_dev,)),
                        dma((3,)), pltpu.VMEM((n_slices, 3, dsl, f), BF16), pltpu.VMEM((n_slices, f, dsl), BF16),
                        dma((3 * n_slices,)), dma((n_slices,))],
        compiler_params=pltpu.CompilerParams(collective_id=0, has_side_effects=True, vmem_limit_bytes=VMEM_LIMIT),
        cost_estimate=pl.CostEstimate(flops=0, bytes_accessed=8 * n_dev * tok * d, transcendentals=0),
        name="spread",
    )(x_tok, dy_tok, table, w_gate, w_up, w_down)


def collect_kernel(n_fs, n_ep, parts, part_ref, dr_ref, gx_ref, dr_home, acc, sib, got,
                   c_send, c_recv, send, recv, t_send, t_recv, own_sem):
    tok = gx_ref.shape[0]
    mine = block_of(0)
    enter(n_fs, n_ep)
    drs = exchange(n_fs, n_ep, dr_ref, dr_home, t_send, t_recv)
    local_dr = pltpu.make_async_copy(dr_ref.at[mine], dr_home.at[mine], own_sem.at[8])
    local_dr.start()
    order = (7, 3, 5, 6, 1, 2, 4, 0)
    loads, shares = {}, {}
    for bits in order:
        theirs = pl.ds(aligned(block_of(bits, 1) * tok, tok), tok)
        shares[bits] = pltpu.make_async_remote_copy(
            src_ref=part_ref.at[theirs], dst_ref=sib.at[bits], send_sem=c_send.at[bits], recv_sem=c_recv.at[bits],
            device_id=peer_of(SIBLING), device_id_type=MESH)
        shares[bits].start()
        ours = pl.ds(aligned(block_of(bits) * tok, tok), tok)
        loads[bits] = pltpu.make_async_copy(part_ref.at[ours], acc.at[bits], own_sem.at[bits])
        loads[bits].start()
    starts = [sum(parts[:q]) for q in range(len(parts))]
    slots = [(q, bits) for q in range(len(parts)) for bits in range(1, 8)]
    hops = {}

    def phase_of(q, bits):
        return next(n for n in range(3) if bits >> ORDERS[q][n] & 1)

    def send_off(q, bits):
        n = slots.index((q, bits))
        rows = pl.ds(starts[q], parts[q])
        hops[(q, bits)] = pltpu.make_async_remote_copy(
            src_ref=acc.at[bits, rows], dst_ref=got.at[bits - 1, rows], send_sem=send.at[n], recv_sem=recv.at[n],
            device_id=peer_of(HOPS[ORDERS[q][phase_of(q, bits)]]), device_id_type=MESH)
        hops[(q, bits)].start()

    def add_arrival(q, bits, phase):
        frm = bits | 1 << ORDERS[q][phase]
        hops[(q, frm)].wait_recv()
        rows = slice(starts[q], starts[q] + parts[q])
        acc[bits, rows, :] = acc[bits, rows, :] + got[frm - 1, rows, :]

    for bits in order:
        loads[bits].wait()
        shares[bits].wait_recv()
        acc[bits] = acc[bits] + sib[bits]
        for q in range(len(parts)):
            if bits and phase_of(q, bits) == 0:
                send_off(q, bits)
    for phase in (1, 2):
        for q in range(len(parts)):
            for bits in range(1, 8):
                if phase_of(q, bits) == phase:
                    for earlier in range(phase):
                        add_arrival(q, bits, earlier)
                    send_off(q, bits)
    for q in range(len(parts)):
        for phase in range(3):
            add_arrival(q, 0, phase)
        rows = slice(starts[q], starts[q] + parts[q])
        gx_ref[rows, :] = acc[0, rows, :].astype(gx_ref.dtype)
    for bits in order:
        shares[bits].wait_send()
    for copy in hops.values():
        copy.wait_send()
    for copy in drs:
        copy.wait()
    local_dr.wait()


def collect(dx_part, dr_part, n_fs, n_ep):
    n_dev = n_fs * n_ep
    tok, d = dx_part.shape[0] // n_dev, dx_part.shape[1]
    quarter = tok // 4 // 8 * 8
    parts = (tok - 2 * quarter, quarter, quarter)
    vmem, hbm = pl.BlockSpec(memory_space=pltpu.VMEM), pl.BlockSpec(memory_space=pl.ANY)
    dma = pltpu.SemaphoreType.DMA
    return pl.pallas_call(
        functools.partial(collect_kernel, n_fs, n_ep, parts),
        out_shape=[jax.ShapeDtypeStruct((tok, d), BF16), jax.ShapeDtypeStruct(dr_part.shape, F32)],
        in_specs=[hbm, vmem], out_specs=[vmem, vmem],
        scratch_shapes=[pltpu.VMEM((8, tok, d), F32), pltpu.VMEM((8, tok, d), F32), pltpu.VMEM((7, tok, d), F32),
                        dma((8,)), dma((8,)), dma((21,)), dma((21,)), dma((n_dev,)), dma((n_dev,)), dma((9,))],
        compiler_params=pltpu.CompilerParams(collective_id=1, has_side_effects=True, vmem_limit_bytes=VMEM_LIMIT),
        cost_estimate=pl.CostEstimate(flops=0, bytes_accessed=8 * n_dev * tok * d, transcendentals=0),
        name="collect",
    )(dx_part, dr_part)


def solution(mesh):
    n_ep, n_fs = mesh.shape["ep"], mesh.shape["fsdp"]
    n_dev = n_ep * n_fs
    both = ("fsdp", "ep")
    tok_spec = P(both, None)
    spec_in = P("ep", "fsdp", None)
    spec_out = P("ep", None, "fsdp")

    def body(x_tok, dy_tok, expert_ids, route_w, w_gate, w_up, w_down):
        tok, top_k = expert_ids.shape
        exp_local, _, _ = w_gate.shape
        n_loc = exp_local // n_fs
        experts = exp_local * n_ep
        capacity = capacity_of(tok, top_k, experts)
        region = n_dev * up(capacity, 16) + TILE

        position, weight = route_tables(expert_ids, route_w, experts, capacity)
        table = jnp.stack([position, weight], axis=1).reshape(n_ep, n_fs, n_loc, 2, tok)
        table = table.transpose(1, 0, 2, 3, 4).reshape(n_dev, n_loc * 2, tok)
        xdy_all, table, own_down, *packed = spread(x_tok, dy_tok, table, w_gate, w_up, w_down, n_fs, n_ep)
        table = table.reshape(n_dev, n_loc, 2, tok)
        me = lax.axis_index("fsdp").astype(jnp.int32)
        weights = []
        for group in range(2):
            weights.append([lax.ppermute(packed[group * (n_fs - 1) + m - 1], "fsdp", [(i, i ^ m) for i in range(n_fs)])
                            for m in range(1, n_fs)])

        pos = table[:, :, 0, :].astype(jnp.int32)
        r = table[:, :, 1, :]
        cnt = jnp.max(pos, axis=2) + 1
        padded = blocks(cnt, 16) * 16
        off = jnp.cumsum(padded, axis=0) - padded
        rows = jnp.sum(padded, axis=0)
        cnt_flat, off_flat = cnt.reshape(-1), off.reshape(-1)
        x_pool = gather_rows(xdy_all, cnt_flat, off_flat, pos, None, region)
        dy_pool, r_pool = gather_rows(xdy_all, cnt_flat, off_flat, pos, r, region)

        dx_pools, dr_pools, pieces = [], [], []
        for k in range(n_loc):
            info = jnp.stack([rows[k], jnp.maximum(1, blocks(rows[k], TILE)), me])
            dxk, drk, *slices = expert_call(
                k, max(k - 1, 0), n_loc, info, x_pool, dy_pool, r_pool, (w_gate, w_up, own_down),
                weights[min(k, 1)], region)
            dx_pools.append(dxk)
            dr_pools.append(drk)
            pieces.append([slices[0]] + [lax.ppermute(slices[m], "fsdp", [(i, i ^ m) for i in range(n_fs)])
                                         for m in range(1, n_fs)])
        dx_part, dr_part = combine_rows(cnt_flat, off_flat, pos, dx_pools, dr_pools, region)
        grad_x, dr_home = collect(dx_part, dr_part, n_fs, n_ep)
        dr_home = dr_home.reshape(n_fs, n_ep, n_loc, tok).transpose(1, 0, 2, 3).reshape(experts, tok)
        hit = expert_ids.T[:, None, :] == jnp.arange(experts, dtype=jnp.int32)[None, :, None]
        route_grad = jnp.sum(jnp.where(hit, dr_home[None], 0.0), axis=1).T
        grads = None
        for k in range(n_loc):
            grads = place(k, n_loc, me.reshape(1), pieces[k], grads)
        return grad_x, route_grad, *grads

    return jax.shard_map(
        body, mesh=mesh,
        in_specs=(tok_spec, tok_spec, tok_spec, tok_spec, spec_in, spec_in, spec_out),
        out_specs=(tok_spec, tok_spec, spec_in, spec_in, spec_out),
        check_vma=False)
```

```python
import functools

import jax
import jax.numpy as jnp
from jax import lax
from jax.experimental import pallas as pl
from jax.experimental.pallas import tpu as pltpu
from jax.sharding import PartitionSpec as P


CAP_FACTOR = 3
CHUNK = 128
TILE = 512
TIERS = (384, 640, 1024)
VMEM_LIMIT = 60 * 1024 * 1024
F32 = jnp.float32
BF16 = jnp.bfloat16


def capacity_of(tok_dev, top_k, experts):
    return max(8, ((CAP_FACTOR * tok_dev * top_k // experts + 7) // 8) * 8)


def up(n, m):
    return (n + m - 1) // m * m


def blocks(n, size):
    return lax.div(n + (size - 1), jnp.full_like(n, size))


def dot(a, b):
    return lax.dot_general(a, b, (((1,), (0,)), ((), ())), preferred_element_type=F32)


def dot_nt(a, b):
    return lax.dot_general(a, b, (((1,), (1,)), ((), ())), preferred_element_type=F32)


def dot_tn(a, b):
    return lax.dot_general(a, b, (((0,), (0,)), ((), ())), preferred_element_type=F32)


def route_tables(expert_ids, route_w, experts, capacity):
    tok_dev, _ = expert_ids.shape
    ids_t, w_t = expert_ids.T, route_w.T
    hit = ids_t[:, None, :] == jnp.arange(experts, dtype=jnp.int32)[None, :, None]
    chosen = jnp.any(hit, axis=0)
    weight = jnp.sum(jnp.where(hit, w_t[:, None, :], 0.0), axis=0)
    earlier = jnp.arange(tok_dev)[:, None] < jnp.arange(tok_dev)[None, :]
    before = dot(chosen.astype(BF16), earlier.astype(BF16))
    position = jnp.where(chosen & (before < capacity), before, -1.0)
    return position, weight


def one_hot_block(pos_row, first, size):
    return lax.broadcasted_iota(jnp.int32, (size, pos_row.shape[1]), 0) + first == pos_row


def tiers(rows, limit, work):
    work(0, TIERS[0])
    for first, last in zip(TIERS, (*TIERS[1:], limit)):
        pl.when(rows > first)(functools.partial(work, first, last - first))


def aligned(v, m=16):
    return pl.multiple_of(v, m)


def gather_kernel(n_src, n_loc, region, slots, with_r, *refs):
    if with_r:
        (cnt, off, pos_ref, r_ref, src_ref, out, r_out, hot, stage, pool, rstage, rpool, sem) = refs
    else:
        (cnt, off, pos_ref, src_ref, out, hot, stage, pool, sem) = refs
    s = pl.program_id(0)
    base = jnp.int32(0)
    starts = []
    for k in range(n_loc):
        n = cnt[s * n_loc + k]
        starts.append(base)
        pos_row = pos_ref[0, k:k + 1, :]

        def build(first, size, base=base, pos_row=pos_row, k=k):
            m = one_hot_block(pos_row, first, size)
            at = pl.ds(aligned(base + first), size)
            hot[at, :] = jnp.where(m, 1.0, 0.0).astype(BF16)
            if with_r:
                r = jnp.sum(jnp.where(m, r_ref[0, k:k + 1, :], 0.0), axis=1, keepdims=True)
                rstage[at, :] = jnp.broadcast_to(r, (size, 128))

        build(0, CHUNK)
        pl.when(n > CHUNK)(functools.partial(build, CHUNK, slots - CHUNK))
        base = base + blocks(n, 16) * 16

    def mm(first, size):
        at = pl.ds(first, size)
        stage[at, :] = dot(hot[at, :], src_ref[...]).astype(BF16)

    tiers(base, hot.shape[0], mm)

    for k in range(n_loc):
        n = cnt[s * n_loc + k]
        to = off[s * n_loc + k] + k * region

        def move(first, size, start=starts[k], to=to):
            dst = pl.ds(aligned(to + first), size)
            frm = pl.ds(aligned(start + first), size)
            pool[dst, :] = stage[frm, :]
            if with_r:
                rpool[dst, :] = rstage[frm, :]

        move(0, CHUNK)
        pl.when(n > CHUNK)(functools.partial(move, CHUNK, slots - CHUNK))

    @pl.when(s == n_src - 1)
    def _():
        def copies(k, i):
            at = pl.ds(aligned(k * region + i * TILE, TILE), TILE)
            made = [pltpu.make_async_copy(pool.at[at], out.at[at], sem)]
            if with_r:
                made.append(pltpu.make_async_copy(rpool.at[at], r_out.at[at], sem))
            return made

        tiles = []
        for k in range(n_loc):
            end = off[s * n_loc + k] + blocks(cnt[s * n_loc + k], 16) * 16
            at = pl.ds(aligned(k * region + end), TILE)
            pool[at, :] = jnp.zeros((TILE, pool.shape[1]), BF16)
            if with_r:
                rpool[at, :] = jnp.zeros((TILE, 128), F32)
            tiles.append(jnp.maximum(1, blocks(end, TILE)))
        for k in range(n_loc):
            def start(i, carry, k=k):
                for copy in copies(k, i):
                    copy.start()
                return carry

            lax.fori_loop(0, tiles[k], start, 0)
        for k in range(n_loc):
            def wait(i, carry, k=k):
                for copy in copies(k, i):
                    copy.wait()
                return carry

            lax.fori_loop(0, tiles[k], wait, 0)


def gather_rows(src, cnt, off, pos, r, region):
    n_src, n_loc, tok = pos.shape
    d = src.shape[1] // 2
    with_r = r is not None
    rows = n_loc * region
    scr = up(n_loc * ((region - TILE) // n_src) + CHUNK, CHUNK)
    table = pl.BlockSpec((1, n_loc, tok), lambda s, *_: (s, 0, 0))
    in_specs = [table] + ([table] if with_r else []) + [pl.BlockSpec((tok, d), lambda s, *_: (s, 1 if with_r else 0))]
    out_shape = [jax.ShapeDtypeStruct((rows, d), BF16)]
    scratch = [pltpu.VMEM((scr, tok), BF16), pltpu.VMEM((scr, d), BF16), pltpu.VMEM((rows, d), BF16)]
    if with_r:
        out_shape.append(jax.ShapeDtypeStruct((rows, 128), F32))
        scratch += [pltpu.VMEM((scr, 128), F32), pltpu.VMEM((rows, 128), F32)]
    out = pl.pallas_call(
        functools.partial(gather_kernel, n_src, n_loc, region, up((region - TILE) // n_src, CHUNK), with_r),
        out_shape=out_shape,
        grid_spec=pltpu.PrefetchScalarGridSpec(
            num_scalar_prefetch=2, grid=(n_src,), in_specs=in_specs,
            out_specs=[pl.BlockSpec(memory_space=pl.ANY)] * len(out_shape),
            scratch_shapes=scratch + [pltpu.SemaphoreType.DMA]),
        compiler_params=pltpu.CompilerParams(vmem_limit_bytes=VMEM_LIMIT, dimension_semantics=("arbitrary",)),
        cost_estimate=pl.CostEstimate(flops=2 * 12000 * tok * d, bytes_accessed=n_src * tok * d * 4, transcendentals=0),
        name="gather_r" if with_r else "gather_x",
    )(*([cnt, off, pos] + ([r] if with_r else []) + [src]))
    return out if with_r else out[0]


def expert_kernel(n_fs, info, x_ref, dy_ref, r_ref, *refs):
    own, peers, refs = refs[:3], refs[3:n_fs + 2], refs[n_fs + 2:]
    (dx_ref, dr_ref), outs, refs = refs[:2], refs[2:n_fs + 2], refs[n_fs + 2:]
    w1_ref, w3_ref, w2t, a_buf, dh1_buf, dh3_buf, dw1, dw3, dw2t = refs
    i = pl.program_id(0)
    d, f = w1_ref.shape
    dsl = d // n_fs

    @pl.when(i == 0)
    def _():
        dw1[...] = jnp.zeros_like(dw1)
        dw3[...] = jnp.zeros_like(dw3)
        dw2t[...] = jnp.zeros_like(dw2t)
        for m in range(n_fs):
            at = pl.ds(aligned((info[2] ^ m) * dsl, dsl), dsl)
            for t, whole in enumerate((w1_ref, w3_ref, w2t)):
                whole[at, :] = peers[m - 1][0, t] if m else own[t][0]

    def tile(m):
        x, dy = x_ref[:m, :], dy_ref[:m, :]
        dy_wide = dy.astype(F32)
        g = (r_ref[:m, 0:1] * dy_wide).astype(BF16)
        step = 256
        for c in range(0, f, step):
            cs = slice(c, c + step)
            h1 = dot(x, w1_ref[:, cs])
            h3 = dot(x, w3_ref[:, cs])
            da = dot(g, w2t[:, cs])
            s = jax.nn.sigmoid(h1)
            hs = h1 * s
            a_buf[:m, cs] = (hs * h3).astype(BF16)
            dh1_buf[:m, cs] = (da * h3 * s * (1.0 + h1 * (1.0 - s))).astype(BF16)
            dh3_buf[:m, cs] = (da * hs).astype(BF16)
        y = dot_nt(a_buf[:m, :], w2t[...])
        dr = jnp.sum(dy_wide * y, axis=1, keepdims=True)
        dr_ref[:m, :] = jnp.broadcast_to(dr, (m, 128))
        dx_ref[:m, :] = (dot_nt(dh1_buf[:m, :], w1_ref[...]) + dot_nt(dh3_buf[:m, :], w3_ref[...])).astype(BF16)
        dw1[...] += dot_tn(x, dh1_buf[:m, :])
        dw3[...] += dot_tn(x, dh3_buf[:m, :])
        dw2t[...] += dot_tn(g, a_buf[:m, :])

    left = info[0] - i * TILE

    @pl.when(left > TILE // 2)
    def _():
        tile(TILE)

    @pl.when((i < info[1]) & (left <= TILE // 2))
    def _():
        tile(TILE // 2)
        dx_ref[TILE // 2:, :] = jnp.zeros((TILE // 2, d), BF16)
        dr_ref[TILE // 2:, :] = jnp.zeros((TILE // 2, 128), F32)

    @pl.when(i == info[1] - 1)
    def _():
        for m in range(n_fs):
            at = pl.ds(aligned((info[2] ^ m) * dsl, dsl), dsl)
            for t, acc in enumerate((dw1, dw3, dw2t)):
                outs[m][t] = acc[at, :]


def expert_call(k, group_at, n_loc, info, x_pool, dy_pool, r_pool, own, peers, region):
    n_fs, (_, _, dsl, f) = len(peers) + 1, peers[0].shape
    d = n_fs * dsl
    first = k * (region // TILE)
    row_map = lambda i, info: (first + jnp.minimum(i, info[1] - 1), 0)
    out_map = lambda i, info: (jnp.minimum(i, info[1] - 1), 0)
    whole3 = lambda i, info: (0, 0, 0)
    mine = lambda i, info: (info[2] * n_loc + k, 0, 0)
    return pl.pallas_call(
        functools.partial(expert_kernel, n_fs),
        out_shape=[jax.ShapeDtypeStruct((region, d), BF16), jax.ShapeDtypeStruct((region, 128), F32)]
        + [jax.ShapeDtypeStruct((3, dsl, f), F32)] * n_fs,
        grid_spec=pltpu.PrefetchScalarGridSpec(
            num_scalar_prefetch=1, grid=(region // TILE - 1,),
            in_specs=[pl.BlockSpec((TILE, d), row_map), pl.BlockSpec((TILE, d), row_map), pl.BlockSpec((TILE, 128), row_map),
                      *[pl.BlockSpec((1, dsl, f), mine)] * 2, pl.BlockSpec((1, dsl, f), lambda i, info: (k, 0, 0)),
                      *[pl.BlockSpec((1, 3, dsl, f), lambda i, info: (group_at, 0, 0, 0))] * (n_fs - 1)],
            out_specs=[pl.BlockSpec((TILE, d), out_map), pl.BlockSpec((TILE, 128), out_map)]
            + [pl.BlockSpec((3, dsl, f), whole3)] * n_fs,
            scratch_shapes=[pltpu.VMEM((d, f), BF16)] * 3 + [pltpu.VMEM((TILE, f), BF16)] * 3 + [pltpu.VMEM((d, f), F32)] * 3),
        compiler_params=pltpu.CompilerParams(vmem_limit_bytes=VMEM_LIMIT, dimension_semantics=("arbitrary",)),
        cost_estimate=pl.CostEstimate(flops=18 * 3000 * d * f, bytes_accessed=24 * d * f, transcendentals=3000 * f),
    )(info, x_pool, dy_pool, r_pool, *own, *peers)


def place_kernel(n_fs, n_loc, ks, first, me, *refs):
    n_pieces = n_fs * len(ks)
    pieces, refs = refs[:n_pieces], refs[n_pieces + (0 if first else 3):]
    outs, (held, turned, in_sem, out_sem) = refs[:3], refs[3:]
    reads = [pltpu.make_async_copy(piece, held.at[n], in_sem.at[n]) for n, piece in enumerate(pieces)]
    for copy in reads:
        copy.start()
    writes = []
    for n, copy in enumerate(reads):
        copy.wait()
        to = (me[0] ^ n % n_fs) * n_loc + ks[n // n_fs]
        for t in range(2):
            writes.append(pltpu.make_async_copy(held.at[n, t], outs[t].at[to], out_sem))
            writes[-1].start()
        turned[n] = held[n, 2].T
        writes.append(pltpu.make_async_copy(turned.at[n], outs[2].at[to], out_sem))
        writes[-1].start()
    for copy in writes:
        copy.wait()


def place(ks, n_loc, me, pieces, grads):
    n_fs = len(pieces) // len(ks)
    _, dsl, f = pieces[0].shape
    hbm = pl.BlockSpec(memory_space=pl.ANY)
    first = grads is None
    n = len(pieces)
    shapes = [(n_fs * n_loc, dsl, f)] * 2 + [(n_fs * n_loc, f, dsl)]
    return pl.pallas_call(
        functools.partial(place_kernel, n_fs, n_loc, ks, first),
        out_shape=[jax.ShapeDtypeStruct(v, F32) for v in shapes],
        in_specs=[pl.BlockSpec(memory_space=pltpu.SMEM)] + [hbm] * (n if first else n + 3),
        out_specs=[hbm] * 3,
        scratch_shapes=[pltpu.VMEM((n, 3, dsl, f), F32), pltpu.VMEM((n, f, dsl), F32),
                        pltpu.SemaphoreType.DMA((n,)), pltpu.SemaphoreType.DMA],
        input_output_aliases={} if first else {n + 1 + t: t for t in range(3)},
        compiler_params=pltpu.CompilerParams(vmem_limit_bytes=VMEM_LIMIT),
        cost_estimate=pl.CostEstimate(flops=0, bytes_accessed=6 * 4 * n * dsl * f, transcendentals=0),
    )(me, *pieces, *([] if first else grads))


def combine_kernel(n_src, n_loc, slots, cnt, off, pos_ref, *refs):
    dx_in, dr_in = refs[:n_loc], refs[n_loc:2 * n_loc]
    out, dr_out, hot, stage, pool, rpool, sem = refs[2 * n_loc:]
    s = pl.program_id(0)
    tok = pos_ref.shape[2]
    d = pool.shape[2]

    @pl.when(s == 0)
    def _():
        def copies(k, i):
            at = pl.ds(aligned(i * TILE, TILE), TILE)
            return [pltpu.make_async_copy(dx_in[k].at[at], pool.at[k, at], sem),
                    pltpu.make_async_copy(dr_in[k].at[at], rpool.at[k, at], sem)]

        tiles = []
        for k in range(n_loc):
            last = (n_src - 1) * n_loc + k
            end = off[last] + blocks(cnt[last], 16) * 16
            tiles.append(jnp.maximum(1, blocks(end, TILE)))
        for k in range(n_loc):
            def start(i, carry, k=k):
                for copy in copies(k, i):
                    copy.start()
                return carry

            lax.fori_loop(0, tiles[k], start, 0)
            at = pl.ds(aligned(tiles[k] * TILE), TILE)
            pool[k, at, :] = jnp.zeros((TILE, d), BF16)
            rpool[k, at, :] = jnp.zeros((TILE, 128), F32)
        for k in range(n_loc):
            def wait(i, carry, k=k):
                for copy in copies(k, i):
                    copy.wait()
                return carry

            lax.fori_loop(0, tiles[k], wait, 0)

    dr_out[...] = jnp.zeros_like(dr_out)
    base = jnp.int32(0)
    for k in range(n_loc):
        n = cnt[s * n_loc + k]
        frm = off[s * n_loc + k]
        pos_row = pos_ref[0, k:k + 1, :]

        def build(first, size, base=base, frm=frm, pos_row=pos_row, k=k):
            m = one_hot_block(pos_row, first, size)
            at = pl.ds(aligned(base + first), size)
            src = pl.ds(aligned(frm + first), size)
            hot[at, :] = jnp.where(m, 1.0, 0.0).astype(BF16)
            stage[at, :] = pool[k, src, :]
            r = jnp.concatenate([rpool[k, src, :]] * (tok // 128), axis=1)
            dr_out[0, k:k + 1, :] += jnp.sum(jnp.where(m, r, 0.0), axis=0, keepdims=True)

        build(0, CHUNK)
        pl.when(n > CHUNK)(functools.partial(build, CHUNK, slots - CHUNK))
        base = base + blocks(n, 16) * 16

    def clear(size):
        tail = pl.ds(aligned(base), size)
        hot[tail, :] = jnp.zeros((size, tok), BF16)
        stage[tail, :] = jnp.zeros((size, d), BF16)

    clear(TIERS[0])
    pl.when(base > TIERS[1])(functools.partial(clear, hot.shape[0] - n_loc * slots))

    def mm(first, size):
        at = pl.ds(first, size)
        part = dot_tn(hot[at, :], stage[at, :])
        out[...] = part if first == 0 else out[...] + part

    tiers(base, n_loc * slots, mm)


def combine_rows(cnt, off, pos, dx_pools, dr_pools, region):
    n_src, n_loc, tok = pos.shape
    d = dx_pools[0].shape[1]
    slots = up((region - TILE) // n_src, CHUNK)
    scr = n_loc * slots + TILE
    hbm = pl.BlockSpec(memory_space=pl.ANY)
    return pl.pallas_call(
        functools.partial(combine_kernel, n_src, n_loc, slots),
        out_shape=[jax.ShapeDtypeStruct((n_src * tok, d), F32), jax.ShapeDtypeStruct((n_src, n_loc, tok), F32)],
        grid_spec=pltpu.PrefetchScalarGridSpec(
            num_scalar_prefetch=2, grid=(n_src,),
            in_specs=[pl.BlockSpec((1, n_loc, tok), lambda s, *_: (s, 0, 0))] + [hbm] * (2 * n_loc),
            out_specs=[pl.BlockSpec((tok, d), lambda s, *_: (s, 0)),
                       pl.BlockSpec((1, n_loc, tok), lambda s, *_: (s, 0, 0))],
            scratch_shapes=[pltpu.VMEM((scr, tok), BF16), pltpu.VMEM((scr, d), BF16),
                            pltpu.VMEM((n_loc, region, d), BF16), pltpu.VMEM((n_loc, region, 128), F32),
                            pltpu.SemaphoreType.DMA]),
        compiler_params=pltpu.CompilerParams(vmem_limit_bytes=VMEM_LIMIT, dimension_semantics=("arbitrary",)),
        cost_estimate=pl.CostEstimate(flops=2 * 12000 * tok * d, bytes_accessed=n_src * tok * d * 4, transcendentals=0),
        name="combine",
    )(cnt, off, pos, *dx_pools, *dr_pools)


MESH = pl.DeviceIdType.MESH
HOPS = ((0, 2), (1, 0), (2, 0))
SIBLING = (0, 1)
SPREAD_ORDERS = ((1, 2, 0), (2, 1, 0), (0, 1, 2), (0, 2, 1))
COLLECT_ORDERS = ((0, 1, 2), (0, 2, 1), (1, 2, 0), (2, 1, 0))


def parts_of(tok):
    long = tok * 5 // 16 // 16 * 16
    return long, long, tok // 2 - long, tok // 2 - long


def here():
    return lax.axis_index("fsdp"), lax.axis_index("ep")


def peer_of(hop):
    f, p = here()
    return {"fsdp": f ^ hop[0], "ep": p ^ hop[1]}


def block_of(bits, core=0):
    f, p = here()
    for axis in range(3):
        if bits >> axis & 1:
            f, p = f ^ HOPS[axis][0], p ^ HOPS[axis][1]
    return f * 4 + (p ^ core)


def enter(n_fs, n_ep):
    barrier = pltpu.get_barrier_semaphore()
    for df in range(n_fs):
        for dp in range(n_ep):
            if df or dp:
                pl.semaphore_signal(barrier, inc=1, device_id=peer_of((df, dp)), device_id_type=MESH)
    pl.semaphore_wait(barrier, n_fs * n_ep - 1)


def exchange(n_fs, n_ep, src, dst, send, recv):
    f, p = here()
    copies = []
    for df in range(n_fs):
        for dp in range(n_ep):
            if df or dp:
                n = df * n_ep + dp
                copies.append(pltpu.make_async_remote_copy(
                    src_ref=src.at[(f ^ df) * n_ep + (p ^ dp)], dst_ref=dst.at[f * n_ep + p],
                    send_sem=send.at[n], recv_sem=recv.at[n], device_id=peer_of((df, dp)), device_id_type=MESH))
                copies[-1].start()
    return copies


def spread_kernel(n_fs, n_ep, n_loc, parts, x_ref, dy_ref, table_ref, wg_ref, wu_ref, wd_ref, full, table_all, *refs):
    n_out = 2 * (n_fs - 1)
    own_down, w_out, refs = refs[0], refs[1:n_out + 1], refs[n_out + 1:]
    own, send, recv, c_send, c_recv, t_send, t_recv, own_sem, w_buf, down_buf, in_sem, out_sem, w_send, w_recv = refs
    tok, d = x_ref.shape
    mine = block_of(0)
    local = []
    for n, src in enumerate((x_ref, dy_ref)):
        local.append(pltpu.make_async_copy(src, own.at[:, pl.ds(n * d, d)], own_sem.at[n]))
        local[-1].start()
    enter(n_fs, n_ep)
    for copy in local:
        copy.wait()
    local = [pltpu.make_async_copy(own, full.at[pl.ds(aligned(mine * tok, tok), tok)], own_sem.at[0]),
             pltpu.make_async_copy(table_ref.at[mine], table_all.at[mine], own_sem.at[2])]
    starts = [sum(parts[:q]) for q in range(len(parts))]
    sem_at = {}
    inbound = {}

    def send_on(q, phase, bits):
        to = pl.ds(aligned(block_of(bits) * tok + starts[q], 16), parts[q])
        src = own.at[pl.ds(starts[q], parts[q])] if bits == 0 else full.at[to]
        n = sem_at.setdefault((q, phase, bits), len(sem_at))
        copy = pltpu.make_async_remote_copy(
            src_ref=src, dst_ref=full.at[to], send_sem=send.at[n], recv_sem=recv.at[n],
            device_id=peer_of(HOPS[SPREAD_ORDERS[q][phase]]), device_id_type=MESH)
        copy.start()
        inbound[(q, phase, bits)] = copy

    shared = []

    def share(q, bits):
        to = pl.ds(aligned(block_of(bits) * tok + starts[q], 16), parts[q])
        src = own.at[pl.ds(starts[q], parts[q])] if bits == 0 else full.at[to]
        n = len(shared)
        copy = pltpu.make_async_remote_copy(
            src_ref=src, dst_ref=full.at[to], send_sem=c_send.at[n], recv_sem=c_recv.at[n],
            device_id=peer_of(SIBLING), device_id_type=MESH)
        copy.start()
        shared.append(copy)

    for phase in range(3):
        for q in range(len(parts)):
            send_on(q, phase, 0)
    for q in range(len(parts)):
        share(q, 0)
    for copy in local:
        copy.start()
    pending = exchange(n_fs, n_ep, table_ref, table_all, t_send, t_recv)
    f, _ = here()
    packs = []
    for k in range(n_loc):
        for m in range(n_fs):
            n = k * n_fs + m
            at = (f ^ m) * n_loc + k
            packs.append([pltpu.make_async_copy(wd_ref.at[at], down_buf.at[n], in_sem.at[3 * n])])
            if m:
                packs[-1] += [pltpu.make_async_copy(w.at[at], w_buf.at[n, t], in_sem.at[3 * n + 1 + t])
                              for t, w in enumerate((wg_ref, wu_ref))]
            for copy in packs[-1]:
                copy.start()
    for n in range(n_loc * n_fs):
        for copy in packs[n]:
            copy.wait()
        w_buf[n, 2] = down_buf[n].T
        k, m = n // n_fs, n % n_fs
        if m == 0:
            copy = pltpu.make_async_copy(w_buf.at[n, 2], own_down.at[k], out_sem.at[n])
        elif k == 0:
            continue
        else:
            copy = pltpu.make_async_copy(w_buf.at[n], w_out[n_fs + m - 2].at[k - 1], out_sem.at[n])
        copy.start()
        local.append(copy)
    for phase in range(3):
        for q in range(len(parts)):
            held = [0]
            for axis in SPREAD_ORDERS[q][:phase]:
                held += [b | 1 << axis for b in held]
            for b in held:
                inbound[(q, phase, b)].wait_recv()
                got = b | 1 << SPREAD_ORDERS[q][phase]
                for later in range(phase + 1, 3):
                    send_on(q, later, got)
                share(q, got)
        if phase == 1:
            for m in range(1, n_fs):
                pending.append(pltpu.make_async_remote_copy(
                    src_ref=w_buf.at[m], dst_ref=w_out[m - 1].at[0], send_sem=w_send.at[m - 1], recv_sem=w_recv.at[m - 1],
                    device_id=peer_of((m, 0)), device_id_type=MESH))
                pending[-1].start()
    for copy in inbound.values():
        copy.wait_send()
    for copy in shared:
        copy.wait()
    for copy in pending:
        copy.wait()
    for copy in local:
        copy.wait()


def spread(x_tok, dy_tok, table, w_gate, w_up, w_down, n_fs, n_ep):
    n_dev = n_fs * n_ep
    tok, d = x_tok.shape
    exp_local, dsl, f = w_gate.shape
    n_loc = exp_local // n_fs
    n_slices, groups = n_loc * n_fs, [1] * (n_fs - 1) + [n_loc - 1] * (n_fs - 1)
    parts = parts_of(tok)
    vmem, hbm = pl.BlockSpec(memory_space=pltpu.VMEM), pl.BlockSpec(memory_space=pl.ANY)
    dma = pltpu.SemaphoreType.DMA
    return pl.pallas_call(
        functools.partial(spread_kernel, n_fs, n_ep, n_loc, parts),
        out_shape=[jax.ShapeDtypeStruct((n_dev * tok, 2 * d), x_tok.dtype), jax.ShapeDtypeStruct(table.shape, table.dtype)]
        + [jax.ShapeDtypeStruct((n_loc, dsl, f), BF16)] + [jax.ShapeDtypeStruct((g, 3, dsl, f), BF16) for g in groups],
        in_specs=[hbm] * 2 + [vmem] + [hbm] * 3, out_specs=[hbm] * (3 + len(groups)),
        scratch_shapes=[pltpu.VMEM((tok, 2 * d), BF16), dma((28,)), dma((28,)), dma((32,)), dma((32,)), dma((n_dev,)), dma((n_dev,)),
                        dma((3,)), pltpu.VMEM((n_slices, 3, dsl, f), BF16), pltpu.VMEM((n_slices, f, dsl), BF16),
                        dma((3 * n_slices,)), dma((n_slices,)), dma((n_fs - 1,)), dma((n_fs - 1,))],
        compiler_params=pltpu.CompilerParams(collective_id=0, has_side_effects=True, vmem_limit_bytes=VMEM_LIMIT),
        cost_estimate=pl.CostEstimate(flops=0, bytes_accessed=8 * n_dev * tok * d, transcendentals=0),
        name="spread",
    )(x_tok, dy_tok, table, w_gate, w_up, w_down)


def collect_kernel(n_fs, n_ep, parts, part_ref, dr_ref, gx_ref, dr_home, acc, sib, got,
                   c_send, c_recv, send, recv, t_send, t_recv, own_sem):
    tok = gx_ref.shape[0]
    mine = block_of(0)
    enter(n_fs, n_ep)
    drs = exchange(n_fs, n_ep, dr_ref, dr_home, t_send, t_recv)
    local_dr = pltpu.make_async_copy(dr_ref.at[mine], dr_home.at[mine], own_sem.at[8])
    local_dr.start()
    order = (7, 3, 5, 6, 1, 2, 4, 0)
    loads, shares = {}, {}
    for bits in order:
        theirs = pl.ds(aligned(block_of(bits, 1) * tok, tok), tok)
        shares[bits] = pltpu.make_async_remote_copy(
            src_ref=part_ref.at[theirs], dst_ref=sib.at[bits], send_sem=c_send.at[bits], recv_sem=c_recv.at[bits],
            device_id=peer_of(SIBLING), device_id_type=MESH)
        shares[bits].start()
        ours = pl.ds(aligned(block_of(bits) * tok, tok), tok)
        loads[bits] = pltpu.make_async_copy(part_ref.at[ours], acc.at[bits], own_sem.at[bits])
        loads[bits].start()
    starts = [sum(parts[:q]) for q in range(len(parts))]
    slots = [(q, bits) for q in range(len(parts)) for bits in range(1, 8)]
    hops = {}

    def phase_of(q, bits):
        return next(n for n in range(3) if bits >> COLLECT_ORDERS[q][n] & 1)

    def send_off(q, bits):
        n = slots.index((q, bits))
        rows = pl.ds(starts[q], parts[q])
        hops[(q, bits)] = pltpu.make_async_remote_copy(
            src_ref=acc.at[bits, rows], dst_ref=got.at[bits - 1, rows], send_sem=send.at[n], recv_sem=recv.at[n],
            device_id=peer_of(HOPS[COLLECT_ORDERS[q][phase_of(q, bits)]]), device_id_type=MESH)
        hops[(q, bits)].start()

    def add_arrival(q, bits, phase):
        frm = bits | 1 << COLLECT_ORDERS[q][phase]
        hops[(q, frm)].wait_recv()
        rows = slice(starts[q], starts[q] + parts[q])
        acc[bits, rows, :] = acc[bits, rows, :] + got[frm - 1, rows, :]

    for bits in order:
        loads[bits].wait()
        shares[bits].wait_recv()
        acc[bits] = acc[bits] + sib[bits]
        for q in range(len(parts)):
            if bits and phase_of(q, bits) == 0:
                send_off(q, bits)
    for phase in (1, 2):
        for q in range(len(parts)):
            for bits in range(1, 8):
                if phase_of(q, bits) == phase:
                    for earlier in range(phase):
                        add_arrival(q, bits, earlier)
                    send_off(q, bits)
    for q in range(len(parts)):
        for phase in range(3):
            add_arrival(q, 0, phase)
        rows = slice(starts[q], starts[q] + parts[q])
        gx_ref[rows, :] = acc[0, rows, :].astype(gx_ref.dtype)
    for bits in order:
        shares[bits].wait_send()
    for copy in hops.values():
        copy.wait_send()
    for copy in drs:
        copy.wait()
    local_dr.wait()


def collect(dx_part, dr_part, n_fs, n_ep):
    n_dev = n_fs * n_ep
    tok, d = dx_part.shape[0] // n_dev, dx_part.shape[1]
    parts = parts_of(tok)
    vmem, hbm = pl.BlockSpec(memory_space=pltpu.VMEM), pl.BlockSpec(memory_space=pl.ANY)
    dma = pltpu.SemaphoreType.DMA
    return pl.pallas_call(
        functools.partial(collect_kernel, n_fs, n_ep, parts),
        out_shape=[jax.ShapeDtypeStruct((tok, d), BF16), jax.ShapeDtypeStruct(dr_part.shape, F32)],
        in_specs=[hbm, vmem], out_specs=[vmem, vmem],
        scratch_shapes=[pltpu.VMEM((8, tok, d), F32), pltpu.VMEM((8, tok, d), F32), pltpu.VMEM((7, tok, d), F32),
                        dma((8,)), dma((8,)), dma((28,)), dma((28,)), dma((n_dev,)), dma((n_dev,)), dma((9,))],
        compiler_params=pltpu.CompilerParams(collective_id=1, has_side_effects=True, vmem_limit_bytes=VMEM_LIMIT),
        cost_estimate=pl.CostEstimate(flops=0, bytes_accessed=8 * n_dev * tok * d, transcendentals=0),
        name="collect",
    )(dx_part, dr_part)


def solution(mesh):
    n_ep, n_fs = mesh.shape["ep"], mesh.shape["fsdp"]
    n_dev = n_ep * n_fs
    both = ("fsdp", "ep")
    tok_spec = P(both, None)
    spec_in = P("ep", "fsdp", None)
    spec_out = P("ep", None, "fsdp")

    def body(x_tok, dy_tok, expert_ids, route_w, w_gate, w_up, w_down):
        tok, top_k = expert_ids.shape
        exp_local, _, _ = w_gate.shape
        n_loc = exp_local // n_fs
        experts = exp_local * n_ep
        capacity = capacity_of(tok, top_k, experts)
        region = n_dev * up(capacity, 16) + TILE

        position, weight = route_tables(expert_ids, route_w, experts, capacity)
        table = jnp.stack([position, weight], axis=1).reshape(n_ep, n_fs, n_loc, 2, tok)
        table = table.transpose(1, 0, 2, 3, 4).reshape(n_dev, n_loc * 2, tok)
        xdy_all, table, own_down, *packed = spread(x_tok, dy_tok, table, w_gate, w_up, w_down, n_fs, n_ep)
        table = table.reshape(n_dev, n_loc, 2, tok)
        me = lax.axis_index("fsdp").astype(jnp.int32)
        first_w, later_w = packed[:n_fs - 1], packed[n_fs - 1:]
        later_w = [lax.ppermute(later_w[m - 1], "fsdp", [(i, i ^ m) for i in range(n_fs)]) for m in range(1, n_fs)]
        weights = [first_w, later_w]

        pos = table[:, :, 0, :].astype(jnp.int32)
        r = table[:, :, 1, :]
        cnt = jnp.max(pos, axis=2) + 1
        padded = blocks(cnt, 16) * 16
        off = jnp.cumsum(padded, axis=0) - padded
        rows = jnp.sum(padded, axis=0)
        cnt_flat, off_flat = cnt.reshape(-1), off.reshape(-1)
        x_pool = gather_rows(xdy_all, cnt_flat, off_flat, pos, None, region)
        dy_pool, r_pool = gather_rows(xdy_all, cnt_flat, off_flat, pos, r, region)

        dx_pools, dr_pools, pieces = [], [], []
        for k in range(n_loc):
            info = jnp.stack([rows[k], jnp.maximum(1, blocks(rows[k], TILE)), me])
            dxk, drk, *slices = expert_call(
                k, max(k - 1, 0), n_loc, info, x_pool, dy_pool, r_pool, (w_gate, w_up, own_down),
                weights[min(k, 1)], region)
            dx_pools.append(dxk)
            dr_pools.append(drk)
            pieces.append([slices[0]] + [lax.ppermute(slices[m], "fsdp", [(i, i ^ m) for i in range(n_fs)])
                                         for m in range(1, n_fs)])
        dx_part, dr_part = combine_rows(cnt_flat, off_flat, pos, dx_pools, dr_pools, region)
        grad_x, dr_home = collect(dx_part, dr_part, n_fs, n_ep)
        dr_home = dr_home.reshape(n_fs, n_ep, n_loc, tok).transpose(1, 0, 2, 3).reshape(experts, tok)
        hit = expert_ids.T[:, None, :] == jnp.arange(experts, dtype=jnp.int32)[None, :, None]
        route_grad = jnp.sum(jnp.where(hit, dr_home[None], 0.0), axis=1).T
        grads = None
        for ks in (tuple(range(n_loc // 2)), tuple(range(n_loc // 2, n_loc))):
            grads = place(ks, n_loc, me.reshape(1), [piece for k in ks for piece in pieces[k]], grads)
        return grad_x, route_grad, *grads

    return jax.shard_map(
        body, mesh=mesh,
        in_specs=(tok_spec, tok_spec, tok_spec, tok_spec, spec_in, spec_in, spec_out),
        out_specs=(tok_spec, tok_spec, spec_in, spec_in, spec_out),
        check_vma=False)
```

```python
import functools

import jax
import jax.numpy as jnp
from jax import lax
from jax.experimental import pallas as pl
from jax.experimental.pallas import tpu as pltpu
from jax.sharding import PartitionSpec as P


CAP_FACTOR = 3
CHUNK = 128
TILE = 512
TIERS = (384, 640, 1024)
VMEM_LIMIT = 60 * 1024 * 1024
F32 = jnp.float32
BF16 = jnp.bfloat16


def capacity_of(tok_dev, top_k, experts):
    return max(8, ((CAP_FACTOR * tok_dev * top_k // experts + 7) // 8) * 8)


def up(n, m):
    return (n + m - 1) // m * m


def blocks(n, size):
    return lax.div(n + (size - 1), jnp.full_like(n, size))


def dot(a, b):
    return lax.dot_general(a, b, (((1,), (0,)), ((), ())), preferred_element_type=F32)


def dot_nt(a, b):
    return lax.dot_general(a, b, (((1,), (1,)), ((), ())), preferred_element_type=F32)


def dot_tn(a, b):
    return lax.dot_general(a, b, (((0,), (0,)), ((), ())), preferred_element_type=F32)


def route_tables(expert_ids, route_w, experts, capacity):
    tok_dev, _ = expert_ids.shape
    ids_t, w_t = expert_ids.T, route_w.T
    hit = ids_t[:, None, :] == jnp.arange(experts, dtype=jnp.int32)[None, :, None]
    chosen = jnp.any(hit, axis=0)
    weight = jnp.sum(jnp.where(hit, w_t[:, None, :], 0.0), axis=0)
    earlier = jnp.arange(tok_dev)[:, None] < jnp.arange(tok_dev)[None, :]
    before = dot(chosen.astype(BF16), earlier.astype(BF16))
    position = jnp.where(chosen & (before < capacity), before, -1.0)
    return position, weight


def one_hot_block(pos_row, first, size):
    return lax.broadcasted_iota(jnp.int32, (size, pos_row.shape[1]), 0) + first == pos_row


def tiers(rows, limit, work):
    work(0, TIERS[0])
    for first, last in zip(TIERS, (*TIERS[1:], limit)):
        pl.when(rows > first)(functools.partial(work, first, last - first))


def aligned(v, m=16):
    return pl.multiple_of(v, m)


def gather_kernel(n_src, n_loc, region, slots, with_r, *refs):
    if with_r:
        (cnt, off, pos_ref, r_ref, src_ref, out, r_out, hot, stage, pool, rstage, rpool, sem) = refs
    else:
        (cnt, off, pos_ref, src_ref, out, hot, stage, pool, sem) = refs
    s = pl.program_id(0)
    base = jnp.int32(0)
    starts = []
    for k in range(n_loc):
        n = cnt[s * n_loc + k]
        starts.append(base)
        pos_row = pos_ref[0, k:k + 1, :]

        def build(first, size, base=base, pos_row=pos_row, k=k):
            m = one_hot_block(pos_row, first, size)
            at = pl.ds(aligned(base + first), size)
            hot[at, :] = jnp.where(m, 1.0, 0.0).astype(BF16)
            if with_r:
                r = jnp.sum(jnp.where(m, r_ref[0, k:k + 1, :], 0.0), axis=1, keepdims=True)
                rstage[at, :] = jnp.broadcast_to(r, (size, 128))

        build(0, CHUNK)
        pl.when(n > CHUNK)(functools.partial(build, CHUNK, slots - CHUNK))
        base = base + blocks(n, 16) * 16

    def mm(first, size):
        at = pl.ds(first, size)
        stage[at, :] = dot(hot[at, :], src_ref[...]).astype(BF16)

    tiers(base, hot.shape[0], mm)

    for k in range(n_loc):
        n = cnt[s * n_loc + k]
        to = off[s * n_loc + k] + k * region

        def move(first, size, start=starts[k], to=to):
            dst = pl.ds(aligned(to + first), size)
            frm = pl.ds(aligned(start + first), size)
            pool[dst, :] = stage[frm, :]
            if with_r:
                rpool[dst, :] = rstage[frm, :]

        move(0, CHUNK)
        pl.when(n > CHUNK)(functools.partial(move, CHUNK, slots - CHUNK))

    @pl.when(s == n_src - 1)
    def _():
        def copies(k, i):
            at = pl.ds(aligned(k * region + i * TILE, TILE), TILE)
            made = [pltpu.make_async_copy(pool.at[at], out.at[at], sem)]
            if with_r:
                made.append(pltpu.make_async_copy(rpool.at[at], r_out.at[at], sem))
            return made

        tiles = []
        for k in range(n_loc):
            end = off[s * n_loc + k] + blocks(cnt[s * n_loc + k], 16) * 16
            at = pl.ds(aligned(k * region + end), TILE)
            pool[at, :] = jnp.zeros((TILE, pool.shape[1]), BF16)
            if with_r:
                rpool[at, :] = jnp.zeros((TILE, 128), F32)
            tiles.append(jnp.maximum(1, blocks(end, TILE)))
        for k in range(n_loc):
            def start(i, carry, k=k):
                for copy in copies(k, i):
                    copy.start()
                return carry

            lax.fori_loop(0, tiles[k], start, 0)
        for k in range(n_loc):
            def wait(i, carry, k=k):
                for copy in copies(k, i):
                    copy.wait()
                return carry

            lax.fori_loop(0, tiles[k], wait, 0)


def gather_rows(src, cnt, off, pos, r, region):
    n_src, n_loc, tok = pos.shape
    d = src.shape[1] // 2
    with_r = r is not None
    rows = n_loc * region
    scr = up(n_loc * ((region - TILE) // n_src) + CHUNK, CHUNK)
    table = pl.BlockSpec((1, n_loc, tok), lambda s, *_: (s, 0, 0))
    in_specs = [table] + ([table] if with_r else []) + [pl.BlockSpec((tok, d), lambda s, *_: (s, 1 if with_r else 0))]
    out_shape = [jax.ShapeDtypeStruct((rows, d), BF16)]
    scratch = [pltpu.VMEM((scr, tok), BF16), pltpu.VMEM((scr, d), BF16), pltpu.VMEM((rows, d), BF16)]
    if with_r:
        out_shape.append(jax.ShapeDtypeStruct((rows, 128), F32))
        scratch += [pltpu.VMEM((scr, 128), F32), pltpu.VMEM((rows, 128), F32)]
    out = pl.pallas_call(
        functools.partial(gather_kernel, n_src, n_loc, region, up((region - TILE) // n_src, CHUNK), with_r),
        out_shape=out_shape,
        grid_spec=pltpu.PrefetchScalarGridSpec(
            num_scalar_prefetch=2, grid=(n_src,), in_specs=in_specs,
            out_specs=[pl.BlockSpec(memory_space=pl.ANY)] * len(out_shape),
            scratch_shapes=scratch + [pltpu.SemaphoreType.DMA]),
        compiler_params=pltpu.CompilerParams(vmem_limit_bytes=VMEM_LIMIT, dimension_semantics=("arbitrary",)),
        cost_estimate=pl.CostEstimate(flops=2 * 12000 * tok * d, bytes_accessed=n_src * tok * d * 4, transcendentals=0),
        name="gather_r" if with_r else "gather_x",
    )(*([cnt, off, pos] + ([r] if with_r else []) + [src]))
    return out if with_r else out[0]


def expert_kernel(n_fs, info, x_ref, dy_ref, r_ref, *refs):
    own, peers, refs = refs[:3], refs[3:n_fs + 2], refs[n_fs + 2:]
    (dx_ref, dr_ref), outs, refs = refs[:2], refs[2:n_fs + 2], refs[n_fs + 2:]
    w1_ref, w3_ref, w2t, a_buf, dh1_buf, dh3_buf, dw1, dw3, dw2t = refs
    i = pl.program_id(0)
    d, f = w1_ref.shape
    dsl = d // n_fs

    @pl.when(i == 0)
    def _():
        dw1[...] = jnp.zeros_like(dw1)
        dw3[...] = jnp.zeros_like(dw3)
        dw2t[...] = jnp.zeros_like(dw2t)
        for m in range(n_fs):
            at = pl.ds(aligned((info[2] ^ m) * dsl, dsl), dsl)
            for t, whole in enumerate((w1_ref, w3_ref, w2t)):
                whole[at, :] = peers[m - 1][0, t] if m else own[t][0]

    def tile(m):
        x, dy = x_ref[:m, :], dy_ref[:m, :]
        dy_wide = dy.astype(F32)
        g = (r_ref[:m, 0:1] * dy_wide).astype(BF16)
        step = 256
        for c in range(0, f, step):
            cs = slice(c, c + step)
            h1 = dot(x, w1_ref[:, cs])
            h3 = dot(x, w3_ref[:, cs])
            da = dot(g, w2t[:, cs])
            s = jax.nn.sigmoid(h1)
            hs = h1 * s
            a_buf[:m, cs] = (hs * h3).astype(BF16)
            dh1_buf[:m, cs] = (da * h3 * s * (1.0 + h1 * (1.0 - s))).astype(BF16)
            dh3_buf[:m, cs] = (da * hs).astype(BF16)
        y = dot_nt(a_buf[:m, :], w2t[...])
        dr = jnp.sum(dy_wide * y, axis=1, keepdims=True)
        dr_ref[:m, :] = jnp.broadcast_to(dr, (m, 128))
        dx_ref[:m, :] = (dot_nt(dh1_buf[:m, :], w1_ref[...]) + dot_nt(dh3_buf[:m, :], w3_ref[...])).astype(BF16)
        dw1[...] += dot_tn(x, dh1_buf[:m, :])
        dw3[...] += dot_tn(x, dh3_buf[:m, :])
        dw2t[...] += dot_tn(g, a_buf[:m, :])

    left = info[0] - i * TILE

    @pl.when(left > TILE // 2)
    def _():
        tile(TILE)

    @pl.when((i < info[1]) & (left <= TILE // 2))
    def _():
        tile(TILE // 2)
        dx_ref[TILE // 2:, :] = jnp.zeros((TILE // 2, d), BF16)
        dr_ref[TILE // 2:, :] = jnp.zeros((TILE // 2, 128), F32)

    @pl.when(i == info[1] - 1)
    def _():
        for m in range(n_fs):
            at = pl.ds(aligned((info[2] ^ m) * dsl, dsl), dsl)
            for t, acc in enumerate((dw1, dw3, dw2t)):
                outs[m][t] = acc[at, :]


def expert_call(k, group_at, n_loc, info, x_pool, dy_pool, r_pool, own, peers, region):
    n_fs, (_, _, dsl, f) = len(peers) + 1, peers[0].shape
    d = n_fs * dsl
    first = k * (region // TILE)
    row_map = lambda i, info: (first + jnp.minimum(i, info[1] - 1), 0)
    out_map = lambda i, info: (jnp.minimum(i, info[1] - 1), 0)
    whole3 = lambda i, info: (0, 0, 0)
    mine = lambda i, info: (info[2] * n_loc + k, 0, 0)
    return pl.pallas_call(
        functools.partial(expert_kernel, n_fs),
        out_shape=[jax.ShapeDtypeStruct((region, d), BF16), jax.ShapeDtypeStruct((region, 128), F32)]
        + [jax.ShapeDtypeStruct((3, dsl, f), F32)] * n_fs,
        grid_spec=pltpu.PrefetchScalarGridSpec(
            num_scalar_prefetch=1, grid=(region // TILE - 1,),
            in_specs=[pl.BlockSpec((TILE, d), row_map), pl.BlockSpec((TILE, d), row_map), pl.BlockSpec((TILE, 128), row_map),
                      *[pl.BlockSpec((1, dsl, f), mine)] * 2, pl.BlockSpec((1, dsl, f), lambda i, info: (k, 0, 0)),
                      *[pl.BlockSpec((1, 3, dsl, f), lambda i, info: (group_at, 0, 0, 0))] * (n_fs - 1)],
            out_specs=[pl.BlockSpec((TILE, d), out_map), pl.BlockSpec((TILE, 128), out_map)]
            + [pl.BlockSpec((3, dsl, f), whole3)] * n_fs,
            scratch_shapes=[pltpu.VMEM((d, f), BF16)] * 3 + [pltpu.VMEM((TILE, f), BF16)] * 3 + [pltpu.VMEM((d, f), F32)] * 3),
        compiler_params=pltpu.CompilerParams(vmem_limit_bytes=VMEM_LIMIT, dimension_semantics=("arbitrary",)),
        cost_estimate=pl.CostEstimate(flops=18 * 3000 * d * f, bytes_accessed=24 * d * f, transcendentals=3000 * f),
    )(info, x_pool, dy_pool, r_pool, *own, *peers)


def place_kernel(n_fs, n_loc, ks, first, me, *refs):
    n_pieces = n_fs * len(ks)
    pieces, refs = refs[:n_pieces], refs[n_pieces + (0 if first else 3):]
    outs, (held, turned, in_sem, out_sem) = refs[:3], refs[3:]
    reads = [pltpu.make_async_copy(piece, held.at[n], in_sem.at[n]) for n, piece in enumerate(pieces)]
    for copy in reads:
        copy.start()
    writes = []
    for n, copy in enumerate(reads):
        copy.wait()
        to = (me[0] ^ n % n_fs) * n_loc + ks[n // n_fs]
        for t in range(2):
            writes.append(pltpu.make_async_copy(held.at[n, t], outs[t].at[to], out_sem))
            writes[-1].start()
        turned[n] = held[n, 2].T
        writes.append(pltpu.make_async_copy(turned.at[n], outs[2].at[to], out_sem))
        writes[-1].start()
    for copy in writes:
        copy.wait()


def place(ks, n_loc, me, pieces, grads):
    n_fs = len(pieces) // len(ks)
    _, dsl, f = pieces[0].shape
    hbm = pl.BlockSpec(memory_space=pl.ANY)
    first = grads is None
    n = len(pieces)
    shapes = [(n_fs * n_loc, dsl, f)] * 2 + [(n_fs * n_loc, f, dsl)]
    return pl.pallas_call(
        functools.partial(place_kernel, n_fs, n_loc, ks, first),
        out_shape=[jax.ShapeDtypeStruct(v, F32) for v in shapes],
        in_specs=[pl.BlockSpec(memory_space=pltpu.SMEM)] + [hbm] * (n if first else n + 3),
        out_specs=[hbm] * 3,
        scratch_shapes=[pltpu.VMEM((n, 3, dsl, f), F32), pltpu.VMEM((n, f, dsl), F32),
                        pltpu.SemaphoreType.DMA((n,)), pltpu.SemaphoreType.DMA],
        input_output_aliases={} if first else {n + 1 + t: t for t in range(3)},
        compiler_params=pltpu.CompilerParams(vmem_limit_bytes=VMEM_LIMIT),
        cost_estimate=pl.CostEstimate(flops=0, bytes_accessed=6 * 4 * n * dsl * f, transcendentals=0),
    )(me, *pieces, *([] if first else grads))


def combine_kernel(n_src, n_loc, slots, cnt, off, pos_ref, *refs):
    dx_in, dr_in = refs[:n_loc], refs[n_loc:2 * n_loc]
    out, dr_out, hot, stage, pool, rpool, sem = refs[2 * n_loc:]
    s = pl.program_id(0)
    tok = pos_ref.shape[2]
    d = pool.shape[2]

    @pl.when(s == 0)
    def _():
        def copies(k, i):
            at = pl.ds(aligned(i * TILE, TILE), TILE)
            return [pltpu.make_async_copy(dx_in[k].at[at], pool.at[k, at], sem),
                    pltpu.make_async_copy(dr_in[k].at[at], rpool.at[k, at], sem)]

        tiles = []
        for k in range(n_loc):
            last = (n_src - 1) * n_loc + k
            end = off[last] + blocks(cnt[last], 16) * 16
            tiles.append(jnp.maximum(1, blocks(end, TILE)))
        for k in range(n_loc):
            def start(i, carry, k=k):
                for copy in copies(k, i):
                    copy.start()
                return carry

            lax.fori_loop(0, tiles[k], start, 0)
            at = pl.ds(aligned(tiles[k] * TILE), TILE)
            pool[k, at, :] = jnp.zeros((TILE, d), BF16)
            rpool[k, at, :] = jnp.zeros((TILE, 128), F32)
        for k in range(n_loc):
            def wait(i, carry, k=k):
                for copy in copies(k, i):
                    copy.wait()
                return carry

            lax.fori_loop(0, tiles[k], wait, 0)

    dr_out[...] = jnp.zeros_like(dr_out)
    base = jnp.int32(0)
    for k in range(n_loc):
        n = cnt[s * n_loc + k]
        frm = off[s * n_loc + k]
        pos_row = pos_ref[0, k:k + 1, :]

        def build(first, size, base=base, frm=frm, pos_row=pos_row, k=k):
            m = one_hot_block(pos_row, first, size)
            at = pl.ds(aligned(base + first), size)
            src = pl.ds(aligned(frm + first), size)
            hot[at, :] = jnp.where(m, 1.0, 0.0).astype(BF16)
            stage[at, :] = pool[k, src, :]
            r = jnp.concatenate([rpool[k, src, :]] * (tok // 128), axis=1)
            dr_out[0, k:k + 1, :] += jnp.sum(jnp.where(m, r, 0.0), axis=0, keepdims=True)

        build(0, CHUNK)
        pl.when(n > CHUNK)(functools.partial(build, CHUNK, slots - CHUNK))
        base = base + blocks(n, 16) * 16

    def clear(size):
        tail = pl.ds(aligned(base), size)
        hot[tail, :] = jnp.zeros((size, tok), BF16)
        stage[tail, :] = jnp.zeros((size, d), BF16)

    clear(TIERS[0])
    pl.when(base > TIERS[1])(functools.partial(clear, hot.shape[0] - n_loc * slots))

    def mm(first, size):
        at = pl.ds(first, size)
        part = dot_tn(hot[at, :], stage[at, :])
        out[...] = part if first == 0 else out[...] + part

    tiers(base, n_loc * slots, mm)


def combine_rows(cnt, off, pos, dx_pools, dr_pools, region):
    n_src, n_loc, tok = pos.shape
    d = dx_pools[0].shape[1]
    slots = up((region - TILE) // n_src, CHUNK)
    scr = n_loc * slots + TILE
    hbm = pl.BlockSpec(memory_space=pl.ANY)
    return pl.pallas_call(
        functools.partial(combine_kernel, n_src, n_loc, slots),
        out_shape=[jax.ShapeDtypeStruct((n_src * tok, d), F32), jax.ShapeDtypeStruct((n_src, n_loc, tok), F32)],
        grid_spec=pltpu.PrefetchScalarGridSpec(
            num_scalar_prefetch=2, grid=(n_src,),
            in_specs=[pl.BlockSpec((1, n_loc, tok), lambda s, *_: (s, 0, 0))] + [hbm] * (2 * n_loc),
            out_specs=[pl.BlockSpec((tok, d), lambda s, *_: (s, 0)),
                       pl.BlockSpec((1, n_loc, tok), lambda s, *_: (s, 0, 0))],
            scratch_shapes=[pltpu.VMEM((scr, tok), BF16), pltpu.VMEM((scr, d), BF16),
                            pltpu.VMEM((n_loc, region, d), BF16), pltpu.VMEM((n_loc, region, 128), F32),
                            pltpu.SemaphoreType.DMA]),
        compiler_params=pltpu.CompilerParams(vmem_limit_bytes=VMEM_LIMIT, dimension_semantics=("arbitrary",)),
        cost_estimate=pl.CostEstimate(flops=2 * 12000 * tok * d, bytes_accessed=n_src * tok * d * 4, transcendentals=0),
        name="combine",
    )(cnt, off, pos, *dx_pools, *dr_pools)


MESH = pl.DeviceIdType.MESH
HOPS = ((0, 2), (1, 0), (2, 0))
SIBLING = (0, 1)
SPREAD_ORDERS = ((1, 2, 0), (2, 1, 0), (0, 1, 2), (0, 2, 1))
COLLECT_ORDERS = ((0, 1, 2), (0, 2, 1), (1, 2, 0), (2, 1, 0))


def parts_of(tok):
    long = tok * 5 // 16 // 16 * 16
    return long, long, tok // 2 - long, tok // 2 - long


def here():
    return lax.axis_index("fsdp"), lax.axis_index("ep")


def peer_of(hop):
    f, p = here()
    return {"fsdp": f ^ hop[0], "ep": p ^ hop[1]}


def block_of(bits, core=0):
    f, p = here()
    for axis in range(3):
        if bits >> axis & 1:
            f, p = f ^ HOPS[axis][0], p ^ HOPS[axis][1]
    return f * 4 + (p ^ core)


def enter(n_fs, n_ep):
    barrier = pltpu.get_barrier_semaphore()
    for df in range(n_fs):
        for dp in range(n_ep):
            if df or dp:
                pl.semaphore_signal(barrier, inc=1, device_id=peer_of((df, dp)), device_id_type=MESH)
    pl.semaphore_wait(barrier, n_fs * n_ep - 1)


def exchange(n_fs, n_ep, src, dst, send, recv):
    f, p = here()
    copies = []
    for df in range(n_fs):
        for dp in range(n_ep):
            if df or dp:
                n = df * n_ep + dp
                copies.append(pltpu.make_async_remote_copy(
                    src_ref=src.at[(f ^ df) * n_ep + (p ^ dp)], dst_ref=dst.at[f * n_ep + p],
                    send_sem=send.at[n], recv_sem=recv.at[n], device_id=peer_of((df, dp)), device_id_type=MESH))
                copies[-1].start()
    return copies


def spread_kernel(n_fs, n_ep, n_loc, parts, x_ref, dy_ref, table_ref, wg_ref, wu_ref, wd_ref, full, table_all, *refs):
    n_out = 3 * (n_fs - 1)
    own_down, w_out, refs = refs[0], refs[1:n_out + 1], refs[n_out + 1:]
    own, send, recv, c_send, c_recv, t_send, t_recv, own_sem, w_buf, down_buf, in_sem, out_sem, w_send, w_recv = refs
    tok, d = x_ref.shape
    mine = block_of(0)
    local = []
    for n, src in enumerate((x_ref, dy_ref)):
        local.append(pltpu.make_async_copy(src, own.at[:, pl.ds(n * d, d)], own_sem.at[n]))
        local[-1].start()
    enter(n_fs, n_ep)
    for copy in local:
        copy.wait()
    local = [pltpu.make_async_copy(own, full.at[pl.ds(aligned(mine * tok, tok), tok)], own_sem.at[0]),
             pltpu.make_async_copy(table_ref.at[mine], table_all.at[mine], own_sem.at[2])]
    starts = [sum(parts[:q]) for q in range(len(parts))]
    sem_at = {}
    inbound = {}

    def send_on(q, phase, bits):
        to = pl.ds(aligned(block_of(bits) * tok + starts[q], 16), parts[q])
        src = own.at[pl.ds(starts[q], parts[q])] if bits == 0 else full.at[to]
        n = sem_at.setdefault((q, phase, bits), len(sem_at))
        copy = pltpu.make_async_remote_copy(
            src_ref=src, dst_ref=full.at[to], send_sem=send.at[n], recv_sem=recv.at[n],
            device_id=peer_of(HOPS[SPREAD_ORDERS[q][phase]]), device_id_type=MESH)
        copy.start()
        inbound[(q, phase, bits)] = copy

    shared = []

    def share(q, bits):
        to = pl.ds(aligned(block_of(bits) * tok + starts[q], 16), parts[q])
        src = own.at[pl.ds(starts[q], parts[q])] if bits == 0 else full.at[to]
        n = len(shared)
        copy = pltpu.make_async_remote_copy(
            src_ref=src, dst_ref=full.at[to], send_sem=c_send.at[n], recv_sem=c_recv.at[n],
            device_id=peer_of(SIBLING), device_id_type=MESH)
        copy.start()
        shared.append(copy)

    for phase in range(3):
        for q in range(len(parts)):
            send_on(q, phase, 0)
    for q in range(len(parts)):
        share(q, 0)
    for copy in local:
        copy.start()
    pending = exchange(n_fs, n_ep, table_ref, table_all, t_send, t_recv)
    f, _ = here()
    packs = []
    for k in range(n_loc):
        for m in range(n_fs):
            n = k * n_fs + m
            at = (f ^ m) * n_loc + k
            packs.append([pltpu.make_async_copy(wd_ref.at[at], down_buf.at[n], in_sem.at[3 * n])])
            if m:
                packs[-1] += [pltpu.make_async_copy(w.at[at], w_buf.at[n, t], in_sem.at[3 * n + 1 + t])
                              for t, w in enumerate((wg_ref, wu_ref))]
            for copy in packs[-1]:
                copy.start()
    for n in range(n_loc * n_fs):
        for copy in packs[n]:
            copy.wait()
        w_buf[n, 2] = down_buf[n].T
        k, m = n // n_fs, n % n_fs
        if m == 0:
            copy = pltpu.make_async_copy(w_buf.at[n, 2], own_down.at[k], out_sem.at[n])
        elif k == 0:
            continue
        else:
            group = min(k, 2)
            copy = pltpu.make_async_copy(w_buf.at[n], w_out[group * (n_fs - 1) + m - 1].at[k - group], out_sem.at[n])
        copy.start()
        local.append(copy)
    for phase in range(3):
        for q in range(len(parts)):
            held = [0]
            for axis in SPREAD_ORDERS[q][:phase]:
                held += [b | 1 << axis for b in held]
            for b in held:
                inbound[(q, phase, b)].wait_recv()
                got = b | 1 << SPREAD_ORDERS[q][phase]
                for later in range(phase + 1, 3):
                    send_on(q, later, got)
                share(q, got)
        if phase == 1:
            for m in range(1, n_fs):
                pending.append(pltpu.make_async_remote_copy(
                    src_ref=w_buf.at[m], dst_ref=w_out[m - 1].at[0], send_sem=w_send.at[m - 1], recv_sem=w_recv.at[m - 1],
                    device_id=peer_of((m, 0)), device_id_type=MESH))
                pending[-1].start()
    for copy in inbound.values():
        copy.wait_send()
    for copy in shared:
        copy.wait()
    for copy in pending:
        copy.wait()
    for copy in local:
        copy.wait()


def spread(x_tok, dy_tok, table, w_gate, w_up, w_down, n_fs, n_ep):
    n_dev = n_fs * n_ep
    tok, d = x_tok.shape
    exp_local, dsl, f = w_gate.shape
    n_loc = exp_local // n_fs
    n_slices, groups = n_loc * n_fs, [1] * (2 * n_fs - 2) + [n_loc - 2] * (n_fs - 1)
    parts = parts_of(tok)
    vmem, hbm = pl.BlockSpec(memory_space=pltpu.VMEM), pl.BlockSpec(memory_space=pl.ANY)
    dma = pltpu.SemaphoreType.DMA
    return pl.pallas_call(
        functools.partial(spread_kernel, n_fs, n_ep, n_loc, parts),
        out_shape=[jax.ShapeDtypeStruct((n_dev * tok, 2 * d), x_tok.dtype), jax.ShapeDtypeStruct(table.shape, table.dtype)]
        + [jax.ShapeDtypeStruct((n_loc, dsl, f), BF16)] + [jax.ShapeDtypeStruct((g, 3, dsl, f), BF16) for g in groups],
        in_specs=[hbm] * 2 + [vmem] + [hbm] * 3, out_specs=[hbm] * (3 + len(groups)),
        scratch_shapes=[pltpu.VMEM((tok, 2 * d), BF16), dma((28,)), dma((28,)), dma((32,)), dma((32,)), dma((n_dev,)), dma((n_dev,)),
                        dma((3,)), pltpu.VMEM((n_slices, 3, dsl, f), BF16), pltpu.VMEM((n_slices, f, dsl), BF16),
                        dma((3 * n_slices,)), dma((n_slices,)), dma((n_fs - 1,)), dma((n_fs - 1,))],
        compiler_params=pltpu.CompilerParams(collective_id=0, has_side_effects=True, vmem_limit_bytes=VMEM_LIMIT),
        cost_estimate=pl.CostEstimate(flops=0, bytes_accessed=8 * n_dev * tok * d, transcendentals=0),
        name="spread",
    )(x_tok, dy_tok, table, w_gate, w_up, w_down)


def collect_kernel(n_fs, n_ep, parts, part_ref, dr_ref, gx_ref, dr_home, acc, sib, got,
                   c_send, c_recv, send, recv, t_send, t_recv, own_sem):
    tok = gx_ref.shape[0]
    mine = block_of(0)
    enter(n_fs, n_ep)
    drs = exchange(n_fs, n_ep, dr_ref, dr_home, t_send, t_recv)
    local_dr = pltpu.make_async_copy(dr_ref.at[mine], dr_home.at[mine], own_sem.at[8])
    local_dr.start()
    order = (7, 3, 5, 6, 1, 2, 4, 0)
    loads, shares = {}, {}
    for bits in order:
        theirs = pl.ds(aligned(block_of(bits, 1) * tok, tok), tok)
        shares[bits] = pltpu.make_async_remote_copy(
            src_ref=part_ref.at[theirs], dst_ref=sib.at[bits], send_sem=c_send.at[bits], recv_sem=c_recv.at[bits],
            device_id=peer_of(SIBLING), device_id_type=MESH)
        shares[bits].start()
        ours = pl.ds(aligned(block_of(bits) * tok, tok), tok)
        loads[bits] = pltpu.make_async_copy(part_ref.at[ours], acc.at[bits], own_sem.at[bits])
        loads[bits].start()
    starts = [sum(parts[:q]) for q in range(len(parts))]
    slots = [(q, bits) for q in range(len(parts)) for bits in range(1, 8)]
    hops = {}

    def phase_of(q, bits):
        return next(n for n in range(3) if bits >> COLLECT_ORDERS[q][n] & 1)

    def send_off(q, bits):
        n = slots.index((q, bits))
        rows = pl.ds(starts[q], parts[q])
        hops[(q, bits)] = pltpu.make_async_remote_copy(
            src_ref=acc.at[bits, rows], dst_ref=got.at[bits - 1, rows], send_sem=send.at[n], recv_sem=recv.at[n],
            device_id=peer_of(HOPS[COLLECT_ORDERS[q][phase_of(q, bits)]]), device_id_type=MESH)
        hops[(q, bits)].start()

    def add_arrival(q, bits, phase):
        frm = bits | 1 << COLLECT_ORDERS[q][phase]
        hops[(q, frm)].wait_recv()
        rows = slice(starts[q], starts[q] + parts[q])
        acc[bits, rows, :] = acc[bits, rows, :] + got[frm - 1, rows, :]

    for bits in order:
        loads[bits].wait()
        shares[bits].wait_recv()
        acc[bits] = acc[bits] + sib[bits]
        for q in range(len(parts)):
            if bits and phase_of(q, bits) == 0:
                send_off(q, bits)
    for phase in (1, 2):
        for q in range(len(parts)):
            for bits in range(1, 8):
                if phase_of(q, bits) == phase:
                    for earlier in range(phase):
                        add_arrival(q, bits, earlier)
                    send_off(q, bits)
    for q in range(len(parts)):
        for phase in range(3):
            add_arrival(q, 0, phase)
        rows = slice(starts[q], starts[q] + parts[q])
        gx_ref[rows, :] = acc[0, rows, :].astype(gx_ref.dtype)
    for bits in order:
        shares[bits].wait_send()
    for copy in hops.values():
        copy.wait_send()
    for copy in drs:
        copy.wait()
    local_dr.wait()


def collect(dx_part, dr_part, n_fs, n_ep):
    n_dev = n_fs * n_ep
    tok, d = dx_part.shape[0] // n_dev, dx_part.shape[1]
    parts = parts_of(tok)
    vmem, hbm = pl.BlockSpec(memory_space=pltpu.VMEM), pl.BlockSpec(memory_space=pl.ANY)
    dma = pltpu.SemaphoreType.DMA
    return pl.pallas_call(
        functools.partial(collect_kernel, n_fs, n_ep, parts),
        out_shape=[jax.ShapeDtypeStruct((tok, d), BF16), jax.ShapeDtypeStruct(dr_part.shape, F32)],
        in_specs=[hbm, vmem], out_specs=[vmem, vmem],
        scratch_shapes=[pltpu.VMEM((8, tok, d), F32), pltpu.VMEM((8, tok, d), F32), pltpu.VMEM((7, tok, d), F32),
                        dma((8,)), dma((8,)), dma((28,)), dma((28,)), dma((n_dev,)), dma((n_dev,)), dma((9,))],
        compiler_params=pltpu.CompilerParams(collective_id=1, has_side_effects=True, vmem_limit_bytes=VMEM_LIMIT),
        cost_estimate=pl.CostEstimate(flops=0, bytes_accessed=8 * n_dev * tok * d, transcendentals=0),
        name="collect",
    )(dx_part, dr_part)


def solution(mesh):
    n_ep, n_fs = mesh.shape["ep"], mesh.shape["fsdp"]
    n_dev = n_ep * n_fs
    both = ("fsdp", "ep")
    tok_spec = P(both, None)
    spec_in = P("ep", "fsdp", None)
    spec_out = P("ep", None, "fsdp")

    def body(x_tok, dy_tok, expert_ids, route_w, w_gate, w_up, w_down):
        tok, top_k = expert_ids.shape
        exp_local, _, _ = w_gate.shape
        n_loc = exp_local // n_fs
        experts = exp_local * n_ep
        capacity = capacity_of(tok, top_k, experts)
        region = n_dev * up(capacity, 16) + TILE

        position, weight = route_tables(expert_ids, route_w, experts, capacity)
        table = jnp.stack([position, weight], axis=1).reshape(n_ep, n_fs, n_loc, 2, tok)
        table = table.transpose(1, 0, 2, 3, 4).reshape(n_dev, n_loc * 2, tok)
        xdy_all, table, own_down, *packed = spread(x_tok, dy_tok, table, w_gate, w_up, w_down, n_fs, n_ep)
        table = table.reshape(n_dev, n_loc, 2, tok)
        me = lax.axis_index("fsdp").astype(jnp.int32)
        weights = [packed[:n_fs - 1]]
        for group in (1, 2):
            weights.append([lax.ppermute(packed[group * (n_fs - 1) + m - 1], "fsdp", [(i, i ^ m) for i in range(n_fs)])
                            for m in range(1, n_fs)])

        pos = table[:, :, 0, :].astype(jnp.int32)
        r = table[:, :, 1, :]
        cnt = jnp.max(pos, axis=2) + 1
        padded = blocks(cnt, 16) * 16
        off = jnp.cumsum(padded, axis=0) - padded
        rows = jnp.sum(padded, axis=0)
        cnt_flat, off_flat = cnt.reshape(-1), off.reshape(-1)
        x_pool = gather_rows(xdy_all, cnt_flat, off_flat, pos, None, region)
        dy_pool, r_pool = gather_rows(xdy_all, cnt_flat, off_flat, pos, r, region)

        dx_pools, dr_pools, pieces = [], [], []
        for k in range(n_loc):
            info = jnp.stack([rows[k], jnp.maximum(1, blocks(rows[k], TILE)), me])
            dxk, drk, *slices = expert_call(
                k, max(k - 2, 0), n_loc, info, x_pool, dy_pool, r_pool, (w_gate, w_up, own_down),
                weights[min(k, 2)], region)
            dx_pools.append(dxk)
            dr_pools.append(drk)
            pieces.append([slices[0]] + [lax.ppermute(slices[m], "fsdp", [(i, i ^ m) for i in range(n_fs)])
                                         for m in range(1, n_fs)])
        dx_part, dr_part = combine_rows(cnt_flat, off_flat, pos, dx_pools, dr_pools, region)
        grad_x, dr_home = collect(dx_part, dr_part, n_fs, n_ep)
        dr_home = dr_home.reshape(n_fs, n_ep, n_loc, tok).transpose(1, 0, 2, 3).reshape(experts, tok)
        hit = expert_ids.T[:, None, :] == jnp.arange(experts, dtype=jnp.int32)[None, :, None]
        route_grad = jnp.sum(jnp.where(hit, dr_home[None], 0.0), axis=1).T
        grads = None
        for ks in (tuple(range(n_loc // 2)), tuple(range(n_loc // 2, n_loc))):
            grads = place(ks, n_loc, me.reshape(1), [piece for k in ks for piece in pieces[k]], grads)
        return grad_x, route_grad, *grads

    return jax.shard_map(
        body, mesh=mesh,
        in_specs=(tok_spec, tok_spec, tok_spec, tok_spec, spec_in, spec_in, spec_out),
        out_specs=(tok_spec, tok_spec, spec_in, spec_in, spec_out),
        check_vma=False)
```
